256 devices in a mesh: rack: 8 (over x, core), chip: 32 (over y, z).
Axes of the slice: x: 4, y: 4, z: 8, core: 2. Of those that a mesh axis runs over, the one named last changes fastest.
Arguments:
- points: float32 [512, 4, 32, 256], P(('rack', 'chip')), may hold values from -6 to 6
- counts: int32 [512, 256], P(('rack', 'chip')), may hold values from 1 to 32
- cells: int32 [512, 256], P(('rack', 'chip')), may hold values from 0 to 2047, as said below
- pfn_weight: float32 [9, 64], replicated, may hold values from -2 to 2
- pfn_gain: float32 [64], replicated, may hold values from 0.5 to 1.5
- pfn_bias: float32 [64], replicated, may hold values from -3 to 3
- conv_weight: float32 [4, 9, 4096], replicated, may hold values from -0.25 to 0.25
- bn_gain: float32 [4, 64], replicated, may hold values from 0.5 to 1.5
- bn_bias: float32 [4, 64], replicated, may hold values from -3 to 3
- cotangent: float32 [512, 64, 4, 128], P(('rack', 'chip')), may hold values from -0.006 to 0.006
Outputs:
- features: float32 [512, 64, 4, 128], P(('rack', 'chip'))
- conv_grads: float32 [4, 9, 4096], replicated
- norm_grads: float32 [2, 4, 64], replicated
- pillar_grad: float32 [512, 64, 256], P(('rack', 'chip'))
The draws below stay inside these ranges and needn't reach their ends.
Inputs may be any that keep to these rules, and one draw needn't show every extreme that they name: `cells`: within one sweep no two pillars share a cell.
All inputs are finite; a program needn't handle non-finite values.
Results may differ from the reference program's by a relative error of at most 0.0003.
Values sent between devices are 32-bit elements; how exact they have to be, the bound alone decides.
No kernel may reach another device: no remote copies, remote signals or barrier semaphores. Data moves between devices by JAX's collectives and lax.ppermute only.
A program may use at most 128 MiB of HBM per device.

```python
import jax
import jax.numpy as jnp
from jax import lax

C = 64
MAXP = 32
LAYERS = 4
GH = 8
GW = 256
PILL = 256
SWEEPS = 512


def draw_cells(key, part):
    keys = jax.random.split(key, SWEEPS)

    def one_sweep(sweep_key):
        return jax.random.permutation(sweep_key, GH * GW)[:PILL].astype(jnp.int32)
    return jax.vmap(one_sweep)(keys)


def touch_ends(values, own_key, least, largest):
    dims = values.shape
    spot = [jax.random.randint(jax.random.fold_in(own_key, axis), (), 0, dims[axis]) for axis in range(len(dims))]
    values = values.at[tuple(spot)].set(least)
    longest = dims.index(max(dims))
    spot[longest] = (spot[longest] + 1) % dims[longest]
    return values.at[tuple(spot)].set(largest)


def steps_of(rng, dims, pieces, smallest, largest):
    def one(axis_at, shards_of):
        heights = jax.random.uniform(jax.random.fold_in(jax.random.fold_in(rng, 6), axis_at), (shards_of,), jnp.float32, smallest / len(pieces), largest / len(pieces))
        return jnp.repeat(jnp.exp(heights), dims[axis_at] // shards_of).reshape((-1,) + (1,) * (len(dims) - axis_at - 1))

    level = one(*pieces[0])
    for cut in pieces[1:]:
        level = level * one(*cut)
    return level


def bell_draw(own_key, shape, spread, bound, pieces=(), kind=jnp.bfloat16):
    values = jax.random.normal(own_key, shape, jnp.float32) * spread
    if len(pieces) > 0:
        values = steps_of(own_key, shape, pieces, -0.22, 0.18) * values
    return jnp.clip(values, min=-bound, max=bound).astype(kind)


def setup_inputs(seed: int = 0) -> dict:
    streams_of = jax.random.split(jax.random.key(seed), 11)
    points = bell_draw(streams_of[0], (SWEEPS, 4, MAXP, PILL), 1.0, 6.0, ((0, 256),), jnp.float32)
    counts = touch_ends(jax.random.randint(streams_of[1], (SWEEPS, PILL), 1, MAXP + 1), jax.random.fold_in(streams_of[1], 1), 1, MAXP).astype(jnp.int32)
    cells = draw_cells(jax.random.fold_in(streams_of[10], 71), 0)
    pfn_weight = bell_draw(streams_of[3], (9, C), 9 ** -0.5, 2.0, (), jnp.float32)
    pfn_gain = jnp.clip(1.0 + 0.1 * jax.random.normal(streams_of[4], (C,), jnp.float32), 0.5, 1.5)
    pfn_bias = bell_draw(streams_of[5], (C,), 0.5, 3.0, (), jnp.float32)
    conv_weight = bell_draw(streams_of[6], (LAYERS, 9, C * C), (9 * C) ** -0.5, 0.25, (), jnp.float32)
    bn_gain = jnp.clip(1.0 + 0.1 * jax.random.normal(streams_of[7], (LAYERS, C), jnp.float32), 0.5, 1.5)
    bn_bias = bell_draw(streams_of[8], (LAYERS, C), 0.5, 3.0, (), jnp.float32)
    cotangent = bell_draw(streams_of[9], (SWEEPS, C, GH // 2, GW // 2), 0.001, 0.006, ((0, 256),), jnp.float32)
    return dict(points=points, counts=counts, cells=cells, pfn_weight=pfn_weight, pfn_gain=pfn_gain, pfn_bias=pfn_bias, conv_weight=conv_weight, bn_gain=bn_gain, bn_bias=bn_bias, cotangent=cotangent)


EPS = 1e-05
PRECISE = lax.Precision.HIGHEST

def channel_shape(vector, ndim):
    return vector.reshape((1, -1) + (1,) * (ndim - 2))

def silu_slope(pre_act):
    sigma = jax.nn.sigmoid(pre_act)
    return sigma * (1.0 + pre_act * (1.0 - sigma))

def pillar_hidden(points, counts, cells, pfn_weight):
    slot_ids = lax.broadcasted_iota(jnp.int32, (1, points.shape[2], 1), 1)
    is_valid = (slot_ids < counts[:, None, :]).astype(jnp.float32)
    point_count = counts.astype(jnp.float32)
    centroid = lax.optimization_barrier(jnp.sum(points[:, 0:3] * is_valid[:, None], axis=2)) / point_count[:, None]
    col_pos = (cells % GW).astype(jnp.float32) * (2.0 / GW) - 1.0
    row_pos = (cells // GW).astype(jnp.float32) * (2.0 / GH) - 1.0
    offsets = points[:, 0:3] - centroid[:, :, None, :]
    grid_off = jnp.stack([points[:, 0] - col_pos[:, None, :], points[:, 1] - row_pos[:, None, :]], axis=1)
    inputs = jnp.concatenate([points, offsets, grid_off], axis=1)
    hidden = jnp.einsum('fc,sfpq->scpq', pfn_weight, inputs, precision=PRECISE)
    return (hidden, is_valid)

def normalize_pillars(hidden, is_valid, mean_val, inv_std, gain, bias):
    scaled = channel_shape(gain, 4) * (hidden - channel_shape(mean_val, 4)) * channel_shape(inv_std, 4) + channel_shape(bias, 4)
    return lax.optimization_barrier(jnp.max(jnp.maximum(scaled, 0.0) * is_valid[:, None], axis=2))

def scatter_pillars(pillar, cells):
    empty = jnp.zeros((pillar.shape[1], GH * GW), pillar.dtype)
    placed = jax.vmap(lambda feature, target: empty.at[:, target].set(feature))(pillar, cells)
    return placed.reshape(pillar.shape[0], pillar.shape[1], GH, GW)

def conv_forward(activation, taps, stride):
    padded = jnp.pad(activation, ((0, 0), (0, 0), (1, 1), (1, 1)))
    height = activation.shape[2] // stride
    width = activation.shape[3] // stride
    result = jnp.zeros((activation.shape[0], C, height, width), jnp.float32)
    for row_tap in range(3):
        for col_tap in range(3):
            tap_slice = padded[:, :, row_tap:row_tap + stride * height:stride, col_tap:col_tap + stride * width:stride]
            kernel = taps[3 * row_tap + col_tap].reshape(C, C)
            result = result + jnp.einsum('oi,nihw->nohw', kernel, tap_slice, precision=PRECISE)
    return result

def conv_backward(activation, taps, grad_z, stride):
    padded = jnp.pad(activation, ((0, 0), (0, 0), (1, 1), (1, 1)))
    height = grad_z.shape[2]
    width = grad_z.shape[3]
    grad_pad = jnp.zeros(padded.shape, jnp.float32)
    tap_grads = []
    for row_tap in range(3):
        for col_tap in range(3):
            tap_slice = padded[:, :, row_tap:row_tap + stride * height:stride, col_tap:col_tap + stride * width:stride]
            tap_grads.append(jnp.einsum('nohw,nihw->oi', grad_z, tap_slice, precision=PRECISE).reshape(C * C))
            kernel = taps[3 * row_tap + col_tap].reshape(C, C)
            back = jnp.einsum('oi,nohw->nihw', kernel, grad_z, precision=PRECISE)
            grad_pad = grad_pad.at[:, :, row_tap:row_tap + stride * height:stride, col_tap:col_tap + stride * width:stride].add(back)
    return (jnp.stack(tap_grads), grad_pad[:, :, 1:-1, 1:-1])

def reference(points, counts, cells, pfn_weight, pfn_gain, pfn_bias, conv_weight, bn_gain, bn_bias, cotangent):

    def hidden_of(args):
        return pillar_hidden(args[0][None], args[1][None], args[2][None], pfn_weight)

    def first_sums(args):
        hidden, is_valid = hidden_of(args)
        return (lax.optimization_barrier(jnp.sum(hidden * is_valid[:, None], axis=(0, 2, 3))), jnp.sum(is_valid))
    totals, counts_each = lax.map(first_sums, (points, counts, cells))
    count_all = jnp.sum(counts_each)
    mean_val = lax.optimization_barrier(jnp.sum(totals, axis=0)) / count_all

    def second_sums(args):
        hidden, is_valid = hidden_of(args)
        centred = hidden - channel_shape(mean_val, 4)
        return lax.optimization_barrier(jnp.sum(centred * centred * is_valid[:, None], axis=(0, 2, 3)))
    variance = lax.optimization_barrier(jnp.sum(lax.map(second_sums, (points, counts, cells)), axis=0)) / count_all
    inv_std = lax.rsqrt(variance + EPS)

    def to_grid(args):
        hidden, is_valid = hidden_of(args)
        pillar = normalize_pillars(hidden, is_valid, mean_val, inv_std, pfn_gain, pfn_bias)
        return scatter_pillars(pillar, args[2][None])[0]
    bev_grid = lax.map(to_grid, (points, counts, cells))
    activations = [bev_grid]
    normals = []
    for layer_idx in range(LAYERS):
        stride = 2 if layer_idx == 0 else 1
        weight = conv_weight[layer_idx]
        pre_norm = lax.map(lambda sweep: conv_forward(sweep[None], weight, stride)[0], activations[-1])
        mean_c = lax.optimization_barrier(jnp.mean(pre_norm, axis=(0, 2, 3)))
        centred = pre_norm - channel_shape(mean_c, 4)
        inv_c = lax.rsqrt(lax.optimization_barrier(jnp.mean(centred * centred, axis=(0, 2, 3))) + EPS)
        normed = centred * channel_shape(inv_c, 4)
        scaled = channel_shape(bn_gain[layer_idx], 4) * normed + channel_shape(bn_bias[layer_idx], 4)
        activations.append(jax.nn.silu(scaled))
        normals.append((normed, inv_c, scaled))
    upstream = cotangent
    grad_list = [None] * LAYERS
    gain_list = [None] * LAYERS
    bias_list = [None] * LAYERS
    pillar_grad = None
    for layer_idx in range(LAYERS - 1, -1, -1):
        stride = 2 if layer_idx == 0 else 1
        weight = conv_weight[layer_idx]
        normed, inv_c, scaled = normals[layer_idx]
        grad_y = upstream * silu_slope(scaled)
        sum_dy = lax.optimization_barrier(jnp.sum(grad_y, axis=(0, 2, 3)))
        sum_dyx = lax.optimization_barrier(jnp.sum(grad_y * normed, axis=(0, 2, 3)))
        entries = float(grad_y.shape[0] * grad_y.shape[2] * grad_y.shape[3])
        grad_z = channel_shape(bn_gain[layer_idx] * inv_c, 4) * (grad_y - channel_shape(sum_dy / entries, 4) - normed * channel_shape(sum_dyx / entries, 4))
        if layer_idx == 0:

            def back_first(args):
                grad_w, grad_in = conv_backward(args[0][None], weight, args[1][None], stride)
                plane = grad_in[0].reshape(grad_in.shape[1], GH * GW)
                return (grad_w, plane[:, args[2]])
            parts, pillar_grad = lax.map(back_first, (activations[0], grad_z, cells))
        else:

            def back_other(args):
                grad_w, grad_in = conv_backward(args[0][None], weight, args[1][None], stride)
                return (grad_w, grad_in[0])
            parts, upstream = lax.map(back_other, (activations[layer_idx], grad_z))
        grad_list[layer_idx] = lax.optimization_barrier(jnp.sum(parts, axis=0))
        gain_list[layer_idx] = sum_dyx
        bias_list[layer_idx] = sum_dy
    norm_grads = jnp.stack([jnp.stack(gain_list), jnp.stack(bias_list)])
    return (activations[-1], jnp.stack(grad_list), norm_grads, pillar_grad)
```

```python
import functools

import jax
import jax.numpy as jnp
from jax import lax
from jax.experimental import pallas as pl
from jax.experimental.pallas import tpu as pltpu
from jax.sharding import Mesh
from jax.sharding import PartitionSpec as P

C = 64
MAXP = 32
LAYERS = 4
GH = 8
GW = 256
PILL = 256
NS = 2
OH = GH // 2
OW = GW // 2
POS = OH * OW
NPOS = NS * POS
PADW = (OH + 2) * OW
EPS = 1e-05
F32 = jnp.float32
BF16 = jnp.bfloat16
ALL = ("x", "k", "y", "z")
WIDE = ("x", "y", "z")
INTERPRET = False


def split(v):
    hi = v.astype(BF16)
    return hi, (v - hi.astype(F32)).astype(BF16)


def dot_nn(a, b):
    return lax.dot_general(a, b, (((1,), (0,)), ((), ())), preferred_element_type=F32)


def dot_nt(a, b):
    return lax.dot_general(a, b, (((1,), (1,)), ((), ())), preferred_element_type=F32)


def dot3(dot, a_hi, a_lo, b_hi, b_lo):
    m = a_hi.shape[0]
    both = dot(jnp.concatenate([a_hi, a_lo], axis=0), b_hi)
    return both[:m] + both[m:] + dot(a_hi, b_lo)


def columns(row):
    return jnp.transpose(jnp.broadcast_to(row, (128, 128)))


def to_row(top, bottom):
    return jnp.sum(jnp.transpose(jnp.concatenate([top, bottom], axis=0)), axis=0, keepdims=True)


def lanes128():
    return lax.broadcasted_iota(jnp.int32, (C, 128), 1)


def from_left(v, lane):
    return jnp.where(lane == 0, 0.0, pltpu.roll(v, 1, 1))


def from_right(v, lane):
    return jnp.where(lane == 127, 0.0, pltpu.roll(v, 127, 1))


def put(hi_ref, lo_ref, row, col, v):
    hi, lo = split(v)
    hi_ref[pl.ds(row, C), pl.ds(col, 128)] = hi
    lo_ref[pl.ds(row, C), pl.ds(col, 128)] = lo


def put_shifted(hi_ref, lo_ref, n, r, v, lane):
    col = n * PADW + (r + 1) * OW
    put(hi_ref, lo_ref, 0, col, from_left(v, lane))
    put(hi_ref, lo_ref, C, col, v)
    put(hi_ref, lo_ref, 2 * C, col, from_right(v, lane))


def zero_borders(refs):
    for ref in refs:
        for n in range(NS):
            for r in (0, OH + 1):
                ref[:, pl.ds(n * PADW + r * OW, OW)] = jnp.zeros((3 * C, OW), BF16)


def conv_padded(w, hi_ref, lo_ref, n):
    w_hi, w_lo = split(w)
    cols = pl.ds(n * PADW, PADW)
    p = dot3(dot_nn, w_hi, w_lo, hi_ref[:, cols], lo_ref[:, cols])
    return p[:C, :POS] + p[C : 2 * C, OW : OW + POS] + p[2 * C :, 2 * OW : 2 * OW + POS]


def store_stats(z_ref, part_ref):
    acc = z_ref[:, pl.ds(0, 128)]
    for t in range(1, NPOS // 128):
        acc = acc + z_ref[:, pl.ds(t * 128, 128)]
    mean = jnp.sum(acc, axis=1, keepdims=True) * (1.0 / NPOS)
    sq = jnp.zeros((C, 128), F32)
    for t in range(NPOS // 128):
        d = z_ref[:, pl.ds(t * 128, 128)] - mean
        sq = sq + d * d
    lane = lax.broadcasted_iota(jnp.int32, (1, 128), 1)
    part_ref[...] = to_row(acc, sq) * jnp.where(lane < C, 1.0 / NPOS, 1.0)


def gathered_stats(g_ref):
    g = g_ref[...]
    rows = g.shape[0]
    total = jnp.sum(g, axis=0, keepdims=True)
    mean = total * (1.0 / rows)
    dev = g - mean
    spread = jnp.sum(dev * dev, axis=0, keepdims=True)
    each = 2.0 * NPOS
    var = (total + each * pltpu.roll(jnp.broadcast_to(spread, (8, 128)), C, 1)[:1]) * (1.0 / (each * rows))
    lane = lax.broadcasted_iota(jnp.int32, (1, 128), 1)
    return jnp.where(lane < C, mean, lax.rsqrt(var + EPS))


def pfn_kernel(pts_ref, cnt_ref, cell_ref, w_ref, hmax_ref, part_ref, base_ref):
    def col(j):
        return w_ref[:, pl.ds(j, 1)]

    wx = col(0) + col(4) + col(7)
    wy = col(1) + col(5) + col(8)
    wz = col(2) + col(6)
    wr = col(3)
    slot = lax.broadcasted_iota(jnp.int32, (MAXP, PILL), 0)
    total = jnp.zeros((C, 1), F32)
    number = jnp.zeros((1, 1), F32)
    for n in range(NS):
        count_i = cnt_ref[pl.ds(n, 1), :]
        count = count_i.astype(F32)
        valid = slot < count_i
        sums = []
        for j in range(4):
            p = pts_ref[pl.ds((n * 4 + j) * MAXP, MAXP), :]
            sums.append(jnp.sum(jnp.where(valid, p, 0.0), axis=0, keepdims=True))
        cell = cell_ref[pl.ds(n, 1), :]
        col_pos = jnp.bitwise_and(cell, GW - 1).astype(F32) * (2.0 / GW) - 1.0
        row_pos = jnp.right_shift(cell, 8).astype(F32) * (2.0 / GH) - 1.0
        base = -(
            col(4) * (sums[0] / count)
            + col(5) * (sums[1] / count)
            + col(6) * (sums[2] / count)
            + col(7) * col_pos
            + col(8) * row_pos
        )
        base_ref[:, pl.ds(n * PILL, PILL)] = base
        weighted = wx * sums[0] + wy * sums[1] + wz * sums[2] + wr * sums[3] + base * count
        total = total + jnp.sum(weighted, axis=1, keepdims=True)
        number = number + jnp.sum(count, axis=1, keepdims=True)
    mean = total / number
    sq_parts = []
    half = C // 2
    for c0 in (0, half):
        ch = slice(c0, c0 + half)
        bx = jnp.broadcast_to(wx[ch], (half, 128))
        by = jnp.broadcast_to(wy[ch], (half, 128))
        bz = jnp.broadcast_to(wz[ch], (half, 128))
        br = jnp.broadcast_to(wr[ch], (half, 128))
        mb = jnp.broadcast_to(mean[ch], (half, 128))
        sq = jnp.zeros((half, 128), F32)
        for n in range(NS):
            for q in range(PILL // 128):
                lanes = pl.ds(q * 128, 128)
                base = base_ref[pl.ds(c0, half), pl.ds(n * PILL + q * 128, 128)] - mb
                count = cnt_ref[pl.ds(n, 1), lanes]

                def step(k8, carry, n=n, lanes=lanes, base=base, count=count, bx=bx, by=by, bz=bz, br=br):
                    best, sq = carry
                    p = [
                        pts_ref[pl.ds(pl.multiple_of((n * 4 + j) * MAXP + k8 * 8, 8), 8), lanes]
                        for j in range(4)
                    ]
                    for i in range(8):
                        px, py, pz, pr = (v[i : i + 1] for v in p)
                        d = bx * px + by * py + (bz * pz + br * pr) + base
                        ok = jnp.broadcast_to(k8 * 8 + i < count, (half, 128))
                        best = jnp.where(ok, jnp.maximum(best, d), best)
                        sq = sq + jnp.where(ok, d * d, 0.0)
                    return best, sq

                start = jnp.full((half, 128), -3.0e38, F32)
                best, sq = lax.fori_loop(0, MAXP // 8, step, (start, sq))
                hmax_ref[pl.ds(c0, half), pl.ds(n * PILL + q * 128, 128)] = best + mb
        sq_parts.append(sq)
    lane = lanes128()
    part_ref[pl.ds(0, 1), :] = to_row(
        jnp.where(lane == 0, total, 0.0), jnp.concatenate(sq_parts, axis=0)
    )
    part_ref[pl.ds(1, 1), :] = jnp.broadcast_to(number, (1, 128))


def target_lane(cell):
    row = jnp.right_shift(cell, 8)
    col = jnp.bitwise_and(cell, GW - 1)
    phase = jnp.bitwise_and(row, 1) * 2 + jnp.bitwise_and(col, 1)
    return phase * POS + jnp.right_shift(row, 1) * OW + jnp.right_shift(col, 1)


def build_onehot(oht_ref, cell):
    target = jnp.broadcast_to(target_lane(cell), (256, PILL))
    iota = lax.broadcasted_iota(jnp.int32, (256, PILL), 0)
    for t in range(GH * GW // 256):
        oht_ref[pl.ds(t * 256, 256), :] = jnp.where(iota + t * 256 == target, 1.0, 0.0).astype(BF16)


def first_conv_kernel(
    g_ref, hmax_ref, cell_ref, gb_ref, w_ref,
    z_ref, part_ref, ev_hi, ev_lo, od_hi, od_lo,
    oht_ref, place_ref,
):
    rows = g_ref.shape[0] // 2
    s = g_ref[pl.ds(0, rows, stride=2), :]
    num = g_ref[pl.ds(1, rows, stride=2), :]
    total = jnp.sum(s, axis=0, keepdims=True)
    number = jnp.sum(num, axis=0, keepdims=True)
    mean = total / number
    dev = s / num - mean
    spread = jnp.sum(num * dev * dev, axis=0, keepdims=True)
    var = (total + pltpu.roll(jnp.broadcast_to(spread, (8, 128)), C, 1)[:1]) / number
    lane_row = lax.broadcasted_iota(jnp.int32, (1, 128), 1)
    stats = columns(jnp.where(lane_row < C, mean, lax.rsqrt(var + EPS)))
    mean_c, inv_c = stats[:C], stats[C:]
    gb = columns(gb_ref[...])
    gain, bias = gb[:C], gb[C:]
    lane = lanes128()
    w_hi, w_lo = split(w_ref[...])
    for n in range(NS):
        build_onehot(oht_ref, cell_ref[pl.ds(n, 1), :])
        tiles = []
        for q in range(PILL // 128):
            h = hmax_ref[:, pl.ds(n * PILL + q * 128, 128)]
            tiles.append(jnp.maximum(gain * (h - mean_c) * inv_c + bias, 0.0))
        p_hi, p_lo = split(jnp.concatenate(tiles, axis=1))
        place_ref[...] = dot_nt(jnp.concatenate([p_hi, p_lo], axis=0), oht_ref[...])
        for pr, refs in ((0, (ev_hi, ev_lo)), (1, (od_hi, od_lo))):
            for part, ref in enumerate(refs):
                width = POS + pr * OW
                if pr:
                    ref[:, pl.ds(n * width, OW)] = jnp.zeros((3 * C, OW), BF16)
                for r in range(OH):
                    even = place_ref[pl.ds(part * C, C), pl.ds(pr * 2 * POS + r * OW, OW)]
                    odd = place_ref[pl.ds(part * C, C), pl.ds((pr * 2 + 1) * POS + r * OW, OW)]
                    at = pl.ds(n * width + (r + pr) * OW, OW)
                    ref[pl.ds(0, C), at] = from_left(odd, lane).astype(BF16)
                    ref[pl.ds(C, C), at] = even.astype(BF16)
                    ref[pl.ds(2 * C, C), at] = odd.astype(BF16)
        at = pl.ds(n * POS, POS)
        z = dot3(dot_nn, w_hi[C : 2 * C], w_lo[C : 2 * C], ev_hi[:, at], ev_lo[:, at])
        at = pl.ds(n * (POS + OW), POS + OW)
        outer_hi = jnp.concatenate([w_hi[:C], w_hi[2 * C :]], axis=0)
        outer_lo = jnp.concatenate([w_lo[:C], w_lo[2 * C :]], axis=0)
        p = dot3(dot_nn, outer_hi, outer_lo, od_hi[:, at], od_lo[:, at])
        z_ref[:, pl.ds(n * POS, POS)] = z + p[:C, :POS] + p[C:, OW:]
    store_stats(z_ref, part_ref)


def conv_kernel(g_ref, z_ref, gb_ref, w_ref, out_ref, part_ref, stats_ref, s_hi, s_lo):
    stats = columns(gathered_stats(g_ref))
    stats_ref[...] = stats
    mean, inv = stats[:C], stats[C:]
    gb = columns(gb_ref[...])
    gain, bias = gb[:C], gb[C:]
    lane = lanes128()
    zero_borders((s_hi, s_lo))
    for n in range(NS):
        for r in range(OH):
            z = z_ref[:, pl.ds(n * POS + r * OW, OW)]
            y = gain * ((z - mean) * inv) + bias
            put_shifted(s_hi, s_lo, n, r, y * jax.nn.sigmoid(y), lane)
    w = w_ref[...]
    for n in range(NS):
        out_ref[:, pl.ds(n * POS, POS)] = conv_padded(w, s_hi, s_lo, n)
    store_stats(out_ref, part_ref)


def turn_kernel(g_ref, z_ref, gb_ref, ct_ref, feat_ref, gy_ref, part_ref, stats_ref):
    stats = columns(gathered_stats(g_ref))
    stats_ref[...] = stats
    mean, inv = stats[:C], stats[C:]
    gb = columns(gb_ref[...])
    gain, bias = gb[:C], gb[C:]
    dy = jnp.zeros((C, 128), F32)
    dx = jnp.zeros((C, 128), F32)
    for n in range(NS):
        for r in range(OH):
            at = pl.ds(n * POS + r * OW, OW)
            rows = pl.ds(n * C * OH + r, C, stride=OH)
            xhat = (z_ref[:, at] - mean) * inv
            y = gain * xhat + bias
            sg = jax.nn.sigmoid(y)
            feat_ref[rows, :] = y * sg
            gy = ct_ref[rows, :] * (sg * (1.0 + y * (1.0 - sg)))
            gy_ref[:, at] = gy
            dy = dy + gy
            dx = dx + gy * xhat
    part_ref[...] = to_row(dy, dx)


def grad_scales(g_ref, stats, gain, sums_ref):
    total = jnp.sum(g_ref[...], axis=0, keepdims=True)
    sums_ref[...] = total
    entries = 2.0 * NPOS * g_ref.shape[0]
    t = columns(total * (1.0 / entries))
    return gain * stats[C:], t[:C], t[C:]


def store_kernel_grad(dw_ref, per_row):
    taps = [per_row[a][:, b * C : (b + 1) * C] for a in range(3) for b in range(3)]
    taps.append(jnp.zeros((C, C), F32))
    for p in range(5):
        dw_ref[pl.ds(p * C, C), :] = jnp.concatenate([taps[2 * p], taps[2 * p + 1]], axis=1)


def back_kernel(
    g_ref, z_ref, gy_ref, stats_ref, gb_ref, zp_ref, statsp_ref, gbp_ref, wb_ref,
    dw_ref, gyp_ref, part_ref, sums_ref,
    s_hi, s_lo, a_hi, a_lo, slope_ref,
):
    stats = stats_ref[...]
    mean, inv = stats[:C], stats[C:]
    gain = columns(gb_ref[...])[:C]
    scale, mean_dy, mean_dx = grad_scales(g_ref, stats, gain, sums_ref)
    statsp = statsp_ref[...]
    meanp, invp = statsp[:C], statsp[C:]
    gbp = columns(gbp_ref[...])
    gainp, biasp = gbp[:C], gbp[C:]
    lane = lanes128()
    zero_borders((s_hi, s_lo, a_hi, a_lo))
    for n in range(NS):
        for r in range(OH):
            at = pl.ds(n * POS + r * OW, OW)
            xhat = (z_ref[:, at] - mean) * inv
            gz = scale * (gy_ref[:, at] - mean_dy - xhat * mean_dx)
            put_shifted(s_hi, s_lo, n, r, gz, lane)
            y = gainp * ((zp_ref[:, at] - meanp) * invp) + biasp
            sg = jax.nn.sigmoid(y)
            slope_ref[:, at] = sg * (1.0 + y * (1.0 - sg))
            put_shifted(a_hi, a_lo, n, r, y * sg, lane)
    wb = wb_ref[...]
    dy = jnp.zeros((C, 128), F32)
    dx = jnp.zeros((C, 128), F32)
    for n in range(NS):
        u = conv_padded(wb, s_hi, s_lo, n)
        for r in range(OH):
            at = pl.ds(n * POS + r * OW, OW)
            gy = u[:, r * OW : (r + 1) * OW] * slope_ref[:, at]
            gyp_ref[:, at] = gy
            dy = dy + gy
            dx = dx + gy * ((zp_ref[:, at] - meanp) * invp)
    part_ref[...] = to_row(dy, dx)
    rows = []
    for a in range(3):
        acc = jnp.zeros((C, 3 * C), F32)
        for n in range(NS):
            g_at = pl.ds(n * PADW + OW, POS)
            a_at = pl.ds(n * PADW + a * OW, POS)
            acc = acc + dot3(
                dot_nt, s_hi[pl.ds(C, C), g_at], s_lo[pl.ds(C, C), g_at], a_hi[:, a_at], a_lo[:, a_at]
            )
        rows.append(acc)
    store_kernel_grad(dw_ref, rows)


def last_back_kernel(
    g_ref, z_ref, gy_ref, stats_ref, gb_ref, cell_ref, v_ref, ev_hi, ev_lo, od_hi, od_lo,
    dw_ref, pg_ref, sums_ref,
    t_hi, t_lo, u_hi, oht_ref,
):
    stats = stats_ref[...]
    mean, inv = stats[:C], stats[C:]
    gain = columns(gb_ref[...])[:C]
    scale, mean_dy, mean_dx = grad_scales(g_ref, stats, gain, sums_ref)
    lane = lanes128()
    v_hi, v_lo = split(v_ref[...])
    width = POS + OW
    rows = [jnp.zeros((C, 3 * C), F32) for _ in range(3)]
    for n in range(NS):
        for ref in (t_hi, t_lo):
            ref[:, pl.ds(POS, OW)] = jnp.zeros((2 * C, OW), BF16)
        for r in range(OH):
            at = pl.ds(n * POS + r * OW, OW)
            xhat = (z_ref[:, at] - mean) * inv
            gz = scale * (gy_ref[:, at] - mean_dy - xhat * mean_dx)
            put(t_hi, t_lo, 0, r * OW, gz)
            put(t_hi, t_lo, C, r * OW, from_right(gz, lane))
        g_hi, g_lo = t_hi[pl.ds(0, C), pl.ds(0, POS)], t_lo[pl.ds(0, C), pl.ds(0, POS)]
        at = pl.ds(n * POS, POS)
        rows[1] = rows[1] + dot3(dot_nt, g_hi, g_lo, ev_hi[:, at], ev_lo[:, at])
        for a, first in ((0, 0), (2, OW)):
            at = pl.ds(n * width + first, POS)
            rows[a] = rows[a] + dot3(dot_nt, g_hi, g_lo, od_hi[:, at], od_lo[:, at])
        v = dot3(dot_nn, v_hi, v_lo, t_hi[...], t_lo[...])
        for pc in range(2):
            above = v[pc * C : (pc + 1) * C, OW:]
            here = v[(2 + pc) * C : (3 + pc) * C, :POS]
            below = v[(4 + pc) * C : (5 + pc) * C, :POS]
            for pr, u in ((0, here), (1, below + above)):
                at = pl.ds((pr * 2 + pc) * POS, POS)
                hi, lo = split(u)
                u_hi[pl.ds(0, C), at] = hi
                u_hi[pl.ds(C, C), at] = lo
        build_onehot(oht_ref, cell_ref[pl.ds(n, 1), :])
        picked = dot_nn(u_hi[...], oht_ref[...])
        pg_ref[pl.ds(n * C, C), :] = picked[:C] + picked[C:]
    store_kernel_grad(dw_ref, rows)


def call(kernel, name, outs, args, scratch=()):
    return pl.pallas_call(
        kernel,
        name=name,
        out_shape=tuple(jax.ShapeDtypeStruct(shape, dtype) for shape, dtype in outs),
        scratch_shapes=[pltpu.VMEM(shape, dtype) for shape, dtype in scratch],
        interpret=INTERPRET,
    )(*args)


def exchange_all(rows, sizes):
    r = rows.shape[0]
    peers = sizes["x"] * sizes["y"] * sizes["z"]
    sent = jnp.broadcast_to(rows[None], (peers, r, 128)).reshape(peers * r, 128)
    return lax.all_to_all(sent, WIDE, 0, 0, tiled=True)


def partner(v):
    return lax.ppermute(v, "k", [(0, 1), (1, 0)])


def share_sums(part, sizes):
    return exchange_all(part + partner(part), sizes)


def share_stats(part, sizes):
    other = partner(part)
    lane = lax.broadcasted_iota(jnp.int32, (1, 128), 1)
    gap = part - other
    gap_sq = jnp.concatenate([gap[:, C:], (gap * gap)[:, :C]], axis=1)
    both = part + other
    joined = jnp.where(lane < C, 0.5 * both, both + (0.5 * NPOS) * gap_sq)
    return exchange_all(joined, sizes)


def share_pillar_stats(part, sizes):
    other = partner(part)
    lane = lax.broadcasted_iota(jnp.int32, (1, 128), 1)
    both = part + other
    gap = part[:1] / part[1:] - other[:1] / other[1:]
    gap_sq = jnp.concatenate([gap[:, C:], (gap * gap)[:, :C]], axis=1)
    weight = part[1:] * other[1:] / both[1:]
    first = jnp.where(lane < C, both[:1], both[:1] + weight * gap_sq)
    return exchange_all(jnp.concatenate([first, both[1:]], axis=0), sizes)


def reduce_kernel_grads(grads, sizes):
    rack, chip = ("x", "k"), ("y", "z")
    n_rack, n_chip = sizes["x"] * sizes["k"], sizes["y"] * sizes["z"]
    rows = grads.shape[0]
    piece = rows // n_rack
    tiny = piece // n_chip
    got = lax.all_to_all(grads.reshape(n_rack, piece, 128), rack, 0, 0, tiled=True)
    part = jnp.sum(got, axis=0)
    got = lax.all_to_all(part.reshape(n_chip, tiny, 128), chip, 0, 0, tiled=True)
    mine = jnp.sum(got, axis=0)
    sent = jnp.broadcast_to(mine[None], (n_chip, tiny, 128))
    got = lax.all_to_all(sent, chip, 0, 0, tiled=True)
    sent = jnp.broadcast_to(got.reshape(1, piece, 128), (n_rack, piece, 128))
    return lax.all_to_all(sent, rack, 0, 0, tiled=True).reshape(rows, 128)


def per_device(
    points, counts, cells, pfn_weight, pfn_gain, pfn_bias, conv_weight, bn_gain, bn_bias, cotangent,
    *, sizes,
):
    w = conv_weight.reshape(LAYERS, 3, 3, C, C)
    w_fwd = jnp.transpose(w, (0, 1, 3, 2, 4)).reshape(LAYERS, 3 * C, 3 * C)
    w_bwd = jnp.transpose(w[1:, ::-1, ::-1], (0, 1, 4, 2, 3)).reshape(LAYERS - 1, 3 * C, 3 * C)
    w0 = jnp.transpose(w[0], (0, 1, 3, 2))
    even = jnp.concatenate([w0[:, 1], jnp.zeros((3, C, C), F32)], axis=2)
    odd = jnp.concatenate([w0[:, 2], w0[:, 0]], axis=2)
    v0 = jnp.stack([even, odd], axis=1).reshape(6 * C, 2 * C)
    gb = jnp.concatenate([bn_gain, bn_bias], axis=1)
    gbs = [gb[l : l + 1] for l in range(LAYERS)]
    pfn_gb = jnp.concatenate([pfn_gain, pfn_bias])[None]
    row = ((1, 128), F32)
    tile = ((128, 128), F32)
    plane = ((C, NPOS), F32)
    pad = ((3 * C, NS * PADW), BF16)

    hmax, part = call(
        pfn_kernel, "pfn", [((C, NS * PILL), F32), ((2, 128), F32)],
        (points.reshape(NS * 4 * MAXP, PILL), counts, cells, pfn_weight.T),
        [((C, NS * PILL), F32)],
    )
    got = share_pillar_stats(part, sizes)
    ev = ((3 * C, NS * POS), BF16)
    od = ((3 * C, NS * (POS + OW)), BF16)
    z, part, *grid0 = call(
        first_conv_kernel, "conv0", [plane, row, ev, ev, od, od],
        (got, hmax, cells, pfn_gb, w_fwd[0]),
        [((GH * GW, PILL), BF16), ((2 * C, GH * GW), F32)],
    )
    pre = [z]
    stats = []
    for l in range(1, LAYERS):
        got = share_stats(part, sizes)
        z, part, st = call(
            conv_kernel, f"conv{l}", [plane, row, tile],
            (got, pre[-1], gbs[l - 1], w_fwd[l]), [pad, pad],
        )
        pre.append(z)
        stats.append(st)
    got = share_stats(part, sizes)
    slab = ((NS * C * OH, OW), F32)
    feat, gy, part, st = call(
        turn_kernel, "turn", [slab, plane, row, tile],
        (got, pre[-1], gbs[-1], cotangent.reshape(NS * C * OH, OW)),
    )
    stats.append(st)
    dw_shape = ((5 * C, 128), F32)
    grads = [None] * LAYERS
    sums = [None] * LAYERS
    for l in range(LAYERS - 1, 0, -1):
        got = share_sums(part, sizes)
        grads[l], gy, part, sums[l] = call(
            back_kernel, f"back{l}", [dw_shape, plane, row, row],
            (got, pre[l], gy, stats[l], gbs[l], pre[l - 1], stats[l - 1], gbs[l - 1], w_bwd[l - 1]),
            [pad, pad, pad, pad, plane],
        )
    got = share_sums(part, sizes)
    tbuf = ((2 * C, POS + OW), BF16)
    grads[0], pillar_grad, sums[0] = call(
        last_back_kernel, "back0", [dw_shape, ((NS * C, PILL), F32), row],
        (got, pre[0], gy, stats[0], gbs[0], cells, v0, *grid0),
        [tbuf, tbuf, ((2 * C, GH * GW), BF16), ((GH * GW, PILL), BF16)],
    )
    total = reduce_kernel_grads(jnp.concatenate(grads, axis=0), sizes)
    total = total.reshape(LAYERS, 5, C, 2, C)
    total = jnp.transpose(total, (0, 1, 3, 2, 4)).reshape(LAYERS, 10, C * C)[:, :9]
    both = jnp.concatenate(sums, axis=0)
    norm_grads = jnp.stack([both[:, C:], both[:, :C]])
    return (
        feat.reshape(NS, C, OH, OW),
        total,
        norm_grads,
        pillar_grad.reshape(NS, C, PILL),
    )


def build(finer):
    sizes = dict(finer.shape)
    split4 = P(ALL, None, None, None)
    return jax.shard_map(
        functools.partial(per_device, sizes=sizes),
        mesh=finer,
        in_specs=(split4, P(ALL, None), P(ALL, None), P(), P(), P(), P(), P(), P(), split4),
        out_specs=(split4, P(), P(), P(ALL, None, None)),
        check_vma=False,
    )


def solution(mesh):
    return build(Mesh(mesh.devices.reshape(4, 2, 4, 8), ALL))
```

```python
import functools

import jax
import jax.numpy as jnp
from jax import lax
from jax.experimental import pallas as pl
from jax.experimental.pallas import tpu as pltpu
from jax.sharding import Mesh
from jax.sharding import PartitionSpec as P

C = 64
MAXP = 32
LAYERS = 4
GH = 8
GW = 256
PILL = 256
NS = 2
TAP_ROWS = C * C // 128
HALF = 256
OH = GH // 2
OW = GW // 2
POS = OH * OW
NPOS = NS * POS
PADW = (OH + 2) * OW
EPS = 1e-05
F32 = jnp.float32
BF16 = jnp.bfloat16
ALL = ("x", "k", "y", "z")
WIDE = ("x", "y", "z")
INTERPRET = False


def split(v):
    hi = v.astype(BF16)
    return hi, (v - hi.astype(F32)).astype(BF16)


def dot_nn(a, b):
    return lax.dot_general(a, b, (((1,), (0,)), ((), ())), preferred_element_type=F32)


def dot_nt(a, b):
    return lax.dot_general(a, b, (((1,), (1,)), ((), ())), preferred_element_type=F32)


def dot3(dot, a_hi, a_lo, b_hi, b_lo):
    m = a_hi.shape[0]
    both = dot(jnp.concatenate([a_hi, a_lo], axis=0), b_hi)
    return both[:m] + both[m:] + dot(a_hi, b_lo)


def columns(row):
    return jnp.transpose(jnp.broadcast_to(row, (128, 128)))


def to_row(top, bottom):
    return jnp.sum(jnp.transpose(jnp.concatenate([top, bottom], axis=0)), axis=0, keepdims=True)


def lanes128():
    return lax.broadcasted_iota(jnp.int32, (C, 128), 1)


def from_left(v, lane):
    return jnp.where(lane == 0, 0.0, pltpu.roll(v, 1, 1))


def from_right(v, lane):
    return jnp.where(lane == 127, 0.0, pltpu.roll(v, 127, 1))


def put(hi_ref, lo_ref, row, col, v):
    hi, lo = split(v)
    hi_ref[pl.ds(row, C), pl.ds(col, 128)] = hi
    lo_ref[pl.ds(row, C), pl.ds(col, 128)] = lo


def put_shifted(hi_ref, lo_ref, n, r, v, lane):
    col = n * PADW + (r + 1) * OW
    put(hi_ref, lo_ref, 0, col, from_left(v, lane))
    put(hi_ref, lo_ref, C, col, v)
    put(hi_ref, lo_ref, 2 * C, col, from_right(v, lane))


def zero_borders(refs):
    for ref in refs:
        for n in range(NS):
            for r in (0, OH + 1):
                ref[:, pl.ds(n * PADW + r * OW, OW)] = jnp.zeros((3 * C, OW), BF16)


def conv_padded(w_hi, w_lo, hi_ref, lo_ref, n):
    cols = pl.ds(n * PADW, PADW)
    p = dot3(dot_nn, w_hi, w_lo, hi_ref[:, cols], lo_ref[:, cols])
    return p[:C, :POS] + p[C : 2 * C, OW : OW + POS] + p[2 * C :, 2 * OW : 2 * OW + POS]


def tap_block(w_ref, buf_ref, layer, tap):
    packed = w_ref[pl.ds(tap * TAP_ROWS * LAYERS + layer, TAP_ROWS, stride=LAYERS), :]
    buf_ref[pl.ds(0, TAP_ROWS, stride=2), :] = packed[:, :C]
    buf_ref[pl.ds(1, TAP_ROWS, stride=2), :] = packed[:, C:]
    return buf_ref[...]


def forward_weights(w_ref, buf_ref, layer):
    rows = []
    for a in range(3):
        rows.append(jnp.concatenate([tap_block(w_ref, buf_ref, layer, 3 * a + b) for b in range(3)], axis=1))
    return jnp.concatenate(rows, axis=0)


def backward_weights(w_ref, buf_ref, layer):
    rows = []
    for a in range(3):
        blocks = [jnp.transpose(tap_block(w_ref, buf_ref, layer, 3 * (2 - a) + 2 - b)) for b in range(3)]
        rows.append(jnp.concatenate(blocks, axis=1))
    return jnp.concatenate(rows, axis=0)


def first_backward_weights(w_ref, buf_ref):
    rows = []
    for a in range(3):
        left, mid, right = (jnp.transpose(tap_block(w_ref, buf_ref, 0, 3 * a + b)) for b in range(3))
        rows.append(jnp.concatenate([mid, jnp.zeros((C, C), F32)], axis=1))
        rows.append(jnp.concatenate([right, left], axis=1))
    return jnp.concatenate(rows, axis=0)


def gain_bias(gain_ref, bias_ref, layer):
    at = pl.ds(layer, 1)
    gb = columns(jnp.concatenate([gain_ref[at, :], bias_ref[at, :]], axis=1))
    return gb[:C], gb[C:]


def store_kernel_grad(refs, k_ref, slot, per_row, buf_ref):
    keep_ref, send_ref = refs
    first = k_ref[0] == 0

    def packed(tap):
        a, b = divmod(tap, 3)
        buf_ref[...] = per_row[a][:, b * C : (b + 1) * C]
        even = buf_ref[pl.ds(0, TAP_ROWS, stride=2), :]
        odd = buf_ref[pl.ds(1, TAP_ROWS, stride=2), :]
        return jnp.concatenate([even, odd], axis=1)

    last = packed(8)
    for tap in range(8):
        rows = packed(tap)
        other = last if tap == 0 else jnp.zeros((TAP_ROWS, 128), F32)
        at = pl.ds(8 + slot * HALF + tap * TAP_ROWS, TAP_ROWS)
        keep_ref[at, :] = jnp.where(first, rows, other)
        send_ref[at, :] = jnp.where(first, other, rows)


def rows_of(g_ref, stride, index):
    peers = g_ref.shape[0] // stride
    if stride == 1:
        return g_ref[...]
    return g_ref[pl.ds(index, peers, stride=stride), :]


def reduced_rows(g_ref, stride, red_ref, count):
    for j in range(count):
        red_ref[pl.ds(j, 1), :] = jnp.sum(rows_of(g_ref, stride, 1 + j), axis=0, keepdims=True)


def store_stats(z_ref, part_ref):
    acc = z_ref[:, pl.ds(0, 128)]
    for t in range(1, NPOS // 128):
        acc = acc + z_ref[:, pl.ds(t * 128, 128)]
    mean = jnp.sum(acc, axis=1, keepdims=True) * (1.0 / NPOS)
    sq = jnp.zeros((C, 128), F32)
    for t in range(NPOS // 128):
        d = z_ref[:, pl.ds(t * 128, 128)] - mean
        sq = sq + d * d
    lane = lax.broadcasted_iota(jnp.int32, (1, 128), 1)
    part_ref[pl.ds(0, 1), :] = to_row(acc, sq) * jnp.where(lane < C, 1.0 / NPOS, 1.0)


def gathered_stats(g):
    rows = g.shape[0]
    total = jnp.sum(g, axis=0, keepdims=True)
    mean = total * (1.0 / rows)
    dev = g - mean
    spread = jnp.sum(dev * dev, axis=0, keepdims=True)
    each = 2.0 * NPOS
    var = (total + each * pltpu.roll(jnp.broadcast_to(spread, (8, 128)), C, 1)[:1]) * (1.0 / (each * rows))
    lane = lax.broadcasted_iota(jnp.int32, (1, 128), 1)
    return jnp.where(lane < C, mean, lax.rsqrt(var + EPS))


def pfn_kernel(pts_ref, cnt_ref, cell_ref, w_ref, hmax_ref, part_ref, base_ref, w_pad):
    w_pad[...] = jnp.zeros((128, 128), F32)
    w_pad[pl.ds(0, 9), pl.ds(0, C)] = w_ref[...]
    w_cols = jnp.transpose(w_pad[...])

    def col(j):
        return w_cols[:C, j : j + 1]

    wx = col(0) + col(4) + col(7)
    wy = col(1) + col(5) + col(8)
    wz = col(2) + col(6)
    wr = col(3)
    slot = lax.broadcasted_iota(jnp.int32, (MAXP, PILL), 0)
    total = jnp.zeros((C, 1), F32)
    number = jnp.zeros((1, 1), F32)
    for n in range(NS):
        count_i = cnt_ref[pl.ds(n, 1), :]
        count = count_i.astype(F32)
        valid = slot < count_i
        sums = []
        for j in range(4):
            p = pts_ref[pl.ds((n * 4 + j) * MAXP, MAXP), :]
            sums.append(jnp.sum(jnp.where(valid, p, 0.0), axis=0, keepdims=True))
        cell = cell_ref[pl.ds(n, 1), :]
        col_pos = jnp.bitwise_and(cell, GW - 1).astype(F32) * (2.0 / GW) - 1.0
        row_pos = jnp.right_shift(cell, 8).astype(F32) * (2.0 / GH) - 1.0
        base = -(
            col(4) * (sums[0] / count)
            + col(5) * (sums[1] / count)
            + col(6) * (sums[2] / count)
            + col(7) * col_pos
            + col(8) * row_pos
        )
        base_ref[:, pl.ds(n * PILL, PILL)] = base
        weighted = wx * sums[0] + wy * sums[1] + wz * sums[2] + wr * sums[3] + base * count
        total = total + jnp.sum(weighted, axis=1, keepdims=True)
        number = number + jnp.sum(count, axis=1, keepdims=True)
    mean = total / number
    sq_parts = []
    half = C // 2
    for c0 in (0, half):
        ch = slice(c0, c0 + half)
        bx = jnp.broadcast_to(wx[ch], (half, 128))
        by = jnp.broadcast_to(wy[ch], (half, 128))
        bz = jnp.broadcast_to(wz[ch], (half, 128))
        br = jnp.broadcast_to(wr[ch], (half, 128))
        mb = jnp.broadcast_to(mean[ch], (half, 128))
        sq = jnp.zeros((half, 128), F32)
        for n in range(NS):
            for q in range(PILL // 128):
                lanes = pl.ds(q * 128, 128)
                base = base_ref[pl.ds(c0, half), pl.ds(n * PILL + q * 128, 128)] - mb
                count = cnt_ref[pl.ds(n, 1), lanes]

                def step(k8, carry, n=n, lanes=lanes, base=base, count=count, bx=bx, by=by, bz=bz, br=br):
                    best, sq = carry
                    p = [
                        pts_ref[pl.ds(pl.multiple_of((n * 4 + j) * MAXP + k8 * 8, 8), 8), lanes]
                        for j in range(4)
                    ]
                    for i in range(8):
                        px, py, pz, pr = (v[i : i + 1] for v in p)
                        d = bx * px + by * py + (bz * pz + br * pr) + base
                        ok = jnp.broadcast_to(k8 * 8 + i < count, (half, 128))
                        best = jnp.where(ok, jnp.maximum(best, d), best)
                        sq = sq + jnp.where(ok, d * d, 0.0)
                    return best, sq

                start = jnp.full((half, 128), -3.0e38, F32)
                best, sq = lax.fori_loop(0, MAXP // 8, step, (start, sq))
                hmax_ref[pl.ds(c0, half), pl.ds(n * PILL + q * 128, 128)] = best + mb
        sq_parts.append(sq)
    lane = lanes128()
    part_ref[pl.ds(0, 1), :] = to_row(
        jnp.where(lane == 0, total, 0.0), jnp.concatenate(sq_parts, axis=0)
    )
    part_ref[pl.ds(1, 1), :] = jnp.broadcast_to(number, (1, 128))


def target_lane(cell):
    row = jnp.right_shift(cell, 8)
    col = jnp.bitwise_and(cell, GW - 1)
    phase = jnp.bitwise_and(row, 1) * 2 + jnp.bitwise_and(col, 1)
    return phase * POS + jnp.right_shift(row, 1) * OW + jnp.right_shift(col, 1)


def build_onehot(oht_ref, cell):
    target = jnp.broadcast_to(target_lane(cell), (256, PILL))
    iota = lax.broadcasted_iota(jnp.int32, (256, PILL), 0)
    for t in range(GH * GW // 256):
        oht_ref[pl.ds(t * 256, 256), :] = jnp.where(iota + t * 256 == target, 1.0, 0.0).astype(BF16)


def first_conv_kernel(
    k_ref, g_ref, hmax_ref, cell_ref, gain_ref, bias_ref, w_ref,
    z_ref, part_ref, ev_hi, ev_lo, od_hi, od_lo, keep_ref, send_ref,
    oht_ref, place_ref, buf_ref,
):
    s = rows_of(g_ref, 2, 0)
    num = rows_of(g_ref, 2, 1)
    total = jnp.sum(s, axis=0, keepdims=True)
    number = jnp.sum(num, axis=0, keepdims=True)
    mean = total / number
    dev = s / num - mean
    spread = jnp.sum(num * dev * dev, axis=0, keepdims=True)
    var = (total + pltpu.roll(jnp.broadcast_to(spread, (8, 128)), C, 1)[:1]) / number
    lane_row = lax.broadcasted_iota(jnp.int32, (1, 128), 1)
    stats = columns(jnp.where(lane_row < C, mean, lax.rsqrt(var + EPS)))
    mean_c, inv_c = stats[:C], stats[C:]
    gain, bias = gain_bias(gain_ref, bias_ref, 0)
    lane = lanes128()
    w_hi, w_lo = split(forward_weights(w_ref, buf_ref, 0))
    for n in range(NS):
        build_onehot(oht_ref, cell_ref[pl.ds(n, 1), :])
        tiles = []
        for q in range(PILL // 128):
            h = hmax_ref[:, pl.ds(n * PILL + q * 128, 128)]
            tiles.append(jnp.maximum(gain * (h - mean_c) * inv_c + bias, 0.0))
        p_hi, p_lo = split(jnp.concatenate(tiles, axis=1))
        place_ref[...] = dot_nt(jnp.concatenate([p_hi, p_lo], axis=0), oht_ref[...])
        for pr, refs in ((0, (ev_hi, ev_lo)), (1, (od_hi, od_lo))):
            for part, ref in enumerate(refs):
                width = POS + pr * OW
                if pr:
                    ref[:, pl.ds(n * width, OW)] = jnp.zeros((3 * C, OW), BF16)
                for r in range(OH):
                    even = place_ref[pl.ds(part * C, C), pl.ds(pr * 2 * POS + r * OW, OW)]
                    odd = place_ref[pl.ds(part * C, C), pl.ds((pr * 2 + 1) * POS + r * OW, OW)]
                    at = pl.ds(n * width + (r + pr) * OW, OW)
                    ref[pl.ds(0, C), at] = from_left(odd, lane).astype(BF16)
                    ref[pl.ds(C, C), at] = even.astype(BF16)
                    ref[pl.ds(2 * C, C), at] = odd.astype(BF16)
        at = pl.ds(n * POS, POS)
        z = dot3(dot_nn, w_hi[C : 2 * C], w_lo[C : 2 * C], ev_hi[:, at], ev_lo[:, at])
        at = pl.ds(n * (POS + OW), POS + OW)
        outer_hi = jnp.concatenate([w_hi[:C], w_hi[2 * C :]], axis=0)
        outer_lo = jnp.concatenate([w_lo[:C], w_lo[2 * C :]], axis=0)
        p = dot3(dot_nn, outer_hi, outer_lo, od_hi[:, at], od_lo[:, at])
        z_ref[:, pl.ds(n * POS, POS)] = z + p[:C, :POS] + p[C:, OW:]
    store_stats(z_ref, part_ref)
    one = jnp.ones((C, POS), BF16)
    rows = first_grad_rows(lambda n: (one, None), (ev_hi, ev_lo, od_hi, od_lo))
    store_kernel_grad((keep_ref, send_ref), k_ref, 0, rows, buf_ref)


def first_grad_rows(grad_of, grid_refs):
    ev_hi, ev_lo, od_hi, od_lo = grid_refs
    rows = [jnp.zeros((C, 3 * C), F32) for _ in range(3)]
    for n in range(NS):
        g_hi, g_lo = grad_of(n)
        for a, hi, lo, start in (
            (0, od_hi, od_lo, n * (POS + OW)),
            (1, ev_hi, ev_lo, n * POS),
            (2, od_hi, od_lo, n * (POS + OW) + OW),
        ):
            at = pl.ds(start, POS)
            if g_lo is None:
                rows[a] = rows[a] + dot_nt(g_hi, hi[:, at]) + dot_nt(g_hi, lo[:, at])
            else:
                rows[a] = rows[a] + dot3(dot_nt, g_hi, g_lo, hi[:, at], lo[:, at])
    return rows


def conv_kernel(
    g_ref, z_ref, gain_ref, bias_ref, w_ref, out_ref, part_ref, stats_ref, s_hi, s_lo, buf_ref, *, layer
):
    stats = columns(gathered_stats(g_ref[...]))
    stats_ref[...] = stats
    mean, inv = stats[:C], stats[C:]
    gain, bias = gain_bias(gain_ref, bias_ref, layer - 1)
    lane = lanes128()
    zero_borders((s_hi, s_lo))
    for n in range(NS):
        for r in range(OH):
            z = z_ref[:, pl.ds(n * POS + r * OW, OW)]
            y = gain * ((z - mean) * inv) + bias
            put_shifted(s_hi, s_lo, n, r, y * jax.nn.sigmoid(y), lane)
    w_hi, w_lo = split(forward_weights(w_ref, buf_ref, layer))
    for n in range(NS):
        out_ref[:, pl.ds(n * POS, POS)] = conv_padded(w_hi, w_lo, s_hi, s_lo, n)
    store_stats(out_ref, part_ref)


def turn_kernel(
    k_ref, g_ref, z_ref, gain_ref, bias_ref, ct_ref, z0_ref, stats0_ref, ev_hi, ev_lo, od_hi, od_lo,
    feat_ref, gy_ref, keep_ref, send_ref, stats_ref, red_ref,
    buf_ref, *, stride,
):
    reduced_rows(g_ref, stride, red_ref, red_ref.shape[0])
    stats = columns(gathered_stats(rows_of(g_ref, stride, 0)))
    stats_ref[...] = stats
    mean, inv = stats[:C], stats[C:]
    gain, bias = gain_bias(gain_ref, bias_ref, LAYERS - 1)
    dy = jnp.zeros((C, 128), F32)
    dx = jnp.zeros((C, 128), F32)
    for n in range(NS):
        for r in range(OH):
            at = pl.ds(n * POS + r * OW, OW)
            rows = pl.ds(n * C * OH + r, C, stride=OH)
            xhat = (z_ref[:, at] - mean) * inv
            y = gain * xhat + bias
            sg = jax.nn.sigmoid(y)
            feat_ref[rows, :] = y * sg
            gy = ct_ref[rows, :] * (sg * (1.0 + y * (1.0 - sg)))
            gy_ref[:, at] = gy
            dy = dy + gy
            dx = dx + gy * xhat
    part = to_row(dy, dx)
    keep_ref[pl.ds(0, 1), :] = part
    send_ref[pl.ds(0, 1), :] = part
    mean0, inv0 = stats0_ref[pl.ds(0, C), pl.ds(0, 1)], stats0_ref[pl.ds(C, C), pl.ds(0, 1)]
    grads = first_grad_rows(
        lambda n: split((z0_ref[:, pl.ds(n * POS, POS)] - mean0) * inv0), (ev_hi, ev_lo, od_hi, od_lo)
    )
    store_kernel_grad((keep_ref, send_ref), k_ref, 0, grads, buf_ref)


def grad_scales(g, stats, gain, sums_ref):
    total = jnp.sum(g, axis=0, keepdims=True)
    sums_ref[...] = total
    entries = 2.0 * NPOS * g.shape[0]
    t = columns(total * (1.0 / entries))
    return gain * stats[C:], t[:C], t[C:]


def back_kernel(
    k_ref, g_ref, z_ref, gy_ref, stats_ref, gain_ref, bias_ref, zp_ref, statsp_ref, w_ref, *refs, layer, stride
):
    grid0 = ()
    if layer == 1:
        grid0, refs = refs[:4], refs[4:]
    gyp_ref, keep_ref, send_ref, sums_ref, red_ref, s_hi, s_lo, a_hi, a_lo, slope_ref, buf_ref = refs
    reduced_rows(g_ref, stride, red_ref, red_ref.shape[0])
    stats = stats_ref[...]
    mean, inv = stats[:C], stats[C:]
    gain, _ = gain_bias(gain_ref, bias_ref, layer)
    scale, mean_dy, mean_dx = grad_scales(rows_of(g_ref, stride, 0), stats, gain, sums_ref)
    statsp = statsp_ref[...]
    meanp, invp = statsp[:C], statsp[C:]
    gainp, biasp = gain_bias(gain_ref, bias_ref, layer - 1)
    lane = lanes128()
    zero_borders((s_hi, s_lo, a_hi, a_lo))
    for n in range(NS):
        for r in range(OH):
            at = pl.ds(n * POS + r * OW, OW)
            xhat = (z_ref[:, at] - mean) * inv
            gz = scale * (gy_ref[:, at] - mean_dy - xhat * mean_dx)
            put_shifted(s_hi, s_lo, n, r, gz, lane)
            y = gainp * ((zp_ref[:, at] - meanp) * invp) + biasp
            sg = jax.nn.sigmoid(y)
            slope_ref[:, at] = sg * (1.0 + y * (1.0 - sg))
            put_shifted(a_hi, a_lo, n, r, y * sg, lane)
    w_hi, w_lo = split(backward_weights(w_ref, buf_ref, layer))
    dy = jnp.zeros((C, 128), F32)
    dx = jnp.zeros((C, 128), F32)
    for n in range(NS):
        u = conv_padded(w_hi, w_lo, s_hi, s_lo, n)
        for r in range(OH):
            at = pl.ds(n * POS + r * OW, OW)
            gy = u[:, r * OW : (r + 1) * OW] * slope_ref[:, at]
            gyp_ref[:, at] = gy
            dy = dy + gy
            dx = dx + gy * ((zp_ref[:, at] - meanp) * invp)
    part = to_row(dy, dx)
    keep_ref[pl.ds(0, 1), :] = part
    send_ref[pl.ds(0, 1), :] = part
    rows = []
    for a in range(3):
        acc = jnp.zeros((C, 3 * C), F32)
        for n in range(NS):
            g_at = pl.ds(n * PADW + OW, POS)
            a_at = pl.ds(n * PADW + a * OW, POS)
            acc = acc + dot3(
                dot_nt, s_hi[pl.ds(C, C), g_at], s_lo[pl.ds(C, C), g_at], a_hi[:, a_at], a_lo[:, a_at]
            )
        rows.append(acc)
    store_kernel_grad((keep_ref, send_ref), k_ref, 0, rows, buf_ref)
    if layer == 1:
        rows = first_grad_rows(lambda n: split(gyp_ref[:, pl.ds(n * POS, POS)]), grid0)
        store_kernel_grad((keep_ref, send_ref), k_ref, 1, rows, buf_ref)


def pick_channels(tile, pair, lane):
    row = lax.broadcasted_iota(jnp.int32, (C, 128), 0)
    want = 2 * pair + jnp.where(lane < C, 0, 1)
    return jnp.sum(jnp.where(row == want, tile, 0.0), axis=0, keepdims=True)


def last_back_kernel(
    k_ref, g_ref, z_ref, gy_ref, stats_ref, gain_ref, bias_ref, cell_ref, w_ref,
    sum_red, xhat_red, red3, red2,
    pg_ref, sums_ref, own_ref,
    t_hi, t_lo, u_hi, oht_ref, buf_ref, *, stride,
):
    stats = stats_ref[...]
    mean, inv = stats[:C], stats[C:]
    gain, _ = gain_bias(gain_ref, bias_ref, 0)
    scale, mean_dy, mean_dx = grad_scales(rows_of(g_ref, stride, 0), stats, gain, sums_ref)
    lane = lanes128()
    count = sum_red.shape[0]
    peers = HALF // count
    for j in range(count):
        pair = lax.rem(j * peers + k_ref[1], TAP_ROWS)
        raw = jnp.sum(rows_of(g_ref, stride, 1 + count + j), axis=0, keepdims=True)
        own_ref[pl.ds(j, 1), :] = pick_channels(scale, pair, lane) * (
            raw
            - pick_channels(mean_dy, pair, lane) * sum_red[pl.ds(j, 1), :]
            - pick_channels(mean_dx, pair, lane) * xhat_red[pl.ds(j, 1), :]
        )
        own_ref[pl.ds(count + j, 1), :] = jnp.sum(rows_of(g_ref, stride, 1 + j), axis=0, keepdims=True)
        own_ref[pl.ds(2 * count + j, 1), :] = red2[pl.ds(j, 1), :]
        own_ref[pl.ds(3 * count + j, 1), :] = red3[pl.ds(j, 1), :]
    v_hi, v_lo = split(first_backward_weights(w_ref, buf_ref))
    for n in range(NS):
        for ref in (t_hi, t_lo):
            ref[:, pl.ds(POS, OW)] = jnp.zeros((2 * C, OW), BF16)
        for r in range(OH):
            at = pl.ds(n * POS + r * OW, OW)
            xhat = (z_ref[:, at] - mean) * inv
            gz = scale * (gy_ref[:, at] - mean_dy - xhat * mean_dx)
            put(t_hi, t_lo, 0, r * OW, gz)
            put(t_hi, t_lo, C, r * OW, from_right(gz, lane))
        v = dot3(dot_nn, v_hi, v_lo, t_hi[...], t_lo[...])
        for pc in range(2):
            above = v[pc * C : (pc + 1) * C, OW:]
            here = v[(2 + pc) * C : (3 + pc) * C, :POS]
            below = v[(4 + pc) * C : (5 + pc) * C, :POS]
            for pr, u in ((0, here), (1, below + above)):
                at = pl.ds((pr * 2 + pc) * POS, POS)
                hi, lo = split(u)
                u_hi[pl.ds(0, C), at] = hi
                u_hi[pl.ds(C, C), at] = lo
        build_onehot(oht_ref, cell_ref[pl.ds(n, 1), :])
        picked = dot_nn(u_hi[...], oht_ref[...])
        pg_ref[pl.ds(n * C, C), :] = picked[:C] + picked[C:]


def pair_kernel(keep_ref, got_ref, out_ref, *, mode, stride, count):
    peers = out_ref.shape[0] // stride
    mine, other = keep_ref[pl.ds(0, 1), :], got_ref[pl.ds(0, 1), :]
    both = mine + other
    lane = lax.broadcasted_iota(jnp.int32, (1, 128), 1)

    def swap(v):
        return pltpu.roll(jnp.broadcast_to(v, (8, 128)), C, 1)[:1]

    if mode == "stats":
        gap = mine - other
        both = jnp.where(lane < C, 0.5 * both, both + (0.5 * NPOS) * swap(gap * gap))
    if mode == "pillars":
        m_num, o_num = keep_ref[pl.ds(1, 1), :], got_ref[pl.ds(1, 1), :]
        number = m_num + o_num
        gap = mine / m_num - other / o_num
        both = jnp.where(lane < C, both, both + (m_num * o_num / number) * swap(gap * gap))
        out_ref[pl.ds(1, peers, stride=stride), :] = jnp.broadcast_to(number, (peers, 128))
    row = jnp.broadcast_to(both, (peers, 128))
    if stride == 1:
        out_ref[...] = row
    else:
        out_ref[pl.ds(0, peers, stride=stride), :] = row
    for j in range(count):
        at = pl.ds(8 + j * peers, peers)
        out_ref[pl.ds(1 + j, peers, stride=stride), :] = keep_ref[at, :] + got_ref[at, :]


def assemble_kernel(k_ref, mine_ref, theirs_ref, out_ref, *, peers):
    first = k_ref[0] == 0
    count = HALF // peers
    per_peer = LAYERS * count
    for l in range(LAYERS):
        for j in range(count):
            at = pl.ds(l * count + j, peers, stride=per_peer)
            rows = jnp.where(first, mine_ref[at, :], theirs_ref[at, :])
            out_ref[pl.ds(j * peers * LAYERS + l, peers, stride=LAYERS), :] = rows
        for start in range(0, TAP_ROWS, peers):
            size = min(peers, TAP_ROWS)
            at = pl.ds(l * count + start // peers, size, stride=per_peer)
            rows = jnp.where(first, theirs_ref[at, :], mine_ref[at, :])
            out_ref[pl.ds((HALF + start) * LAYERS + l, size, stride=LAYERS), :] = rows


def call(kernel, name, outs, args, scratch=(), scalar=False, **params):
    specs = [pl.BlockSpec(memory_space=pltpu.VMEM)] * len(args)
    if scalar:
        specs[0] = pl.BlockSpec(memory_space=pltpu.SMEM)
    return pl.pallas_call(
        functools.partial(kernel, **params) if params else kernel,
        name=name,
        out_shape=tuple(jax.ShapeDtypeStruct(shape, dtype) for shape, dtype in outs),
        in_specs=specs,
        scratch_shapes=[pltpu.VMEM(shape, dtype) for shape, dtype in scratch],
        compiler_params=pltpu.CompilerParams(vmem_limit_bytes=20 << 20),
        interpret=INTERPRET,
    )(*args)


def partner(v):
    return lax.ppermute(v, "k", [(0, 1), (1, 0)])


def to_peers(rows):
    return lax.all_to_all(rows, WIDE, 0, 0, tiled=True)


def exchange(name, mode, keep, send, peers, stride=1, count=0):
    got = partner(send)
    (out,) = call(
        pair_kernel, name, [((peers * stride, 128), F32)], (keep, got), mode=mode, stride=stride, count=count
    )
    return to_peers(out)


def per_device(
    points, counts, cells, pfn_weight, pfn_gain, pfn_bias, conv_weight, bn_gain, bn_bias, cotangent,
    *, sizes,
):
    peers = sizes["x"] * sizes["y"] * sizes["z"]
    count = HALF // peers
    place = jnp.stack([lax.axis_index("k"), lax.axis_index(WIDE)]).astype(jnp.int32)
    w = conv_weight.reshape(LAYERS, 9, TAP_ROWS, 128).transpose(1, 2, 0, 3).reshape(9 * TAP_ROWS * LAYERS, 128)
    row = ((1, 128), F32)
    rows8 = ((8, 128), F32)
    tile = ((128, 128), F32)
    plane = ((C, NPOS), F32)
    pad = ((3 * C, NS * PADW), BF16)
    buf = ((C, C), F32)
    red = ((count, 128), F32)
    one = ((8 + HALF, 128), F32)
    two = ((8 + 2 * HALF, 128), F32)
    stride1 = 1 << (1 + count - 1).bit_length()
    stride2 = 1 << (1 + 2 * count - 1).bit_length()

    hmax, part = call(
        pfn_kernel, "pfn", [((C, NS * PILL), F32), rows8],
        (points.reshape(NS * 4 * MAXP, PILL), counts, cells, pfn_weight),
        [((C, NS * PILL), F32), tile],
    )
    got = exchange("pair_p", "pillars", part, part, peers, 2)
    ev = ((3 * C, NS * POS), BF16)
    od = ((3 * C, NS * (POS + OW)), BF16)
    z, part, *grid0, keep, send = call(
        first_conv_kernel, "conv0", [plane, rows8, ev, ev, od, od, one, one],
        (place, got, hmax, cells, pfn_gain[None], pfn_bias[None], w),
        [((GH * GW, PILL), BF16), ((2 * C, GH * GW), F32), buf], scalar=True,
    )
    pre = [z]
    stats = []
    for l in range(1, LAYERS):
        got = exchange("pair_s", "stats", part, part, peers)
        z, part, st = call(
            conv_kernel, f"conv{l}", [plane, rows8, tile],
            (got, pre[-1], bn_gain, bn_bias, w), [pad, pad, buf], layer=l,
        )
        pre.append(z)
        stats.append(st)
    keep = jnp.concatenate([part, keep[8:]], axis=0)
    send = jnp.concatenate([part, send[8:]], axis=0)
    got = exchange("pair_t", "stats", keep, send, peers, stride1, count)
    slab = ((NS * C * OH, OW), F32)
    feat, gy, keep, send, st, sum_red = call(
        turn_kernel, "turn", [slab, plane, one, one, tile, red],
        (place, got, pre[-1], bn_gain, bn_bias, cotangent.reshape(NS * C * OH, OW), pre[0], stats[0], *grid0),
        [buf], scalar=True, stride=stride1,
    )
    stats.append(st)
    sums = [None] * LAYERS
    reds = [None] * LAYERS
    for l in range(LAYERS - 1, 0, -1):
        got = exchange("pair_g", "sums", keep, send, peers, stride1, count)
        shape = two if l == 1 else one
        gy, keep, send, sums[l], reds[l] = call(
            back_kernel, f"back{l}", [plane, shape, shape, row, red],
            (place, got, pre[l], gy, stats[l], bn_gain, bn_bias, pre[l - 1], stats[l - 1], w)
            + (tuple(grid0) if l == 1 else ()),
            [pad, pad, pad, pad, plane, buf], scalar=True, layer=l, stride=stride1,
        )
    got = exchange("pair_z", "sums", keep, send, peers, stride2, 2 * count)
    tbuf = ((2 * C, POS + OW), BF16)
    pillar_grad, sums[0], own = call(
        last_back_kernel, "back0", [((NS * C, PILL), F32), row, ((LAYERS * count, 128), F32)],
        (place, got, pre[0], gy, stats[0], bn_gain, bn_bias, cells, w, sum_red, reds[3], reds[2], reds[1]),
        [tbuf, tbuf, ((2 * C, GH * GW), BF16), ((GH * GW, PILL), BF16), buf], scalar=True, stride=stride2,
    )
    own = jnp.broadcast_to(own[None], (peers, LAYERS * count, 128)).reshape(peers * LAYERS * count, 128)
    mine = to_peers(own)
    (total,) = call(
        assemble_kernel, "assemble", [((9 * TAP_ROWS * LAYERS, 128), F32)], (place, mine, partner(mine)),
        scalar=True, peers=peers,
    )
    total = total.reshape(9, TAP_ROWS, LAYERS, 128).transpose(2, 0, 1, 3).reshape(LAYERS, 9, C * C)
    both = jnp.concatenate(sums, axis=0)
    norm_grads = jnp.stack([both[:, C:], both[:, :C]])
    return (
        feat.reshape(NS, C, OH, OW),
        total,
        norm_grads,
        pillar_grad.reshape(NS, C, PILL),
    )


def build(finer):
    sizes = dict(finer.shape)
    split4 = P(ALL, None, None, None)
    return jax.shard_map(
        functools.partial(per_device, sizes=sizes),
        mesh=finer,
        in_specs=(split4, P(ALL, None), P(ALL, None), P(), P(), P(), P(), P(), P(), split4),
        out_specs=(split4, P(), P(), P(ALL, None, None)),
        check_vma=False,
    )


def solution(mesh):
    return build(Mesh(mesh.devices.reshape(4, 2, 4, 8), ALL))
```

```python
import functools

import jax
import jax.numpy as jnp
from jax import lax
from jax.experimental import pallas as pl
from jax.experimental.pallas import tpu as pltpu
from jax.sharding import Mesh
from jax.sharding import PartitionSpec as P

C = 64
MAXP = 32
LAYERS = 4
GH = 8
GW = 256
PILL = 256
NS = 2
TAP_ROWS = C * C // 128
BLOCK = 4 * TAP_ROWS
OH = GH // 2
OW = GW // 2
POS = OH * OW
NPOS = NS * POS
PADW = (OH + 2) * OW
EPS = 1e-05
F32 = jnp.float32
BF16 = jnp.bfloat16
ALL = ("x", "k", "y", "z")
WIDE = ("x", "y", "z")
INTERPRET = False


def split(v):
    hi = v.astype(BF16)
    return hi, (v - hi.astype(F32)).astype(BF16)


def dot_nn(a, b):
    return lax.dot_general(a, b, (((1,), (0,)), ((), ())), preferred_element_type=F32)


def dot_nt(a, b):
    return lax.dot_general(a, b, (((1,), (1,)), ((), ())), preferred_element_type=F32)


def dot3(dot, a_hi, a_lo, b_hi, b_lo):
    m = a_hi.shape[0]
    both = dot(jnp.concatenate([a_hi, a_lo], axis=0), b_hi)
    return both[:m] + both[m:] + dot(a_hi, b_lo)


def columns(row):
    return jnp.transpose(jnp.broadcast_to(row, (128, 128)))


def to_row(top, bottom):
    return jnp.sum(jnp.transpose(jnp.concatenate([top, bottom], axis=0)), axis=0, keepdims=True)


def lanes128():
    return lax.broadcasted_iota(jnp.int32, (C, 128), 1)


def from_left(v, lane):
    return jnp.where(lane == 0, 0.0, pltpu.roll(v, 1, 1))


def from_right(v, lane):
    return jnp.where(lane == 127, 0.0, pltpu.roll(v, 127, 1))


def lanes_from(start, size=OW):
    return pl.ds(pl.multiple_of(start, 128), size)


def each_sweep(body, init=0):
    return lax.fori_loop(0, NS, body, init)


def each_row(body):
    def step(t, _):
        n = lax.div(t, OH)
        body(lanes_from(t * OW), n, t - n * OH)
        return _

    lax.fori_loop(0, NS * OH, step, 0)


def put(hi_ref, lo_ref, row, col, v):
    hi, lo = split(v)
    col = pl.multiple_of(col, 128)
    hi_ref[pl.ds(row, C), pl.ds(col, 128)] = hi
    lo_ref[pl.ds(row, C), pl.ds(col, 128)] = lo


def put_shifted(hi_ref, lo_ref, n, r, v, lane):
    col = n * PADW + (r + 1) * OW
    put(hi_ref, lo_ref, 0, col, from_left(v, lane))
    put(hi_ref, lo_ref, C, col, v)
    put(hi_ref, lo_ref, 2 * C, col, from_right(v, lane))


def zero_borders(refs):
    for ref in refs:
        for n in range(NS):
            for r in (0, OH + 1):
                ref[:, pl.ds(n * PADW + r * OW, OW)] = jnp.zeros((3 * C, OW), BF16)


def conv_padded(w_hi, w_lo, hi_ref, lo_ref, n):
    cols = lanes_from(n * PADW, PADW)
    p = dot3(dot_nn, w_hi, w_lo, hi_ref[:, cols], lo_ref[:, cols])
    return p[:C, :POS] + p[C : 2 * C, OW : OW + POS] + p[2 * C :, 2 * OW : 2 * OW + POS]


def choose(layer, layers, read):
    value = read(layers[0])
    for l in layers[1:]:
        value = jnp.where(layer == l, read(l), value)
    return value


def tap_block(w_ref, buf_ref, layer, layers, tap):
    packed = choose(
        layer, layers, lambda l: w_ref[pl.ds(tap * TAP_ROWS * LAYERS + l, TAP_ROWS, stride=LAYERS), :]
    )
    buf_ref[pl.ds(0, TAP_ROWS, stride=2), :] = packed[:, :C]
    buf_ref[pl.ds(1, TAP_ROWS, stride=2), :] = packed[:, C:]
    return buf_ref[...]


def forward_weights(w_ref, buf_ref, layer, layers):
    rows = []
    for a in range(3):
        rows.append(jnp.concatenate([tap_block(w_ref, buf_ref, layer, layers, 3 * a + b) for b in range(3)], axis=1))
    return jnp.concatenate(rows, axis=0)


def backward_weights(w_ref, buf_ref, layer, layers):
    rows = []
    for a in range(3):
        blocks = [jnp.transpose(tap_block(w_ref, buf_ref, layer, layers, 3 * (2 - a) + 2 - b)) for b in range(3)]
        rows.append(jnp.concatenate(blocks, axis=1))
    return jnp.concatenate(rows, axis=0)


def first_backward_weights(w_ref, buf_ref):
    rows = []
    for a in range(3):
        left, mid, right = (jnp.transpose(tap_block(w_ref, buf_ref, 0, (0,), 3 * a + b)) for b in range(3))
        rows.append(jnp.concatenate([mid, jnp.zeros((C, C), F32)], axis=1))
        rows.append(jnp.concatenate([right, left], axis=1))
    return jnp.concatenate(rows, axis=0)


def gain_bias(gain_ref, bias_ref, layer, layers):
    def row(l):
        at = pl.ds(l, 1)
        return jnp.concatenate([gain_ref[at, :], bias_ref[at, :]], axis=1)

    gb = columns(choose(layer, layers, row))
    return gb[:C], gb[C:]


def first_core():
    return lax.axis_index("k") == 0


def store_half(refs, slot, mine_first, mine_second):
    keep_ref, send_ref = refs
    first = first_core()
    for t in range(4):
        at = pl.ds(8 + slot * BLOCK + t * TAP_ROWS, TAP_ROWS)
        keep_ref[at, :] = jnp.where(first, mine_first[t], mine_second[t])
        send_ref[at, :] = jnp.where(first, mine_second[t], mine_first[t])


def store_kernel_grad(refs, slot, per_row, buf_ref):
    def packed(tap):
        a, b = divmod(tap, 3)
        buf_ref[...] = per_row[a][:, b * C : (b + 1) * C]
        even = buf_ref[pl.ds(0, TAP_ROWS, stride=2), :]
        odd = buf_ref[pl.ds(1, TAP_ROWS, stride=2), :]
        return jnp.concatenate([even, odd], axis=1)

    taps = [packed(tap) for tap in range(9)]
    store_half(refs, slot, taps[:4], taps[4:8])
    return taps[8]


def rows_of(g_ref, stride, index):
    peers = g_ref.shape[0] // stride
    if stride == 1:
        return g_ref[...]
    return g_ref[pl.ds(index, peers, stride=stride), :]


def reduced_rows(g_ref, stride, red_ref, count):
    for j in range(count):
        red_ref[pl.ds(j, 1), :] = jnp.sum(rows_of(g_ref, stride, 1 + j), axis=0, keepdims=True)


def store_stats(z_ref, part_ref):
    acc = z_ref[:, pl.ds(0, 128)]
    for t in range(1, NPOS // 128):
        acc = acc + z_ref[:, pl.ds(t * 128, 128)]
    mean = jnp.sum(acc, axis=1, keepdims=True) * (1.0 / NPOS)
    sq = jnp.zeros((C, 128), F32)
    for t in range(NPOS // 128):
        d = z_ref[:, pl.ds(t * 128, 128)] - mean
        sq = sq + d * d
    lane = lax.broadcasted_iota(jnp.int32, (1, 128), 1)
    part_ref[pl.ds(0, 1), :] = to_row(acc, sq) * jnp.where(lane < C, 1.0 / NPOS, 1.0)


def gathered_stats(g):
    rows = g.shape[0]
    total = jnp.sum(g, axis=0, keepdims=True)
    mean = total * (1.0 / rows)
    dev = g - mean
    spread = jnp.sum(dev * dev, axis=0, keepdims=True)
    each = 2.0 * NPOS
    var = (total + each * pltpu.roll(jnp.broadcast_to(spread, (8, 128)), C, 1)[:1]) * (1.0 / (each * rows))
    lane = lax.broadcasted_iota(jnp.int32, (1, 128), 1)
    return jnp.where(lane < C, mean, lax.rsqrt(var + EPS))


def pfn_kernel(pts_in, cnt_in, cell_in, w_in, hmax_ref, part_ref, base_ref, w_pad, pts_ref, cnt_ref, cell_ref, w_ref, sems):
    copies = [
        pltpu.make_async_copy(src, dst, sems.at[i])
        for i, (src, dst) in enumerate(
            ((pts_in, pts_ref), (cnt_in, cnt_ref), (cell_in, cell_ref), (w_in, w_ref))
        )
    ]
    for copy in copies:
        copy.start()
    for copy in copies:
        copy.wait()
    w_pad[...] = jnp.zeros((128, 128), F32)
    w_pad[pl.ds(0, 9), pl.ds(0, C)] = w_ref[...]
    w_cols = jnp.transpose(w_pad[...])

    def col(j):
        return w_cols[:C, j : j + 1]

    wx = col(0) + col(4) + col(7)
    wy = col(1) + col(5) + col(8)
    wz = col(2) + col(6)
    wr = col(3)
    slot = lax.broadcasted_iota(jnp.int32, (MAXP, PILL), 0)
    total = jnp.zeros((C, 1), F32)
    number = jnp.zeros((1, 1), F32)
    for n in range(NS):
        count_i = cnt_ref[pl.ds(n, 1), :]
        count = count_i.astype(F32)
        valid = slot < count_i
        sums = []
        for j in range(4):
            p = pts_ref[pl.ds((n * 4 + j) * MAXP, MAXP), :]
            sums.append(jnp.sum(jnp.where(valid, p, 0.0), axis=0, keepdims=True))
        cell = cell_ref[pl.ds(n, 1), :]
        col_pos = jnp.bitwise_and(cell, GW - 1).astype(F32) * (2.0 / GW) - 1.0
        row_pos = jnp.right_shift(cell, 8).astype(F32) * (2.0 / GH) - 1.0
        base = -(
            col(4) * (sums[0] / count)
            + col(5) * (sums[1] / count)
            + col(6) * (sums[2] / count)
            + col(7) * col_pos
            + col(8) * row_pos
        )
        base_ref[:, pl.ds(n * PILL, PILL)] = base
        weighted = wx * sums[0] + wy * sums[1] + wz * sums[2] + wr * sums[3] + base * count
        total = total + jnp.sum(weighted, axis=1, keepdims=True)
        number = number + jnp.sum(count, axis=1, keepdims=True)
    mean = total / number
    sq_parts = []
    half = C // 2
    for c0 in (0, half):
        ch = slice(c0, c0 + half)
        bx = jnp.broadcast_to(wx[ch], (half, 128))
        by = jnp.broadcast_to(wy[ch], (half, 128))
        bz = jnp.broadcast_to(wz[ch], (half, 128))
        br = jnp.broadcast_to(wr[ch], (half, 128))
        mb = jnp.broadcast_to(mean[ch], (half, 128))
        sq = jnp.zeros((half, 128), F32)
        for n in range(NS):
            for q in range(PILL // 128):
                lanes = pl.ds(q * 128, 128)
                base = base_ref[pl.ds(c0, half), pl.ds(n * PILL + q * 128, 128)] - mb
                count = cnt_ref[pl.ds(n, 1), lanes]

                def step(k8, carry, n=n, lanes=lanes, base=base, count=count, bx=bx, by=by, bz=bz, br=br):
                    best, sq = carry
                    p = [
                        pts_ref[pl.ds(pl.multiple_of((n * 4 + j) * MAXP + k8 * 8, 8), 8), lanes]
                        for j in range(4)
                    ]
                    for i in range(8):
                        px, py, pz, pr = (v[i : i + 1] for v in p)
                        d = bx * px + by * py + (bz * pz + br * pr) + base
                        ok = jnp.broadcast_to(k8 * 8 + i < count, (half, 128))
                        best = jnp.where(ok, jnp.maximum(best, d), best)
                        sq = sq + jnp.where(ok, d * d, 0.0)
                    return best, sq

                start = jnp.full((half, 128), -3.0e38, F32)
                best, sq = lax.fori_loop(0, MAXP // 8, step, (start, sq))
                hmax_ref[pl.ds(c0, half), pl.ds(n * PILL + q * 128, 128)] = best + mb
        sq_parts.append(sq)
    lane = lanes128()
    part_ref[pl.ds(0, 1), :] = to_row(
        jnp.where(lane == 0, total, 0.0), jnp.concatenate(sq_parts, axis=0)
    )
    part_ref[pl.ds(1, 1), :] = jnp.broadcast_to(number, (1, 128))


def cells_of(cell_ref, n):
    return jnp.where(n == 0, cell_ref[pl.ds(0, 1), :], cell_ref[pl.ds(1, 1), :])


def target_lane(cell):
    row = jnp.right_shift(cell, 8)
    col = jnp.bitwise_and(cell, GW - 1)
    phase = jnp.bitwise_and(row, 1) * 2 + jnp.bitwise_and(col, 1)
    return phase * POS + jnp.right_shift(row, 1) * OW + jnp.right_shift(col, 1)


def build_onehot(oht_ref, cell):
    target = jnp.broadcast_to(target_lane(cell), (256, PILL))
    iota = lax.broadcasted_iota(jnp.int32, (256, PILL), 0)
    for t in range(GH * GW // 256):
        oht_ref[pl.ds(t * 256, 256), :] = jnp.where(iota + t * 256 == target, 1.0, 0.0).astype(BF16)


def first_conv_kernel(
    g_ref, hmax_ref, cell_ref, gain_ref, bias_ref, w_ref,
    z_ref, part_ref, ev_hi, ev_lo, od_hi, od_lo,
    oht_ref, place_ref, buf_ref,
):
    s = rows_of(g_ref, 2, 0)
    num = rows_of(g_ref, 2, 1)
    total = jnp.sum(s, axis=0, keepdims=True)
    number = jnp.sum(num, axis=0, keepdims=True)
    mean = total / number
    dev = s / num - mean
    spread = jnp.sum(num * dev * dev, axis=0, keepdims=True)
    var = (total + pltpu.roll(jnp.broadcast_to(spread, (8, 128)), C, 1)[:1]) / number
    lane_row = lax.broadcasted_iota(jnp.int32, (1, 128), 1)
    stats = columns(jnp.where(lane_row < C, mean, lax.rsqrt(var + EPS)))
    mean_c, inv_c = stats[:C], stats[C:]
    gain, bias = gain_bias(gain_ref, bias_ref, 0, (0,))
    lane = lanes128()
    w_hi, w_lo = split(forward_weights(w_ref, buf_ref, 0, (0,)))
    outer_hi = jnp.concatenate([w_hi[:C], w_hi[2 * C :]], axis=0)
    outer_lo = jnp.concatenate([w_lo[:C], w_lo[2 * C :]], axis=0)

    def sweep(n, _):
        build_onehot(oht_ref, cells_of(cell_ref, n))
        tiles = []
        for q in range(PILL // 128):
            h = hmax_ref[:, lanes_from(n * PILL + q * 128)]
            tiles.append(jnp.maximum(gain * (h - mean_c) * inv_c + bias, 0.0))
        p_hi, p_lo = split(jnp.concatenate(tiles, axis=1))
        place_ref[...] = dot_nt(jnp.concatenate([p_hi, p_lo], axis=0), oht_ref[...])
        for pr, refs in ((0, (ev_hi, ev_lo)), (1, (od_hi, od_lo))):
            for part, ref in enumerate(refs):
                width = POS + pr * OW
                if pr:
                    ref[:, lanes_from(n * width)] = jnp.zeros((3 * C, OW), BF16)
                for r in range(OH):
                    even = place_ref[pl.ds(part * C, C), pl.ds(pr * 2 * POS + r * OW, OW)]
                    odd = place_ref[pl.ds(part * C, C), pl.ds((pr * 2 + 1) * POS + r * OW, OW)]
                    at = lanes_from(n * width + (r + pr) * OW)
                    ref[pl.ds(0, C), at] = from_left(odd, lane).astype(BF16)
                    ref[pl.ds(C, C), at] = even.astype(BF16)
                    ref[pl.ds(2 * C, C), at] = odd.astype(BF16)
        at = lanes_from(n * POS, POS)
        z = dot3(dot_nn, w_hi[C : 2 * C], w_lo[C : 2 * C], ev_hi[:, at], ev_lo[:, at])
        at = lanes_from(n * (POS + OW), POS + OW)
        p = dot3(dot_nn, outer_hi, outer_lo, od_hi[:, at], od_lo[:, at])
        z_ref[:, lanes_from(n * POS, POS)] = z + p[:C, :POS] + p[C:, OW:]
        return _

    each_sweep(sweep)
    store_stats(z_ref, part_ref)


def first_grad_rows(grad_of, grid_refs):
    ev_hi, ev_lo, od_hi, od_lo = grid_refs

    def sweep(n, rows):
        g_hi, g_lo = grad_of(n)
        out = []
        for row, hi, lo, start in zip(
            rows,
            (od_hi, ev_hi, od_hi),
            (od_lo, ev_lo, od_lo),
            (n * (POS + OW), n * POS, n * (POS + OW) + OW),
        ):
            at = lanes_from(start, POS)
            out.append(row + dot3(dot_nt, g_hi, g_lo, hi[:, at], lo[:, at]))
        return tuple(out)

    return each_sweep(sweep, tuple(jnp.zeros((C, 3 * C), F32) for _ in range(3)))


def first_input_sums(grid_refs):
    ev_hi, ev_lo, od_hi, od_lo = grid_refs
    one = jnp.ones((16, POS), BF16)

    def sweep(n, rows):
        out = []
        for row, hi, lo, start in zip(
            rows,
            (od_hi, ev_hi, od_hi),
            (od_lo, ev_lo, od_lo),
            (n * (POS + OW), n * POS, n * (POS + OW) + OW),
        ):
            at = lanes_from(start, POS)
            out.append(row + dot_nt(one, hi[:, at]) + dot_nt(one, lo[:, at]))
        return tuple(out)

    rows = each_sweep(sweep, tuple(jnp.zeros((16, 3 * C), F32) for _ in range(3)))
    return [jnp.broadcast_to(row[:1], (C, 3 * C)) for row in rows]


def conv_kernel(
    l_ref, g_ref, z_ref, gain_ref, bias_ref, w_ref, out_ref, part_ref, stats_ref, s_hi, s_lo, buf_ref
):
    layer = l_ref[0]
    stats = columns(gathered_stats(g_ref[...]))
    stats_ref[...] = stats
    mean, inv = stats[:C], stats[C:]
    gain, bias = gain_bias(gain_ref, bias_ref, layer - 1, (0, 1, 2))
    lane = lanes128()
    zero_borders((s_hi, s_lo))
    w_hi, w_lo = split(forward_weights(w_ref, buf_ref, layer, (1, 2, 3)))

    def activate(at, n, r):
        y = gain * ((z_ref[:, at] - mean) * inv) + bias
        put_shifted(s_hi, s_lo, n, r, y * jax.nn.sigmoid(y), lane)

    def sweep(n, _):
        out_ref[:, lanes_from(n * POS, POS)] = conv_padded(w_hi, w_lo, s_hi, s_lo, n)
        return _

    each_row(activate)
    each_sweep(sweep)
    store_stats(out_ref, part_ref)


def turn_kernel(
    g_ref, z_ref, gain_ref, bias_ref, ct_ref, z0_ref, stats0_ref, ev_hi, ev_lo, od_hi, od_lo,
    feat_ref, gy_ref, keep_ref, send_ref, stats_ref,
    buf_ref,
):
    stats = columns(gathered_stats(g_ref[...]))
    stats_ref[...] = stats
    mean, inv = stats[:C], stats[C:]
    gain, bias = gain_bias(gain_ref, bias_ref, LAYERS - 1, (LAYERS - 1,))
    dy = jnp.zeros((C, 128), F32)
    dx = jnp.zeros((C, 128), F32)
    for n in range(NS):
        for r in range(OH):
            at = pl.ds(n * POS + r * OW, OW)
            rows = pl.ds(n * C * OH + r, C, stride=OH)
            xhat = (z_ref[:, at] - mean) * inv
            y = gain * xhat + bias
            sg = jax.nn.sigmoid(y)
            feat_ref[rows, :] = y * sg
            gy = ct_ref[rows, :] * (sg * (1.0 + y * (1.0 - sg)))
            gy_ref[:, at] = gy
            dy = dy + gy
            dx = dx + gy * xhat
    part = to_row(dy, dx)
    keep_ref[pl.ds(0, 1), :] = part
    send_ref[pl.ds(0, 1), :] = part
    mean0, inv0 = stats0_ref[pl.ds(0, C), pl.ds(0, 1)], stats0_ref[pl.ds(C, C), pl.ds(0, 1)]
    grads = first_grad_rows(
        lambda n: split((z0_ref[:, lanes_from(n * POS, POS)] - mean0) * inv0), (ev_hi, ev_lo, od_hi, od_lo)
    )
    refs = (keep_ref, send_ref)
    none = jnp.zeros((TAP_ROWS, 128), F32)
    last = store_kernel_grad(refs, 0, grads, buf_ref)
    store_half(refs, 2, [last, none, none, none], [none] * 4)
    grads = first_input_sums((ev_hi, ev_lo, od_hi, od_lo))
    last = store_kernel_grad(refs, 1, grads, buf_ref)
    store_half(refs, 3, [last, none, none, none], [none] * 4)


def grad_scales(g, stats, gain):
    total = jnp.sum(g, axis=0, keepdims=True)
    entries = 2.0 * NPOS * g.shape[0]
    t = columns(total * (1.0 / entries))
    return gain * stats[C:], t[:C], t[C:], total


def back_kernel(
    g_ref, z_ref, gy_ref, stats_ref, gain_ref, bias_ref, zp_ref, statsp_ref, w_ref, *refs, layers, stride
):
    (layer,) = layers
    if layer == 1:
        grid0, last3_ref, last2_ref, refs = refs[:4], refs[4], refs[5], refs[6:]
    gyp_ref, keep_ref, send_ref, sums_ref, red_ref, *refs = refs
    if layer != 1:
        last_ref, *refs = refs
    s_hi, s_lo, a_hi, a_lo, slope_ref, buf_ref = refs
    reduced_rows(g_ref, stride, red_ref, red_ref.shape[0])
    stats = stats_ref[...]
    mean, inv = stats[:C], stats[C:]
    gain, _ = gain_bias(gain_ref, bias_ref, layer, layers)
    scale, mean_dy, mean_dx, sums_ref[...] = grad_scales(rows_of(g_ref, stride, 0), stats, gain)
    statsp = statsp_ref[...]
    meanp, invp = statsp[:C], statsp[C:]
    gainp, biasp = gain_bias(gain_ref, bias_ref, layer - 1, tuple(l - 1 for l in layers))
    lane = lanes128()
    zero_borders((s_hi, s_lo, a_hi, a_lo))
    w_hi, w_lo = split(backward_weights(w_ref, buf_ref, layer, layers))

    def turn_back(at, n, r):
        xhat = (z_ref[:, at] - mean) * inv
        gz = scale * (gy_ref[:, at] - mean_dy - xhat * mean_dx)
        put_shifted(s_hi, s_lo, n, r, gz, lane)
        y = gainp * ((zp_ref[:, at] - meanp) * invp) + biasp
        sg = jax.nn.sigmoid(y)
        slope_ref[:, at] = sg * (1.0 + y * (1.0 - sg))
        put_shifted(a_hi, a_lo, n, r, y * sg, lane)

    def sweep(n, carry):
        dy, dx = carry
        u = conv_padded(w_hi, w_lo, s_hi, s_lo, n)
        for r in range(OH):
            at = lanes_from(n * POS + r * OW)
            gy = u[:, r * OW : (r + 1) * OW] * slope_ref[:, at]
            gyp_ref[:, at] = gy
            dy = dy + gy
            dx = dx + gy * ((zp_ref[:, at] - meanp) * invp)
        return dy, dx

    each_row(turn_back)
    zero = jnp.zeros((C, 128), F32)
    dy, dx = each_sweep(sweep, (zero, zero))
    part = to_row(dy, dx)
    keep_ref[pl.ds(0, 1), :] = part
    send_ref[pl.ds(0, 1), :] = part
    span = NS * PADW - 2 * OW
    g_at = pl.ds(OW, span)
    g_hi, g_lo = s_hi[pl.ds(C, C), g_at], s_lo[pl.ds(C, C), g_at]
    rows = [
        dot3(dot_nt, g_hi, g_lo, a_hi[:, pl.ds(a * OW, span)], a_lo[:, pl.ds(a * OW, span)]) for a in range(3)
    ]
    refs = (keep_ref, send_ref)
    last = store_kernel_grad(refs, 0, rows, buf_ref)
    if layer == 1:
        rows = first_grad_rows(lambda n: split(gyp_ref[:, lanes_from(n * POS, POS)]), grid0)
        last0 = store_kernel_grad(refs, 1, rows, buf_ref)
        none = jnp.zeros((TAP_ROWS, 128), F32)
        store_half(refs, 2, [last0, none, none, none], [last, last2_ref[...], last3_ref[...], none])
        store_half(refs, 3, [none] * 4, [none] * 4)
    else:
        last_ref[...] = last


def pick_channels(tile, pair, lane):
    row = lax.broadcasted_iota(jnp.int32, (C, 128), 0)
    want = 2 * pair + jnp.where(lane < C, 0, 1)
    return jnp.sum(jnp.where(row == want, tile, 0.0), axis=0, keepdims=True)


def last_back_kernel(
    g_ref, z_ref, gy_ref, stats_ref, gain_ref, bias_ref, cell_ref, w_ref,
    first_red, red3, red2, sums1, sums2, sums3,
    pg_ref, norm_ref, own_ref,
    t_hi, t_lo, u_hi, oht_ref, buf_ref, *, stride,
):
    stats = stats_ref[...]
    mean, inv = stats[:C], stats[C:]
    gain, _ = gain_bias(gain_ref, bias_ref, 0, (0,))
    scale, mean_dy, mean_dx, sums0 = grad_scales(rows_of(g_ref, stride, 0), stats, gain)
    for l, row in enumerate((sums0, sums1[...], sums2[...], sums3[...])):
        norm_ref[pl.ds(l, 1), :] = row[:, C:]
        norm_ref[pl.ds(LAYERS + l, 1), :] = row[:, :C]
    lane = lanes128()
    count = red3.shape[0]
    peers = BLOCK // count
    spot = lax.axis_index(WIDE)

    def first_grad(raw, normed, plain, pair):
        return pick_channels(scale, pair, lane) * (
            raw - pick_channels(mean_dy, pair, lane) * plain - pick_channels(mean_dx, pair, lane) * normed
        )

    for j in range(count):
        pair = lax.rem(j * peers + spot, TAP_ROWS)
        here, raw, ends = (
            jnp.sum(rows_of(g_ref, stride, 1 + q * count + j), axis=0, keepdims=True) for q in range(3)
        )
        normed, plain, normed_end, plain_end = (first_red[pl.ds(q * count + j, 1), :] for q in range(4))
        ends = jnp.where(first_core(), first_grad(ends, normed_end, plain_end, pair), ends)
        own = (first_grad(raw, normed, plain, pair), here, red2[pl.ds(j, 1), :], red3[pl.ds(j, 1), :], ends)
        for q in range(5):
            own_ref[pl.ds(q * count + j, 1), :] = own[q]
    v_hi, v_lo = split(first_backward_weights(w_ref, buf_ref))

    def sweep(n, _):
        for ref in (t_hi, t_lo):
            ref[:, pl.ds(POS, OW)] = jnp.zeros((2 * C, OW), BF16)
        for r in range(OH):
            at = lanes_from(n * POS + r * OW)
            xhat = (z_ref[:, at] - mean) * inv
            gz = scale * (gy_ref[:, at] - mean_dy - xhat * mean_dx)
            put(t_hi, t_lo, 0, r * OW, gz)
            put(t_hi, t_lo, C, r * OW, from_right(gz, lane))
        v = dot3(dot_nn, v_hi, v_lo, t_hi[...], t_lo[...])
        for pc in range(2):
            above = v[pc * C : (pc + 1) * C, OW:]
            here = v[(2 + pc) * C : (3 + pc) * C, :POS]
            below = v[(4 + pc) * C : (5 + pc) * C, :POS]
            for pr, u in ((0, here), (1, below + above)):
                at = pl.ds((pr * 2 + pc) * POS, POS)
                hi, lo = split(u)
                u_hi[pl.ds(0, C), at] = hi
                u_hi[pl.ds(C, C), at] = lo
        build_onehot(oht_ref, cells_of(cell_ref, n))
        picked = dot_nn(u_hi[...], oht_ref[...])
        pg_ref[pl.ds(pl.multiple_of(n * C, C), C), :] = picked[:C] + picked[C:]
        return _

    each_sweep(sweep)


def pair_kernel(*refs, mode, stride, count):
    *ins, out_ref = refs
    keep_ref, got_ref = (ins[0].at[pl.ds(0, 8)], ins[0].at[pl.ds(8, 8)]) if len(ins) == 1 else ins
    peers = out_ref.shape[0] // stride
    mine, other = keep_ref[pl.ds(0, 1), :], got_ref[pl.ds(0, 1), :]
    both = mine + other
    lane = lax.broadcasted_iota(jnp.int32, (1, 128), 1)

    def swap(v):
        return pltpu.roll(jnp.broadcast_to(v, (8, 128)), C, 1)[:1]

    if mode == "stats":
        gap = mine - other
        both = jnp.where(lane < C, 0.5 * both, both + (0.5 * NPOS) * swap(gap * gap))
    if mode == "pillars":
        m_num, o_num = keep_ref[pl.ds(1, 1), :], got_ref[pl.ds(1, 1), :]
        number = m_num + o_num
        gap = mine / m_num - other / o_num
        both = jnp.where(lane < C, both, both + (m_num * o_num / number) * swap(gap * gap))
        out_ref[pl.ds(1, peers, stride=stride), :] = jnp.broadcast_to(number, (peers, 128))
    row = jnp.broadcast_to(both, (peers, 128))
    if stride == 1:
        out_ref[...] = row
    else:
        out_ref[pl.ds(0, peers, stride=stride), :] = row
    for j in range(count):
        at = pl.ds(8 + j * peers, peers)
        out_ref[pl.ds(1 + j, peers, stride=stride), :] = keep_ref[at, :] + got_ref[at, :]


def assemble_kernel(mine_ref, theirs_ref, out_ref, *, peers):
    first = first_core()
    count = BLOCK // peers
    per_peer = (LAYERS + 1) * count

    def halves(at):
        mine, theirs = mine_ref[at, :], theirs_ref[at, :]
        return jnp.where(first, mine, theirs), jnp.where(first, theirs, mine)

    for l in range(LAYERS):
        for j in range(count):
            for h, rows in enumerate(halves(pl.ds(l * count + j, peers, stride=per_peer))):
                out_ref[pl.ds((h * BLOCK + j * peers) * LAYERS + l, peers, stride=LAYERS), :] = rows
        size = min(peers, TAP_ROWS)
        for step in range(0, TAP_ROWS, size):
            start = max(l - 1, 0) * TAP_ROWS + step
            at = pl.ds(start % peers * per_peer + LAYERS * count + start // peers, size, stride=per_peer)
            rows = halves(at)[0 if l == 0 else 1]
            out_ref[pl.ds((2 * BLOCK + step) * LAYERS + l, size, stride=LAYERS), :] = rows


def call(kernel, name, outs, args, scratch=(), scalar=False, copies=False, **params):
    specs = [pl.BlockSpec(memory_space=pltpu.HBM if copies else pltpu.VMEM)] * len(args)
    if scalar:
        specs[0] = pl.BlockSpec(memory_space=pltpu.SMEM)
    return pl.pallas_call(
        functools.partial(kernel, **params) if params else kernel,
        name=name,
        out_shape=tuple(jax.ShapeDtypeStruct(shape, dtype) for shape, dtype in outs),
        in_specs=specs,
        scratch_shapes=[pltpu.VMEM(shape, dtype) for shape, dtype in scratch]
        + [pltpu.SemaphoreType.DMA((len(args),))] * copies,
        compiler_params=pltpu.CompilerParams(vmem_limit_bytes=20 << 20),
        interpret=INTERPRET,
    )(*args)


def partner(v):
    return lax.ppermute(v, "k", [(0, 1), (1, 0)])


def to_peers(rows, peers):
    sent = rows.reshape(peers, -1, 1, 128)
    return lax.all_to_all(sent, WIDE, 0, 0, tiled=True).reshape(-1, 128)


def exchange(name, mode, keep, send, peers, stride=1, count=0):
    pair = (keep, partner(send)) if send is not None else (lax.all_gather(keep, "k", tiled=True),)
    (out,) = call(
        pair_kernel, name, [((peers * stride, 128), F32)], pair, mode=mode, stride=stride, count=count
    )
    return to_peers(out, peers)


def per_device(
    points, counts, cells, pfn_weight, pfn_gain, pfn_bias, conv_weight, bn_gain, bn_bias, cotangent,
    *, sizes,
):
    peers = sizes["x"] * sizes["y"] * sizes["z"]
    count = BLOCK // peers
    w = conv_weight.reshape(LAYERS, 9, TAP_ROWS, 128).transpose(1, 2, 0, 3).reshape(9 * TAP_ROWS * LAYERS, 128)
    row = ((1, 128), F32)
    rows8 = ((8, 128), F32)
    tile = ((128, 128), F32)
    plane = ((C, NPOS), F32)
    pad = ((3 * C, NS * PADW), BF16)
    buf = ((C, C), F32)
    end = ((TAP_ROWS, 128), F32)

    hmax, part = call(
        pfn_kernel, "pfn", [((C, NS * PILL), F32), rows8],
        (points.reshape(NS * 4 * MAXP, PILL), counts, cells, pfn_weight),
        [((C, NS * PILL), F32), tile, ((NS * 4 * MAXP, PILL), F32), ((NS, PILL), jnp.int32), ((NS, PILL), jnp.int32), ((9, C), F32)],
        copies=True,
    )
    got = exchange("pair_p", "pillars", part, None, peers, 2)
    ev = ((3 * C, NS * POS), BF16)
    od = ((3 * C, NS * (POS + OW)), BF16)
    z, part, *grid0 = call(
        first_conv_kernel, "conv0", [plane, rows8, ev, ev, od, od],
        (got, hmax, cells, pfn_gain[None], pfn_bias[None], w),
        [((GH * GW, PILL), BF16), ((2 * C, GH * GW), F32), buf],
    )
    pre = [z]
    stats = []
    for l in range(1, LAYERS):
        got = exchange("pair_s", "stats", part, None, peers)
        z, part, st = call(
            conv_kernel, "conv", [plane, rows8, tile],
            (jnp.full((1,), l, jnp.int32), got, pre[-1], bn_gain, bn_bias, w), [pad, pad, buf], scalar=True,
        )
        pre.append(z)
        stats.append(st)
    got = exchange("pair_s", "stats", part, part, peers)
    slab = ((NS * C * OH, OW), F32)
    payload = ((8 + 4 * BLOCK, 128), F32)
    feat, gy, keep, send, st = call(
        turn_kernel, "turn", [slab, plane, payload, payload, tile],
        (got, pre[-1], bn_gain, bn_bias, cotangent.reshape(NS * C * OH, OW), pre[0], stats[0], *grid0),
        [buf],
    )
    stats.append(st)
    sums = [None] * LAYERS
    reds = [None] * LAYERS
    ends = []
    blocks = 4
    for l in range(LAYERS - 1, 0, -1):
        got = exchange(f"pair_g{blocks}", "sums", keep, send, peers, 1 + blocks * count, blocks * count)
        after = 4 if l == 1 else 1
        payload = ((8 + after * BLOCK, 128), F32)
        gy, keep, send, sums[l], reds[l], *end_rows = call(
            back_kernel, f"back{l}", [plane, payload, payload, row, ((blocks * count, 128), F32)] + [end] * (l > 1),
            (got, pre[l], gy, stats[l], bn_gain, bn_bias, pre[l - 1], stats[l - 1], w)
            + ((*grid0, *ends) if l == 1 else ()),
            [pad, pad, pad, pad, plane, buf], layers=(l,), stride=1 + blocks * count,
        )
        ends += end_rows
        blocks = after
    got = exchange(f"pair_g{blocks}", "sums", keep, send, peers, 1 + blocks * count, blocks * count)
    tbuf = ((2 * C, POS + OW), BF16)
    pillar_grad, norm_grads, own = call(
        last_back_kernel, "back0",
        [((NS * C, PILL), F32), ((2 * LAYERS, C), F32), (((LAYERS + 1) * count, 128), F32)],
        (got, pre[0], gy, stats[0], bn_gain, bn_bias, cells, w, reds[3], reds[2], reds[1], *sums[1:]),
        [tbuf, tbuf, ((2 * C, GH * GW), BF16), ((GH * GW, PILL), BF16), buf], stride=1 + blocks * count,
    )
    rows = (LAYERS + 1) * count
    mine = to_peers(jnp.broadcast_to(own[None], (peers, rows, 128)).reshape(peers * rows, 128), peers)
    (total,) = call(
        assemble_kernel, "assemble", [((9 * TAP_ROWS * LAYERS, 128), F32)], (mine, partner(mine)), peers=peers
    )
    total = total.reshape(9, TAP_ROWS, LAYERS, 128).transpose(2, 0, 1, 3).reshape(LAYERS, 9, C * C)
    return (
        feat.reshape(NS, C, OH, OW),
        total,
        norm_grads.reshape(2, LAYERS, C),
        pillar_grad.reshape(NS, C, PILL),
    )


def build(finer):
    sizes = dict(finer.shape)
    split4 = P(ALL, None, None, None)
    return jax.shard_map(
        functools.partial(per_device, sizes=sizes),
        mesh=finer,
        in_specs=(split4, P(ALL, None), P(ALL, None), P(), P(), P(), P(), P(), P(), split4),
        out_specs=(split4, P(), P(), P(ALL, None, None)),
        check_vma=False,
    )


def solution(mesh):
    return build(Mesh(mesh.devices.reshape(4, 2, 4, 8), ALL))
```

```python
import functools

import jax
import jax.numpy as jnp
from jax import lax
from jax.experimental import pallas as pl
from jax.experimental.pallas import tpu as pltpu
from jax.sharding import Mesh
from jax.sharding import PartitionSpec as P

C = 64
MAXP = 32
LAYERS = 4
GH = 8
GW = 256
PILL = 256
NS = 2
TAP_ROWS = C * C // 128
BLOCK = 4 * TAP_ROWS
OH = GH // 2
OW = GW // 2
POS = OH * OW
NPOS = NS * POS
PADW = (OH + 2) * OW
EPS = 1e-05
F32 = jnp.float32
BF16 = jnp.bfloat16
ALL = ("x", "k", "y", "z")
WIDE = ("x", "y", "z")
INTERPRET = False
GB_ROW = C
TARGET_ROW = C + 8
KEPT_ROWS = C + 16


def split(v):
    hi = v.astype(BF16)
    return hi, (v - hi.astype(F32)).astype(BF16)


def dot_nn(a, b):
    return lax.dot_general(a, b, (((1,), (0,)), ((), ())), preferred_element_type=F32)


def dot_nt(a, b):
    return lax.dot_general(a, b, (((1,), (1,)), ((), ())), preferred_element_type=F32)


def dot3(dot, a_hi, a_lo, b_hi, b_lo):
    m = a_hi.shape[0]
    both = dot(jnp.concatenate([a_hi, a_lo], axis=0), b_hi)
    return both[:m] + both[m:] + dot(a_hi, b_lo)


def columns(row):
    return jnp.transpose(jnp.broadcast_to(row, (128, 128)))


def to_row(top, bottom):
    return jnp.sum(jnp.transpose(jnp.concatenate([top, bottom], axis=0)), axis=0, keepdims=True)


def lanes128():
    return lax.broadcasted_iota(jnp.int32, (C, 128), 1)


def from_left(v, lane):
    return jnp.where(lane == 0, 0.0, pltpu.roll(v, 1, 1))


def from_right(v, lane):
    return jnp.where(lane == 127, 0.0, pltpu.roll(v, 127, 1))


def lanes_from(start, size=OW):
    if isinstance(start, int):
        return pl.ds(start, size)
    return pl.ds(pl.multiple_of(start, 128), size)


def each_sweep(body, init=0):
    return lax.fori_loop(0, NS, body, init)


def each_row(body):
    for t in range(NS * OH):
        body(lanes_from(t * OW), t // OH, t % OH)


def put(hi_ref, lo_ref, row, col, v):
    hi, lo = split(v)
    hi_ref[pl.ds(row, C), lanes_from(col)] = hi
    lo_ref[pl.ds(row, C), lanes_from(col)] = lo


def put_shifted(hi_ref, lo_ref, n, r, v, lane):
    col = n * PADW + (r + 1) * OW
    put(hi_ref, lo_ref, 0, col, from_left(v, lane))
    put(hi_ref, lo_ref, C, col, v)
    put(hi_ref, lo_ref, 2 * C, col, from_right(v, lane))


def zero_borders(refs):
    for ref in refs:
        for n in range(NS):
            for r in (0, OH + 1):
                ref[:, pl.ds(n * PADW + r * OW, OW)] = jnp.zeros((3 * C, OW), BF16)


def conv_padded(w_hi, w_lo, hi_ref, lo_ref, n):
    cols = lanes_from(n * PADW, PADW)
    p = dot3(dot_nn, w_hi, w_lo, hi_ref[:, cols], lo_ref[:, cols])
    return p[:C, :POS] + p[C : 2 * C, OW : OW + POS] + p[2 * C :, 2 * OW : 2 * OW + POS]


def tap_block(w_ref, buf_ref, layer, tap):
    packed = w_ref[pl.ds(tap * TAP_ROWS * LAYERS + layer, TAP_ROWS, stride=LAYERS), :]
    buf_ref[pl.ds(0, TAP_ROWS, stride=2), :] = packed[:, :C]
    buf_ref[pl.ds(1, TAP_ROWS, stride=2), :] = packed[:, C:]
    return buf_ref[...]


def forward_weights(w_ref, buf_ref, layer):
    rows = []
    for a in range(3):
        rows.append(jnp.concatenate([tap_block(w_ref, buf_ref, layer, 3 * a + b) for b in range(3)], axis=1))
    return jnp.concatenate(rows, axis=0)


def backward_weights(w_ref, buf_ref, layer):
    rows = []
    for a in range(3):
        blocks = [jnp.transpose(tap_block(w_ref, buf_ref, layer, 3 * (2 - a) + 2 - b)) for b in range(3)]
        rows.append(jnp.concatenate(blocks, axis=1))
    return jnp.concatenate(rows, axis=0)


def first_backward_weights(w_ref, buf_ref):
    rows = []
    for a in range(3):
        left, mid, right = (jnp.transpose(tap_block(w_ref, buf_ref, 0, 3 * a + b)) for b in range(3))
        rows.append(jnp.concatenate([mid, jnp.zeros((C, C), F32)], axis=1))
        rows.append(jnp.concatenate([right, left], axis=1))
    return jnp.concatenate(rows, axis=0)


def gain_bias(gb_ref, row):
    gb = columns(gb_ref[pl.ds(GB_ROW + row, 1), pl.ds(0, 128)])
    return gb[:C], gb[C:]


def first_core():
    return lax.axis_index("k") == 0


def store_half(refs, slot, mine_first, mine_second):
    keep_ref, send_ref = refs
    first = first_core()
    for t in range(4):
        at = pl.ds(8 + slot * BLOCK + t * TAP_ROWS, TAP_ROWS)
        keep_ref[at, :] = jnp.where(first, mine_first[t], mine_second[t])
        send_ref[at, :] = jnp.where(first, mine_second[t], mine_first[t])


def store_kernel_grad(refs, slot, per_row, buf_ref):
    def packed(tap):
        a, b = divmod(tap, 3)
        buf_ref[...] = per_row[a][:, b * C : (b + 1) * C]
        even = buf_ref[pl.ds(0, TAP_ROWS, stride=2), :]
        odd = buf_ref[pl.ds(1, TAP_ROWS, stride=2), :]
        return jnp.concatenate([even, odd], axis=1)

    taps = [packed(tap) for tap in range(9)]
    store_half(refs, slot, taps[:4], taps[4:8])
    return taps[8]


def rows_of(g_ref, stride, index):
    peers = g_ref.shape[0] // stride
    if stride == 1:
        return g_ref[...]
    return g_ref[pl.ds(index, peers, stride=stride), :]


def reduced_rows(g_ref, stride, red_ref, count):
    for j in range(count):
        red_ref[pl.ds(j, 1), :] = jnp.sum(rows_of(g_ref, stride, 1 + j), axis=0, keepdims=True)


def store_stats(z_ref, part_ref):
    acc = z_ref[:, pl.ds(0, 128)]
    for t in range(1, NPOS // 128):
        acc = acc + z_ref[:, pl.ds(t * 128, 128)]
    mean = jnp.sum(acc, axis=1, keepdims=True) * (1.0 / NPOS)
    sq = jnp.zeros((C, 128), F32)
    for t in range(NPOS // 128):
        d = z_ref[:, pl.ds(t * 128, 128)] - mean
        sq = sq + d * d
    lane = lax.broadcasted_iota(jnp.int32, (1, 128), 1)
    part_ref[pl.ds(0, 1), :] = to_row(acc, sq) * jnp.where(lane < C, 1.0 / NPOS, 1.0)


def gathered_stats(g):
    rows = g.shape[0]
    total = jnp.sum(g, axis=0, keepdims=True)
    mean = total * (1.0 / rows)
    dev = g - mean
    spread = jnp.sum(dev * dev, axis=0, keepdims=True)
    each = 2.0 * NPOS
    var = (total + each * pltpu.roll(jnp.broadcast_to(spread, (8, 128)), C, 1)[:1]) * (1.0 / (each * rows))
    lane = lax.broadcasted_iota(jnp.int32, (1, 128), 1)
    return jnp.where(lane < C, mean, lax.rsqrt(var + EPS))


def pfn_kernel(
    pts_in, cnt_in, cell_in, w_in, gain_in, bias_in, pgain_in, pbias_in,
    kept_ref, part_ref,
    base_ref, w_pad, pts_ref, cnt_ref, cell_ref, w_ref, gain_ref, bias_ref, pgain_ref, pbias_ref, sems,
):
    copies = [
        pltpu.make_async_copy(src, dst, sems.at[i])
        for i, (src, dst) in enumerate(
            (
                (pts_in, pts_ref), (cnt_in, cnt_ref), (cell_in, cell_ref), (w_in, w_ref),
                (gain_in, gain_ref), (bias_in, bias_ref), (pgain_in, pgain_ref), (pbias_in, pbias_ref),
            )
        )
    ]
    for copy in copies:
        copy.start()
    for copy in copies:
        copy.wait()
    kept_ref[pl.ds(GB_ROW, 16), :] = jnp.zeros((16, NS * PILL), F32)
    lanes = pl.ds(0, 128)
    kept_ref[pl.ds(GB_ROW, LAYERS), lanes] = jnp.concatenate([gain_ref[...], bias_ref[...]], axis=1)
    kept_ref[pl.ds(GB_ROW + LAYERS, 1), lanes] = jnp.concatenate([pgain_ref[...], pbias_ref[...]], axis=1)
    kept_ref[pl.ds(TARGET_ROW, NS), pl.ds(0, PILL)] = target_lane(cell_ref[...]).astype(F32)
    w_pad[...] = jnp.zeros((128, 128), F32)
    w_pad[pl.ds(0, 9), pl.ds(0, C)] = w_ref[...]
    w_cols = jnp.transpose(w_pad[...])

    def col(j):
        return w_cols[:C, j : j + 1]

    wx = col(0) + col(4) + col(7)
    wy = col(1) + col(5) + col(8)
    wz = col(2) + col(6)
    wr = col(3)
    slot = lax.broadcasted_iota(jnp.int32, (MAXP, PILL), 0)
    total = jnp.zeros((C, 1), F32)
    number = jnp.zeros((1, 1), F32)
    for n in range(NS):
        count_i = cnt_ref[pl.ds(n, 1), :]
        count = count_i.astype(F32)
        valid = slot < count_i
        sums = []
        for j in range(4):
            p = pts_ref[pl.ds((n * 4 + j) * MAXP, MAXP), :]
            sums.append(jnp.sum(jnp.where(valid, p, 0.0), axis=0, keepdims=True))
        cell = cell_ref[pl.ds(n, 1), :]
        col_pos = jnp.bitwise_and(cell, GW - 1).astype(F32) * (2.0 / GW) - 1.0
        row_pos = jnp.right_shift(cell, 8).astype(F32) * (2.0 / GH) - 1.0
        base = -(
            col(4) * (sums[0] / count)
            + col(5) * (sums[1] / count)
            + col(6) * (sums[2] / count)
            + col(7) * col_pos
            + col(8) * row_pos
        )
        base_ref[:, pl.ds(n * PILL, PILL)] = base
        weighted = wx * sums[0] + wy * sums[1] + wz * sums[2] + wr * sums[3] + base * count
        total = total + jnp.sum(weighted, axis=1, keepdims=True)
        number = number + jnp.sum(count, axis=1, keepdims=True)
    mean = total / number
    sq_parts = []
    half = C // 2
    for c0 in (0, half):
        ch = slice(c0, c0 + half)
        bx = jnp.broadcast_to(wx[ch], (half, 128))
        by = jnp.broadcast_to(wy[ch], (half, 128))
        bz = jnp.broadcast_to(wz[ch], (half, 128))
        br = jnp.broadcast_to(wr[ch], (half, 128))
        mb = jnp.broadcast_to(mean[ch], (half, 128))

        def tile(t, sq, c0=c0, bx=bx, by=by, bz=bz, br=br, mb=mb):
            n = lax.div(t, PILL // 128)
            lanes = lanes_from((t - n * (PILL // 128)) * 128)
            base = base_ref[pl.ds(c0, half), lanes_from(t * 128)] - mb
            count = jnp.where(n == 0, cnt_ref[pl.ds(0, 1), lanes], cnt_ref[pl.ds(1, 1), lanes])

            def step(k8, carry):
                best, sq = carry
                p = [
                    pts_ref[pl.ds(pl.multiple_of((n * 4 + j) * MAXP + k8 * 8, 8), 8), lanes] for j in range(4)
                ]
                for i in range(8):
                    px, py, pz, pr = (v[i : i + 1] for v in p)
                    d = bx * px + by * py + (bz * pz + br * pr) + base
                    ok = jnp.broadcast_to(k8 * 8 + i < count, (half, 128))
                    best = jnp.where(ok, jnp.maximum(best, d), best)
                    sq = sq + jnp.where(ok, d * d, 0.0)
                return best, sq

            best, sq = lax.fori_loop(0, MAXP // 8, step, (jnp.full((half, 128), -3.0e38, F32), sq))
            kept_ref[pl.ds(c0, half), lanes_from(t * 128)] = best + mb
            return sq

        sq = lax.fori_loop(0, NS * PILL // 128, tile, jnp.zeros((half, 128), F32))
        sq_parts.append(sq)
    lane = lanes128()
    part_ref[pl.ds(0, 1), :] = to_row(
        jnp.where(lane == 0, total, 0.0), jnp.concatenate(sq_parts, axis=0)
    )
    part_ref[pl.ds(1, 1), :] = jnp.broadcast_to(number, (1, 128))


def targets_of(kept_ref, n):
    at = pl.ds(0, PILL)
    first, second = kept_ref[pl.ds(TARGET_ROW, 1), at], kept_ref[pl.ds(TARGET_ROW + 1, 1), at]
    return jnp.where(n == 0, first, second).astype(jnp.int32)


def target_lane(cell):
    row = jnp.right_shift(cell, 8)
    col = jnp.bitwise_and(cell, GW - 1)
    phase = jnp.bitwise_and(row, 1) * 2 + jnp.bitwise_and(col, 1)
    return phase * POS + jnp.right_shift(row, 1) * OW + jnp.right_shift(col, 1)


def build_onehot(oht_ref, target):
    wide = jnp.broadcast_to(target, (256, PILL))
    iota = lax.broadcasted_iota(jnp.int32, (256, PILL), 0)

    def step(t, _):
        rows = pl.ds(pl.multiple_of(t * 256, 256), 256)
        oht_ref[rows, :] = jnp.where(iota + t * 256 == wide, 1.0, 0.0).astype(BF16)
        return _

    lax.fori_loop(0, GH * GW // 256, step, 0)


def first_conv_kernel(
    g_ref, kept_ref, w_ref,
    z_ref, part_ref, ev_hi, ev_lo, od_hi, od_lo,
    oht_ref, place_ref, buf_ref,
):
    s = rows_of(g_ref, 2, 0)
    num = rows_of(g_ref, 2, 1)
    total = jnp.sum(s, axis=0, keepdims=True)
    number = jnp.sum(num, axis=0, keepdims=True)
    mean = total / number
    dev = s / num - mean
    spread = jnp.sum(num * dev * dev, axis=0, keepdims=True)
    var = (total + pltpu.roll(jnp.broadcast_to(spread, (8, 128)), C, 1)[:1]) / number
    lane_row = lax.broadcasted_iota(jnp.int32, (1, 128), 1)
    stats = columns(jnp.where(lane_row < C, mean, lax.rsqrt(var + EPS)))
    mean_c, inv_c = stats[:C], stats[C:]
    gain, bias = gain_bias(kept_ref, LAYERS)
    lane = lanes128()
    w_hi, w_lo = split(forward_weights(w_ref, buf_ref, 0))
    outer_hi = jnp.concatenate([w_hi[:C], w_hi[2 * C :]], axis=0)
    outer_lo = jnp.concatenate([w_lo[:C], w_lo[2 * C :]], axis=0)

    def sweep(n, _):
        build_onehot(oht_ref, targets_of(kept_ref, n))
        tiles = []
        for q in range(PILL // 128):
            h = kept_ref[pl.ds(0, C), lanes_from(n * PILL + q * 128)]
            tiles.append(jnp.maximum(gain * (h - mean_c) * inv_c + bias, 0.0))
        p_hi, p_lo = split(jnp.concatenate(tiles, axis=1))
        place_ref[...] = dot_nt(jnp.concatenate([p_hi, p_lo], axis=0), oht_ref[...])
        for pr, refs in ((0, (ev_hi, ev_lo)), (1, (od_hi, od_lo))):
            for part, ref in enumerate(refs):
                width = POS + pr * OW
                if pr:
                    ref[:, lanes_from(n * width)] = jnp.zeros((3 * C, OW), BF16)
                for r in range(OH):
                    even = place_ref[pl.ds(part * C, C), pl.ds(pr * 2 * POS + r * OW, OW)]
                    odd = place_ref[pl.ds(part * C, C), pl.ds((pr * 2 + 1) * POS + r * OW, OW)]
                    at = lanes_from(n * width + (r + pr) * OW)
                    ref[pl.ds(0, C), at] = from_left(odd, lane).astype(BF16)
                    ref[pl.ds(C, C), at] = even.astype(BF16)
                    ref[pl.ds(2 * C, C), at] = odd.astype(BF16)
        at = lanes_from(n * POS, POS)
        z = dot3(dot_nn, w_hi[C : 2 * C], w_lo[C : 2 * C], ev_hi[:, at], ev_lo[:, at])
        at = lanes_from(n * (POS + OW), POS + OW)
        p = dot3(dot_nn, outer_hi, outer_lo, od_hi[:, at], od_lo[:, at])
        z_ref[:, lanes_from(n * POS, POS)] = z + p[:C, :POS] + p[C:, OW:]
        return _

    each_sweep(sweep)
    store_stats(z_ref, part_ref)


def first_grad_rows(grad_of, grid_refs):
    ev_hi, ev_lo, od_hi, od_lo = grid_refs

    def sweep(n, rows):
        g_hi, g_lo = grad_of(n)
        out = []
        for row, hi, lo, start in zip(
            rows,
            (od_hi, ev_hi, od_hi),
            (od_lo, ev_lo, od_lo),
            (n * (POS + OW), n * POS, n * (POS + OW) + OW),
        ):
            at = lanes_from(start, POS)
            out.append(row + dot3(dot_nt, g_hi, g_lo, hi[:, at], lo[:, at]))
        return tuple(out)

    return each_sweep(sweep, tuple(jnp.zeros((C, 3 * C), F32) for _ in range(3)))


def first_input_sums(grid_refs):
    ev_hi, ev_lo, od_hi, od_lo = grid_refs
    one = jnp.ones((16, POS), BF16)

    def sweep(n, rows):
        out = []
        for row, hi, lo, start in zip(
            rows,
            (od_hi, ev_hi, od_hi),
            (od_lo, ev_lo, od_lo),
            (n * (POS + OW), n * POS, n * (POS + OW) + OW),
        ):
            at = lanes_from(start, POS)
            out.append(row + dot_nt(one, hi[:, at]) + dot_nt(one, lo[:, at]))
        return tuple(out)

    rows = each_sweep(sweep, tuple(jnp.zeros((16, 3 * C), F32) for _ in range(3)))
    return [jnp.broadcast_to(row[:1], (C, 3 * C)) for row in rows]


def conv_kernel(
    g_ref, z_ref, gb_ref, w_ref, out_ref, part_ref, stats_ref, s_hi, s_lo, buf_ref, *, layer
):
    stats = columns(gathered_stats(g_ref[...]))
    stats_ref[...] = stats
    mean, inv = stats[:C], stats[C:]
    gain, bias = gain_bias(gb_ref, layer - 1)
    lane = lanes128()
    zero_borders((s_hi, s_lo))
    w_hi, w_lo = split(forward_weights(w_ref, buf_ref, layer))

    def activate(at, n, r):
        y = gain * ((z_ref[:, at] - mean) * inv) + bias
        put_shifted(s_hi, s_lo, n, r, y * jax.nn.sigmoid(y), lane)

    def sweep(n, _):
        out_ref[:, lanes_from(n * POS, POS)] = conv_padded(w_hi, w_lo, s_hi, s_lo, n)
        return _

    each_row(activate)
    each_sweep(sweep)
    store_stats(out_ref, part_ref)


def turn_kernel(
    g_ref, z_ref, gb_ref, ct_ref, z0_ref, stats0_ref, ev_hi, ev_lo, od_hi, od_lo,
    feat_ref, gy_ref, keep_ref, send_ref, stats_ref,
    buf_ref,
):
    stats = columns(gathered_stats(g_ref[...]))
    stats_ref[...] = stats
    mean, inv = stats[:C], stats[C:]
    gain, bias = gain_bias(gb_ref, LAYERS - 1)
    dy = jnp.zeros((C, 128), F32)
    dx = jnp.zeros((C, 128), F32)
    for n in range(NS):
        for r in range(OH):
            at = pl.ds(n * POS + r * OW, OW)
            rows = pl.ds(n * C * OH + r, C, stride=OH)
            xhat = (z_ref[:, at] - mean) * inv
            y = gain * xhat + bias
            sg = jax.nn.sigmoid(y)
            feat_ref[rows, :] = y * sg
            gy = ct_ref[rows, :] * (sg * (1.0 + y * (1.0 - sg)))
            gy_ref[:, at] = gy
            dy = dy + gy
            dx = dx + gy * xhat
    part = to_row(dy, dx)
    keep_ref[pl.ds(0, 1), :] = part
    send_ref[pl.ds(0, 1), :] = part
    mean0, inv0 = stats0_ref[pl.ds(0, C), pl.ds(0, 1)], stats0_ref[pl.ds(C, C), pl.ds(0, 1)]
    grads = first_grad_rows(
        lambda n: split((z0_ref[:, lanes_from(n * POS, POS)] - mean0) * inv0), (ev_hi, ev_lo, od_hi, od_lo)
    )
    refs = (keep_ref, send_ref)
    none = jnp.zeros((TAP_ROWS, 128), F32)
    last = store_kernel_grad(refs, 0, grads, buf_ref)
    store_half(refs, 2, [last, none, none, none], [none] * 4)
    grads = first_input_sums((ev_hi, ev_lo, od_hi, od_lo))
    last = store_kernel_grad(refs, 1, grads, buf_ref)
    store_half(refs, 3, [last, none, none, none], [none] * 4)


def grad_scales(g, stats, gain):
    total = jnp.sum(g, axis=0, keepdims=True)
    entries = 2.0 * NPOS * g.shape[0]
    t = columns(total * (1.0 / entries))
    return gain * stats[C:], t[:C], t[C:], total


def padded_grad_rows(s_hi, s_lo, a_hi, a_lo):
    span = NS * PADW - 2 * OW
    g_at = pl.ds(OW, span)
    g_hi, g_lo = s_hi[pl.ds(C, C), g_at], s_lo[pl.ds(C, C), g_at]
    return [
        dot3(dot_nt, g_hi, g_lo, a_hi[:, pl.ds(a * OW, span)], a_lo[:, pl.ds(a * OW, span)]) for a in range(3)
    ]


def back_kernel(
    g_ref, z_ref, gy_ref, stats_ref, gb_ref, zp_ref, statsp_ref, w_ref, *refs, layer, stride
):
    if layer == 1:
        grid0, last3_ref, last2_ref, refs = refs[:4], refs[4], refs[5], refs[6:]
    gyp_ref, sums_ref, red_ref, keep_ref, send_ref, *refs = refs
    if layer != 1:
        last_ref, *refs = refs
    s_hi, s_lo, a_hi, a_lo, slope_ref, buf_ref = refs
    reduced_rows(g_ref, stride, red_ref, red_ref.shape[0])
    stats = stats_ref[...]
    mean, inv = stats[:C], stats[C:]
    gain, _ = gain_bias(gb_ref, layer)
    scale, mean_dy, mean_dx, sums_ref[...] = grad_scales(rows_of(g_ref, stride, 0), stats, gain)
    statsp = statsp_ref[...]
    meanp, invp = statsp[:C], statsp[C:]
    gainp, biasp = gain_bias(gb_ref, layer - 1)
    lane = lanes128()
    zero_borders((s_hi, s_lo, a_hi, a_lo))
    w_hi, w_lo = split(backward_weights(w_ref, buf_ref, layer))

    def turn_back(at, n, r):
        xhat = (z_ref[:, at] - mean) * inv
        gz = scale * (gy_ref[:, at] - mean_dy - xhat * mean_dx)
        put_shifted(s_hi, s_lo, n, r, gz, lane)
        y = gainp * ((zp_ref[:, at] - meanp) * invp) + biasp
        sg = jax.nn.sigmoid(y)
        slope_ref[:, at] = sg * (1.0 + y * (1.0 - sg))
        put_shifted(a_hi, a_lo, n, r, y * sg, lane)

    def sweep(n, carry):
        dy, dx = carry
        u = conv_padded(w_hi, w_lo, s_hi, s_lo, n)
        for r in range(OH):
            at = lanes_from(n * POS + r * OW)
            gy = u[:, r * OW : (r + 1) * OW] * slope_ref[:, at]
            gyp_ref[:, at] = gy
            dy = dy + gy
            dx = dx + gy * ((zp_ref[:, at] - meanp) * invp)
        return dy, dx

    each_row(turn_back)
    zero = jnp.zeros((C, 128), F32)
    dy, dx = each_sweep(sweep, (zero, zero))
    part = to_row(dy, dx)
    keep_ref[pl.ds(0, 1), :] = part
    send_ref[pl.ds(0, 1), :] = part
    refs = (keep_ref, send_ref)
    last = store_kernel_grad(refs, 0, padded_grad_rows(s_hi, s_lo, a_hi, a_lo), buf_ref)
    if layer != 1:
        last_ref[...] = last
        return
    rows = first_grad_rows(lambda n: split(gyp_ref[:, lanes_from(n * POS, POS)]), grid0)
    last0 = store_kernel_grad(refs, 1, rows, buf_ref)
    none = jnp.zeros((TAP_ROWS, 128), F32)
    store_half(refs, 2, [last0, none, none, none], [last, last2_ref[...], last3_ref[...], none])


def pick_channels(tile, pair, lane):
    row = lax.broadcasted_iota(jnp.int32, (C, 128), 0)
    want = 2 * pair + jnp.where(lane < C, 0, 1)
    return jnp.sum(jnp.where(row == want, tile, 0.0), axis=0, keepdims=True)


def own_rows_kernel(
    g_ref, stats_ref, gb_ref, first_red, red3, red2, sums1, sums2, sums3, norm_ref, out_ref, scale_ref, *, stride
):
    stats = stats_ref[...]
    gain, _ = gain_bias(gb_ref, 0)
    scale, mean_dy, mean_dx, sums0 = grad_scales(rows_of(g_ref, stride, 0), stats, gain)
    for l, row in enumerate((sums0, sums1[...], sums2[...], sums3[...])):
        norm_ref[pl.ds(l, 1), :] = row[:, C:]
        norm_ref[pl.ds(LAYERS + l, 1), :] = row[:, :C]
    for i, tile in enumerate((scale, mean_dy, mean_dx)):
        scale_ref[pl.ds(i * C, C), :] = tile
    lane = lanes128()
    count = red3.shape[0]
    peers = BLOCK // count
    spot = lax.axis_index(WIDE)

    def first_grad(raw, normed, plain, pair):
        return pick_channels(scale, pair, lane) * (
            raw - pick_channels(mean_dy, pair, lane) * plain - pick_channels(mean_dx, pair, lane) * normed
        )

    for j in range(count):
        pair = lax.rem(j * peers + spot, TAP_ROWS)
        here, raw, ends = (
            jnp.sum(rows_of(g_ref, stride, 1 + q * count + j), axis=0, keepdims=True) for q in range(3)
        )
        normed, plain, normed_end, plain_end = (first_red[pl.ds(q * count + j, 1), :] for q in range(4))
        ends = jnp.where(first_core(), first_grad(ends, normed_end, plain_end, pair), ends)
        own = (first_grad(raw, normed, plain, pair), here, red2[pl.ds(j, 1), :], red3[pl.ds(j, 1), :], ends)
        for q in range(5):
            at = pl.ds(q * count + j, peers, stride=5 * count)
            out_ref[at, :] = jnp.broadcast_to(own[q], (peers, 128))


def last_back_kernel(
    z_ref, gy_ref, stats_ref, scale_ref, kept_ref, w_ref, pg_ref, t_hi, t_lo, u_hi, oht_ref, buf_ref
):
    mean, inv = stats_ref[pl.ds(0, C), :], stats_ref[pl.ds(C, C), :]
    scale, mean_dy, mean_dx = (scale_ref[pl.ds(i * C, C), :] for i in range(3))
    lane = lanes128()
    v_hi, v_lo = split(first_backward_weights(w_ref, buf_ref))

    def sweep(n, _):
        for ref in (t_hi, t_lo):
            ref[:, pl.ds(POS, OW)] = jnp.zeros((2 * C, OW), BF16)
        for r in range(OH):
            at = lanes_from(n * POS + r * OW)
            xhat = (z_ref[:, at] - mean) * inv
            gz = scale * (gy_ref[:, at] - mean_dy - xhat * mean_dx)
            put(t_hi, t_lo, 0, r * OW, gz)
            put(t_hi, t_lo, C, r * OW, from_right(gz, lane))
        v = dot3(dot_nn, v_hi, v_lo, t_hi[...], t_lo[...])
        for pc in range(2):
            above = v[pc * C : (pc + 1) * C, OW:]
            here = v[(2 + pc) * C : (3 + pc) * C, :POS]
            below = v[(4 + pc) * C : (5 + pc) * C, :POS]
            for pr, u in ((0, here), (1, below + above)):
                at = pl.ds((pr * 2 + pc) * POS, POS)
                hi, lo = split(u)
                u_hi[pl.ds(0, C), at] = hi
                u_hi[pl.ds(C, C), at] = lo
        build_onehot(oht_ref, targets_of(kept_ref, n))
        picked = dot_nn(u_hi[...], oht_ref[...])
        pg_ref[pl.ds(pl.multiple_of(n * C, C), C), :] = picked[:C] + picked[C:]
        return _

    each_sweep(sweep)


def pair_kernel(*refs, mode, stride):
    *ins, out_ref = refs
    peers = out_ref.shape[0] // stride
    if len(ins) == 1:
        keep_ref, got_ref = ins[0].at[pl.ds(0, 8)], ins[0].at[pl.ds(8, 8)]
    else:
        keep_ref, got_ref = ins
    mine, other = keep_ref[pl.ds(0, 1), :], got_ref[pl.ds(0, 1), :]
    both = mine + other
    lane = lax.broadcasted_iota(jnp.int32, (1, 128), 1)

    def swap(v):
        return pltpu.roll(jnp.broadcast_to(v, (8, 128)), C, 1)[:1]

    if mode == "stats":
        gap = mine - other
        both = jnp.where(lane < C, 0.5 * both, both + (0.5 * NPOS) * swap(gap * gap))
    if mode == "pillars":
        m_num, o_num = keep_ref[pl.ds(1, 1), :], got_ref[pl.ds(1, 1), :]
        number = m_num + o_num
        gap = mine / m_num - other / o_num
        both = jnp.where(lane < C, both, both + (m_num * o_num / number) * swap(gap * gap))
        out_ref[pl.ds(1, peers, stride=stride), :] = jnp.broadcast_to(number, (peers, 128))
    row = jnp.broadcast_to(both, (peers, 128))
    if stride == 1:
        out_ref[...] = row
    else:
        out_ref[pl.ds(0, peers, stride=stride), :] = row
    for j, start in enumerate(range(8, keep_ref.shape[0], peers)):
        at = pl.ds(start, peers)
        out_ref[pl.ds(1 + j, peers, stride=stride), :] = keep_ref[at, :] + got_ref[at, :]


def assemble_kernel(both_ref, out_ref, *, peers):
    count = BLOCK // peers
    per_peer = (LAYERS + 1) * count

    def rows_at(core, start, size):
        return both_ref[pl.ds(core * peers * per_peer + start, size, stride=per_peer), :]

    for l in range(LAYERS):
        for j in range(count):
            for core in range(2):
                at = pl.ds((core * BLOCK + j * peers) * LAYERS + l, peers, stride=LAYERS)
                out_ref[at, :] = rows_at(core, l * count + j, peers)
        size = min(peers, TAP_ROWS)
        for step in range(0, TAP_ROWS, size):
            start = max(l - 1, 0) * TAP_ROWS + step
            rows = rows_at(min(l, 1), start % peers * per_peer + LAYERS * count + start // peers, size)
            out_ref[pl.ds((2 * BLOCK + step) * LAYERS + l, size, stride=LAYERS), :] = rows


def call(kernel, name, outs, args, scratch=(), copies=False, **params):
    specs = [pl.BlockSpec(memory_space=pltpu.HBM if copies else pltpu.VMEM)] * len(args)
    return pl.pallas_call(
        functools.partial(kernel, **params) if params else kernel,
        name=name,
        out_shape=tuple(jax.ShapeDtypeStruct(shape, dtype) for shape, dtype in outs),
        in_specs=specs,
        scratch_shapes=[pltpu.VMEM(shape, dtype) for shape, dtype in scratch]
        + [pltpu.SemaphoreType.DMA((len(args),))] * copies,
        compiler_params=None if copies else pltpu.CompilerParams(vmem_limit_bytes=20 << 20),
        interpret=INTERPRET,
    )(*args)


def partner(v):
    return lax.ppermute(v, "k", [(0, 1), (1, 0)])


def to_peers(rows, peers):
    sent = rows.reshape(peers, -1, 1, 128)
    return lax.all_to_all(sent, WIDE, 0, 0, tiled=True).reshape(-1, 128)


def exchange(name, mode, keep, peers, send=None):
    pair = (lax.all_gather(keep, "k", tiled=True),) if send is None else (keep, partner(send))
    rows = (2 if mode == "pillars" else 1) + (keep.shape[0] - 8) // peers
    (out,) = call(pair_kernel, name, [((peers * rows, 128), F32)], pair, mode=mode, stride=rows)
    return to_peers(out, peers)


def per_device(
    points, counts, cells, pfn_weight, pfn_gain, pfn_bias, conv_weight, bn_gain, bn_bias, cotangent,
    *, sizes,
):
    peers = sizes["x"] * sizes["y"] * sizes["z"]
    count = BLOCK // peers
    w = conv_weight.reshape(LAYERS, 9, TAP_ROWS, 128).transpose(1, 2, 0, 3).reshape(9 * TAP_ROWS * LAYERS, 128)
    row = ((1, 128), F32)
    rows8 = ((8, 128), F32)
    tile = ((128, 128), F32)
    plane = ((C, NPOS), F32)
    pad = ((3 * C, NS * PADW), BF16)
    buf = ((C, C), F32)
    end = ((TAP_ROWS, 128), F32)

    ints = ((NS, PILL), jnp.int32)
    vectors = [((LAYERS, C), F32)] * 2 + [((1, C), F32)] * 2
    kept, part = call(
        pfn_kernel, "pfn", [((KEPT_ROWS, NS * PILL), F32), rows8],
        (
            points.reshape(NS * 4 * MAXP, PILL), counts, cells, pfn_weight,
            bn_gain, bn_bias, pfn_gain[None], pfn_bias[None],
        ),
        [((C, NS * PILL), F32), tile, ((NS * 4 * MAXP, PILL), F32), ints, ints, ((9, C), F32)] + vectors,
        copies=True,
    )
    got = exchange("pair_p", "pillars", part, peers)
    ev = ((3 * C, NS * POS), BF16)
    od = ((3 * C, NS * (POS + OW)), BF16)
    z, part, *grid0 = call(
        first_conv_kernel, "conv0", [plane, rows8, ev, ev, od, od],
        (got, kept, w),
        [((GH * GW, PILL), BF16), ((2 * C, GH * GW), F32), buf],
    )
    pre = [z]
    stats = []
    for l in range(1, LAYERS):
        got = exchange("pair_s", "stats", part, peers)
        z, part, st = call(
            conv_kernel, f"conv{l}", [plane, rows8, tile], (got, pre[-1], kept, w), [pad, pad, buf], layer=l
        )
        pre.append(z)
        stats.append(st)
    got = exchange("pair_s", "stats", part, peers)
    slab = ((NS * C * OH, OW), F32)
    four = ((8 + 4 * BLOCK, 128), F32)
    feat, gy, keep, send, st = call(
        turn_kernel, "turn", [slab, plane, four, four, tile],
        (got, pre[-1], kept, cotangent.reshape(NS * C * OH, OW), pre[0], stats[0], *grid0), [buf],
    )
    stats.append(st)
    sums = [None] * LAYERS
    reds = []
    ends = []
    for l in range(LAYERS - 1, 0, -1):
        got = exchange("pair_g", "sums", keep, peers, send)
        blocks = got.shape[0] // peers - 1
        fresh = ((8 + (3 if l == 1 else 1) * BLOCK, 128), F32)
        gy, sums[l], red, keep, send, *last = call(
            back_kernel, f"back{l}",
            [plane, row, ((blocks, 128), F32), fresh, fresh] + [end] * (l > 1),
            (got, pre[l], gy, stats[l], kept, pre[l - 1], stats[l - 1], w) + ((*grid0, *ends) if l == 1 else ()),
            [pad, pad, pad, pad, plane, buf], layer=l, stride=blocks + 1,
        )
        reds.append(red)
        ends += last
    got = exchange("pair_z", "sums", keep, peers, send)
    rows = (LAYERS + 1) * count
    norm_grads, own, scales = call(
        own_rows_kernel, "own_rows", [((2 * LAYERS, C), F32), ((peers * rows, 128), F32), ((3 * C, 128), F32)],
        (got, stats[0], kept, *reds, *sums[1:]), stride=got.shape[0] // peers,
    )
    both = lax.all_gather(to_peers(own, peers), "k", tiled=True)
    tbuf = ((2 * C, POS + OW), BF16)
    (pillar_grad,) = call(
        last_back_kernel, "back0", [((NS * C, PILL), F32)],
        (pre[0], gy, stats[0], scales, kept, w),
        [tbuf, tbuf, ((2 * C, GH * GW), BF16), ((GH * GW, PILL), BF16), buf],
    )
    (total,) = call(
        assemble_kernel, "assemble", [((9 * TAP_ROWS * LAYERS, 128), F32)], (both,), peers=peers
    )
    total = total.reshape(9, TAP_ROWS, LAYERS, 128).transpose(2, 0, 1, 3).reshape(LAYERS, 9, C * C)
    return (
        feat.reshape(NS, C, OH, OW),
        total,
        norm_grads.reshape(2, LAYERS, C),
        pillar_grad.reshape(NS, C, PILL),
    )


def build(finer):
    sizes = dict(finer.shape)
    split4 = P(ALL, None, None, None)
    return jax.shard_map(
        functools.partial(per_device, sizes=sizes),
        mesh=finer,
        in_specs=(split4, P(ALL, None), P(ALL, None), P(), P(), P(), P(), P(), P(), split4),
        out_specs=(split4, P(), P(), P(ALL, None, None)),
        check_vma=False,
    )


def solution(mesh):
    return build(Mesh(mesh.devices.reshape(4, 2, 4, 8), ALL))
```

```python
import functools

import jax
import jax.numpy as jnp
from jax import lax
from jax.experimental import pallas as pl
from jax.experimental.pallas import tpu as pltpu
from jax.sharding import Mesh
from jax.sharding import PartitionSpec as P

C = 64
MAXP = 32
LAYERS = 4
GH = 8
GW = 256
PILL = 256
NS = 2
TAP_ROWS = C * C // 128
BLOCK = 4 * TAP_ROWS
OH = GH // 2
OW = GW // 2
POS = OH * OW
NPOS = NS * POS
PADW = (OH + 2) * OW
EPS = 1e-05
F32 = jnp.float32
BF16 = jnp.bfloat16
ALL = ("x", "k", "y", "z")
WIDE = ("x", "y", "z")
INTERPRET = False
GB_ROW = C
TARGET_ROW = C + 8
KEPT_ROWS = C + 16


def split(v):
    hi = v.astype(BF16)
    return hi, (v - hi.astype(F32)).astype(BF16)


def dot_nn(a, b):
    return lax.dot_general(a, b, (((1,), (0,)), ((), ())), preferred_element_type=F32)


def dot_nt(a, b):
    return lax.dot_general(a, b, (((1,), (1,)), ((), ())), preferred_element_type=F32)


def dot3(dot, a_hi, a_lo, b_hi, b_lo):
    m = a_hi.shape[0]
    both = dot(jnp.concatenate([a_hi, a_lo], axis=0), b_hi)
    return both[:m] + both[m:] + dot(a_hi, b_lo)


def columns(row):
    return jnp.transpose(jnp.broadcast_to(row, (128, 128)))


def to_row(top, bottom):
    return jnp.sum(jnp.transpose(jnp.concatenate([top, bottom], axis=0)), axis=0, keepdims=True)


def lanes128():
    return lax.broadcasted_iota(jnp.int32, (C, 128), 1)


def from_left(v, lane):
    return jnp.where(lane == 0, 0.0, pltpu.roll(v, 1, 1))


def from_right(v, lane):
    return jnp.where(lane == 127, 0.0, pltpu.roll(v, 127, 1))


def lanes_from(start, size=OW):
    if isinstance(start, int):
        return pl.ds(start, size)
    return pl.ds(pl.multiple_of(start, 128), size)


def each_sweep(body, init=0):
    return lax.fori_loop(0, NS, body, init)


def each_row(body):
    for t in range(NS * OH):
        body(lanes_from(t * OW), t // OH, t % OH)


def put(hi_ref, lo_ref, row, col, v):
    hi, lo = split(v)
    hi_ref[pl.ds(row, C), lanes_from(col)] = hi
    lo_ref[pl.ds(row, C), lanes_from(col)] = lo


def put_shifted(hi_ref, lo_ref, n, r, v, lane):
    col = n * PADW + (r + 1) * OW
    put(hi_ref, lo_ref, 0, col, from_left(v, lane))
    put(hi_ref, lo_ref, C, col, v)
    put(hi_ref, lo_ref, 2 * C, col, from_right(v, lane))


def zero_borders(refs):
    for ref in refs:
        for n in range(NS):
            for r in (0, OH + 1):
                ref[:, pl.ds(n * PADW + r * OW, OW)] = jnp.zeros((3 * C, OW), BF16)


def conv_padded(w_hi, w_lo, hi_ref, lo_ref, n):
    cols = lanes_from(n * PADW, PADW)
    p = dot3(dot_nn, w_hi, w_lo, hi_ref[:, cols], lo_ref[:, cols])
    return p[:C, :POS] + p[C : 2 * C, OW : OW + POS] + p[2 * C :, 2 * OW : 2 * OW + POS]


def tap_block(w_ref, buf_ref, layer, tap):
    packed = w_ref[pl.ds(tap * TAP_ROWS * LAYERS + layer, TAP_ROWS, stride=LAYERS), :]
    buf_ref[pl.ds(0, TAP_ROWS, stride=2), :] = packed[:, :C]
    buf_ref[pl.ds(1, TAP_ROWS, stride=2), :] = packed[:, C:]
    return buf_ref[...]


def forward_weights(w_ref, buf_ref, layer):
    rows = []
    for a in range(3):
        rows.append(jnp.concatenate([tap_block(w_ref, buf_ref, layer, 3 * a + b) for b in range(3)], axis=1))
    return jnp.concatenate(rows, axis=0)


def backward_weights(w_ref, buf_ref, layer):
    rows = []
    for a in range(3):
        blocks = [jnp.transpose(tap_block(w_ref, buf_ref, layer, 3 * (2 - a) + 2 - b)) for b in range(3)]
        rows.append(jnp.concatenate(blocks, axis=1))
    return jnp.concatenate(rows, axis=0)


def first_backward_weights(w_ref, buf_ref):
    rows = []
    for a in range(3):
        left, mid, right = (jnp.transpose(tap_block(w_ref, buf_ref, 0, 3 * a + b)) for b in range(3))
        rows.append(jnp.concatenate([mid, jnp.zeros((C, C), F32)], axis=1))
        rows.append(jnp.concatenate([right, left], axis=1))
    return jnp.concatenate(rows, axis=0)


def gain_bias(gb_ref, row):
    gb = columns(gb_ref[pl.ds(GB_ROW + row, 1), pl.ds(0, 128)])
    return gb[:C], gb[C:]


def first_core():
    return lax.axis_index("k") == 0


def store_half(refs, slot, mine_first, mine_second):
    keep_ref, send_ref = refs
    first = first_core()
    for t in range(4):
        at = pl.ds(8 + slot * BLOCK + t * TAP_ROWS, TAP_ROWS)
        keep_ref[at, :] = jnp.where(first, mine_first[t], mine_second[t])
        send_ref[at, :] = jnp.where(first, mine_second[t], mine_first[t])


def store_kernel_grad(refs, slot, per_row, buf_ref):
    def packed(tap):
        a, b = divmod(tap, 3)
        buf_ref[...] = per_row[a][:, b * C : (b + 1) * C]
        even = buf_ref[pl.ds(0, TAP_ROWS, stride=2), :]
        odd = buf_ref[pl.ds(1, TAP_ROWS, stride=2), :]
        return jnp.concatenate([even, odd], axis=1)

    taps = [packed(tap) for tap in range(9)]
    store_half(refs, slot, taps[:4], taps[4:8])
    return taps[8]


def rows_of(g_ref, stride, index):
    peers = g_ref.shape[0] // stride
    if stride == 1:
        return g_ref[...]
    return g_ref[pl.ds(index, peers, stride=stride), :]


def reduced_rows(g_ref, stride, red_ref, count):
    for j in range(count):
        red_ref[pl.ds(j, 1), :] = jnp.sum(rows_of(g_ref, stride, 1 + j), axis=0, keepdims=True)


def store_stats(z_ref, part_ref):
    acc = z_ref[:, pl.ds(0, 128)]
    for t in range(1, NPOS // 128):
        acc = acc + z_ref[:, pl.ds(t * 128, 128)]
    mean = jnp.sum(acc, axis=1, keepdims=True) * (1.0 / NPOS)
    sq = jnp.zeros((C, 128), F32)
    for t in range(NPOS // 128):
        d = z_ref[:, pl.ds(t * 128, 128)] - mean
        sq = sq + d * d
    lane = lax.broadcasted_iota(jnp.int32, (1, 128), 1)
    part_ref[pl.ds(0, 1), :] = to_row(acc, sq) * jnp.where(lane < C, 1.0 / NPOS, 1.0)


def gathered_stats(g):
    rows = g.shape[0]
    total = jnp.sum(g, axis=0, keepdims=True)
    mean = total * (1.0 / rows)
    dev = g - mean
    spread = jnp.sum(dev * dev, axis=0, keepdims=True)
    each = 2.0 * NPOS
    var = (total + each * pltpu.roll(jnp.broadcast_to(spread, (8, 128)), C, 1)[:1]) * (1.0 / (each * rows))
    lane = lax.broadcasted_iota(jnp.int32, (1, 128), 1)
    return jnp.where(lane < C, mean, lax.rsqrt(var + EPS))


def pfn_kernel(
    pts_in, cnt_in, cell_in, w_in, gain_in, bias_in, pgain_in, pbias_in,
    kept_ref, part_ref,
    base_ref, w_pad, pts_ref, cnt_ref, cell_ref, w_ref, gain_ref, bias_ref, pgain_ref, pbias_ref, sems,
):
    copies = [
        pltpu.make_async_copy(src, dst, sems.at[i])
        for i, (src, dst) in enumerate(
            (
                (pts_in, pts_ref), (cnt_in, cnt_ref), (cell_in, cell_ref), (w_in, w_ref),
                (gain_in, gain_ref), (bias_in, bias_ref), (pgain_in, pgain_ref), (pbias_in, pbias_ref),
            )
        )
    ]
    for copy in copies:
        copy.start()
    for copy in copies:
        copy.wait()
    kept_ref[pl.ds(GB_ROW, 16), :] = jnp.zeros((16, NS * PILL), F32)
    lanes = pl.ds(0, 128)
    kept_ref[pl.ds(GB_ROW, LAYERS), lanes] = jnp.concatenate([gain_ref[...], bias_ref[...]], axis=1)
    kept_ref[pl.ds(GB_ROW + LAYERS, 1), lanes] = jnp.concatenate([pgain_ref[...], pbias_ref[...]], axis=1)
    kept_ref[pl.ds(TARGET_ROW, NS), pl.ds(0, PILL)] = target_lane(cell_ref[...]).astype(F32)
    w_pad[...] = jnp.zeros((128, 128), F32)
    w_pad[pl.ds(0, 9), pl.ds(0, C)] = w_ref[...]
    w_cols = jnp.transpose(w_pad[...])

    def col(j):
        return w_cols[:C, j : j + 1]

    wx = col(0) + col(4) + col(7)
    wy = col(1) + col(5) + col(8)
    wz = col(2) + col(6)
    wr = col(3)
    slot = lax.broadcasted_iota(jnp.int32, (MAXP, PILL), 0)
    total = jnp.zeros((C, 1), F32)
    number = jnp.zeros((1, 1), F32)
    for n in range(NS):
        count_i = cnt_ref[pl.ds(n, 1), :]
        count = count_i.astype(F32)
        valid = slot < count_i
        sums = []
        for j in range(4):
            p = pts_ref[pl.ds((n * 4 + j) * MAXP, MAXP), :]
            sums.append(jnp.sum(jnp.where(valid, p, 0.0), axis=0, keepdims=True))
        cell = cell_ref[pl.ds(n, 1), :]
        col_pos = jnp.bitwise_and(cell, GW - 1).astype(F32) * (2.0 / GW) - 1.0
        row_pos = jnp.right_shift(cell, 8).astype(F32) * (2.0 / GH) - 1.0
        base = -(
            col(4) * (sums[0] / count)
            + col(5) * (sums[1] / count)
            + col(6) * (sums[2] / count)
            + col(7) * col_pos
            + col(8) * row_pos
        )
        base_ref[:, pl.ds(n * PILL, PILL)] = base
        weighted = wx * sums[0] + wy * sums[1] + wz * sums[2] + wr * sums[3] + base * count
        total = total + jnp.sum(weighted, axis=1, keepdims=True)
        number = number + jnp.sum(count, axis=1, keepdims=True)
    mean = total / number
    sq_parts = []
    half = C // 2
    for c0 in (0, half):
        ch = slice(c0, c0 + half)
        bx = jnp.broadcast_to(wx[ch], (half, 128))
        by = jnp.broadcast_to(wy[ch], (half, 128))
        bz = jnp.broadcast_to(wz[ch], (half, 128))
        br = jnp.broadcast_to(wr[ch], (half, 128))
        mb = jnp.broadcast_to(mean[ch], (half, 128))

        def tile(t, sq, c0=c0, bx=bx, by=by, bz=bz, br=br, mb=mb):
            n = lax.div(t, PILL // 128)
            lanes = lanes_from((t - n * (PILL // 128)) * 128)
            base = base_ref[pl.ds(c0, half), lanes_from(t * 128)] - mb
            count = jnp.where(n == 0, cnt_ref[pl.ds(0, 1), lanes], cnt_ref[pl.ds(1, 1), lanes])

            def step(k8, carry):
                best, sq = carry
                p = [
                    pts_ref[pl.ds(pl.multiple_of((n * 4 + j) * MAXP + k8 * 8, 8), 8), lanes] for j in range(4)
                ]
                for i in range(8):
                    px, py, pz, pr = (v[i : i + 1] for v in p)
                    d = bx * px + by * py + (bz * pz + br * pr) + base
                    ok = jnp.broadcast_to(k8 * 8 + i < count, (half, 128))
                    best = jnp.where(ok, jnp.maximum(best, d), best)
                    sq = sq + jnp.where(ok, d * d, 0.0)
                return best, sq

            best, sq = lax.fori_loop(0, MAXP // 8, step, (jnp.full((half, 128), -3.0e38, F32), sq))
            kept_ref[pl.ds(c0, half), lanes_from(t * 128)] = best + mb
            return sq

        sq = lax.fori_loop(0, NS * PILL // 128, tile, jnp.zeros((half, 128), F32))
        sq_parts.append(sq)
    lane = lanes128()
    part_ref[pl.ds(0, 1), :] = to_row(
        jnp.where(lane == 0, total, 0.0), jnp.concatenate(sq_parts, axis=0)
    )
    part_ref[pl.ds(1, 1), :] = jnp.broadcast_to(number, (1, 128))


def targets_of(kept_ref, n):
    at = pl.ds(0, PILL)
    first, second = kept_ref[pl.ds(TARGET_ROW, 1), at], kept_ref[pl.ds(TARGET_ROW + 1, 1), at]
    return jnp.where(n == 0, first, second).astype(jnp.int32)


def target_lane(cell):
    row = jnp.right_shift(cell, 8)
    col = jnp.bitwise_and(cell, GW - 1)
    phase = jnp.bitwise_and(row, 1) * 2 + jnp.bitwise_and(col, 1)
    return phase * POS + jnp.right_shift(row, 1) * OW + jnp.right_shift(col, 1)


def build_onehot(oht_ref, target):
    wide = jnp.broadcast_to(target, (256, PILL))
    iota = lax.broadcasted_iota(jnp.int32, (256, PILL), 0)

    def step(t, _):
        rows = pl.ds(pl.multiple_of(t * 256, 256), 256)
        oht_ref[rows, :] = jnp.where(iota + t * 256 == wide, 1.0, 0.0).astype(BF16)
        return _

    lax.fori_loop(0, GH * GW // 256, step, 0)


def first_conv_kernel(
    g_ref, kept_ref, w_ref,
    z_ref, part_ref, ev_hi, ev_lo, od_hi, od_lo,
    oht_ref, place_ref, buf_ref,
):
    s = rows_of(g_ref, 2, 0)
    num = rows_of(g_ref, 2, 1)
    total = jnp.sum(s, axis=0, keepdims=True)
    number = jnp.sum(num, axis=0, keepdims=True)
    mean = total / number
    dev = s / num - mean
    spread = jnp.sum(num * dev * dev, axis=0, keepdims=True)
    var = (total + pltpu.roll(jnp.broadcast_to(spread, (8, 128)), C, 1)[:1]) / number
    lane_row = lax.broadcasted_iota(jnp.int32, (1, 128), 1)
    stats = columns(jnp.where(lane_row < C, mean, lax.rsqrt(var + EPS)))
    mean_c, inv_c = stats[:C], stats[C:]
    gain, bias = gain_bias(kept_ref, LAYERS)
    lane = lanes128()
    w_hi, w_lo = split(forward_weights(w_ref, buf_ref, 0))
    outer_hi = jnp.concatenate([w_hi[:C], w_hi[2 * C :]], axis=0)
    outer_lo = jnp.concatenate([w_lo[:C], w_lo[2 * C :]], axis=0)

    def sweep(n, _):
        build_onehot(oht_ref, targets_of(kept_ref, n))
        tiles = []
        for q in range(PILL // 128):
            h = kept_ref[pl.ds(0, C), lanes_from(n * PILL + q * 128)]
            tiles.append(jnp.maximum(gain * (h - mean_c) * inv_c + bias, 0.0))
        p_hi, p_lo = split(jnp.concatenate(tiles, axis=1))
        place_ref[...] = dot_nt(jnp.concatenate([p_hi, p_lo], axis=0), oht_ref[...])
        for pr, refs in ((0, (ev_hi, ev_lo)), (1, (od_hi, od_lo))):
            for part, ref in enumerate(refs):
                width = POS + pr * OW
                if pr:
                    ref[:, lanes_from(n * width)] = jnp.zeros((3 * C, OW), BF16)
                for r in range(OH):
                    even = place_ref[pl.ds(part * C, C), pl.ds(pr * 2 * POS + r * OW, OW)]
                    odd = place_ref[pl.ds(part * C, C), pl.ds((pr * 2 + 1) * POS + r * OW, OW)]
                    at = lanes_from(n * width + (r + pr) * OW)
                    ref[pl.ds(0, C), at] = from_left(odd, lane).astype(BF16)
                    ref[pl.ds(C, C), at] = even.astype(BF16)
                    ref[pl.ds(2 * C, C), at] = odd.astype(BF16)
        at = lanes_from(n * POS, POS)
        z = dot3(dot_nn, w_hi[C : 2 * C], w_lo[C : 2 * C], ev_hi[:, at], ev_lo[:, at])
        at = lanes_from(n * (POS + OW), POS + OW)
        p = dot3(dot_nn, outer_hi, outer_lo, od_hi[:, at], od_lo[:, at])
        z_ref[:, lanes_from(n * POS, POS)] = z + p[:C, :POS] + p[C:, OW:]
        return _

    each_sweep(sweep)
    store_stats(z_ref, part_ref)


def first_grad_rows(grad_of, grid_refs, extra=0):
    ev_hi, ev_lo, od_hi, od_lo = grid_refs
    ones = [jnp.ones((extra, POS), BF16)] * (extra > 0)

    def sweep(n, rows):
        g_hi, g_lo = grad_of(n)
        whole = jnp.concatenate([g_hi, g_lo, *ones], axis=0)
        upper = jnp.concatenate([g_hi, *ones], axis=0) if extra else g_hi
        out = []
        for row, hi, lo, start in zip(
            rows,
            (od_hi, ev_hi, od_hi),
            (od_lo, ev_lo, od_lo),
            (n * (POS + OW), n * POS, n * (POS + OW) + OW),
        ):
            at = lanes_from(start, POS)
            high = dot_nt(whole, hi[:, at])
            both = jnp.concatenate([high[:C] + high[C : 2 * C], high[2 * C :]], axis=0) if extra else high[:C] + high[C:]
            out.append(row + both + dot_nt(upper, lo[:, at]))
        return tuple(out)

    return each_sweep(sweep, tuple(jnp.zeros((C + extra, 3 * C), F32) for _ in range(3)))


def conv_kernel(
    g_ref, z_ref, gb_ref, w_ref, out_ref, part_ref, stats_ref, s_hi, s_lo, buf_ref, *, layer
):
    stats = columns(gathered_stats(g_ref[...]))
    stats_ref[...] = stats
    mean, inv = stats[:C], stats[C:]
    gain, bias = gain_bias(gb_ref, layer - 1)
    lane = lanes128()
    zero_borders((s_hi, s_lo))
    w_hi, w_lo = split(forward_weights(w_ref, buf_ref, layer))

    def activate(at, n, r):
        y = gain * ((z_ref[:, at] - mean) * inv) + bias
        put_shifted(s_hi, s_lo, n, r, y * jax.nn.sigmoid(y), lane)

    def sweep(n, _):
        out_ref[:, lanes_from(n * POS, POS)] = conv_padded(w_hi, w_lo, s_hi, s_lo, n)
        return _

    each_row(activate)
    each_sweep(sweep)
    store_stats(out_ref, part_ref)


def turn_kernel(
    g_ref, z_ref, gb_ref, ct_ref, z0_ref, stats0_ref, ev_hi, ev_lo, od_hi, od_lo,
    feat_ref, gy_ref, keep_ref, send_ref, stats_ref,
    buf_ref,
):
    stats = columns(gathered_stats(g_ref[...]))
    stats_ref[...] = stats
    mean, inv = stats[:C], stats[C:]
    gain, bias = gain_bias(gb_ref, LAYERS - 1)
    dy = jnp.zeros((C, 128), F32)
    dx = jnp.zeros((C, 128), F32)
    for n in range(NS):
        for r in range(OH):
            at = pl.ds(n * POS + r * OW, OW)
            rows = pl.ds(n * C * OH + r, C, stride=OH)
            xhat = (z_ref[:, at] - mean) * inv
            y = gain * xhat + bias
            sg = jax.nn.sigmoid(y)
            feat_ref[rows, :] = y * sg
            gy = ct_ref[rows, :] * (sg * (1.0 + y * (1.0 - sg)))
            gy_ref[:, at] = gy
            dy = dy + gy
            dx = dx + gy * xhat
    part = to_row(dy, dx)
    keep_ref[pl.ds(0, 1), :] = part
    send_ref[pl.ds(0, 1), :] = part
    mean0, inv0 = stats0_ref[pl.ds(0, C), pl.ds(0, 1)], stats0_ref[pl.ds(C, C), pl.ds(0, 1)]
    grads = first_grad_rows(
        lambda n: split((z0_ref[:, lanes_from(n * POS, POS)] - mean0) * inv0), (ev_hi, ev_lo, od_hi, od_lo), 16
    )
    refs = (keep_ref, send_ref)
    none = jnp.zeros((TAP_ROWS, 128), F32)
    last = store_kernel_grad(refs, 0, [row[:C] for row in grads], buf_ref)
    sums = [jnp.broadcast_to(row[C : C + 1], (C, 3 * C)) for row in grads]
    last_sums = store_kernel_grad(refs, 1, sums, buf_ref)
    store_half(refs, 2, [last, last_sums, none, none], [none] * 4)


def grad_scales(g, stats, gain):
    total = jnp.sum(g, axis=0, keepdims=True)
    entries = 2.0 * NPOS * g.shape[0]
    t = columns(total * (1.0 / entries))
    return gain * stats[C:], t[:C], t[C:], total


def padded_grad_rows(s_hi, s_lo, a_hi, a_lo):
    span = NS * PADW - 2 * OW
    g_at = pl.ds(OW, span)
    g_hi, g_lo = s_hi[pl.ds(C, C), g_at], s_lo[pl.ds(C, C), g_at]
    return [
        dot3(dot_nt, g_hi, g_lo, a_hi[:, pl.ds(a * OW, span)], a_lo[:, pl.ds(a * OW, span)]) for a in range(3)
    ]


def back_kernel(
    g_ref, z_ref, gy_ref, stats_ref, gb_ref, zp_ref, statsp_ref, w_ref, *refs, layer, stride
):
    if layer == 1:
        grid0, last3_ref, last2_ref, refs = refs[:4], refs[4], refs[5], refs[6:]
    gyp_ref, sums_ref, red_ref, keep_ref, send_ref, *refs = refs
    if layer != 1:
        last_ref, *refs = refs
    s_hi, s_lo, a_hi, a_lo, slope_ref, buf_ref = refs
    reduced_rows(g_ref, stride, red_ref, red_ref.shape[0])
    stats = stats_ref[...]
    mean, inv = stats[:C], stats[C:]
    gain, _ = gain_bias(gb_ref, layer)
    scale, mean_dy, mean_dx, sums_ref[...] = grad_scales(rows_of(g_ref, stride, 0), stats, gain)
    statsp = statsp_ref[...]
    meanp, invp = statsp[:C], statsp[C:]
    gainp, biasp = gain_bias(gb_ref, layer - 1)
    lane = lanes128()
    zero_borders((s_hi, s_lo, a_hi, a_lo))
    w_hi, w_lo = split(backward_weights(w_ref, buf_ref, layer))

    def turn_back(at, n, r):
        xhat = (z_ref[:, at] - mean) * inv
        gz = scale * (gy_ref[:, at] - mean_dy - xhat * mean_dx)
        put_shifted(s_hi, s_lo, n, r, gz, lane)
        y = gainp * ((zp_ref[:, at] - meanp) * invp) + biasp
        sg = jax.nn.sigmoid(y)
        slope_ref[:, at] = sg * (1.0 + y * (1.0 - sg))
        put_shifted(a_hi, a_lo, n, r, y * sg, lane)

    def sweep(n, carry):
        dy, dx = carry
        u = conv_padded(w_hi, w_lo, s_hi, s_lo, n)
        for r in range(OH):
            at = lanes_from(n * POS + r * OW)
            gy = u[:, r * OW : (r + 1) * OW] * slope_ref[:, at]
            gyp_ref[:, at] = gy
            dy = dy + gy
            dx = dx + gy * ((zp_ref[:, at] - meanp) * invp)
        return dy, dx

    each_row(turn_back)
    zero = jnp.zeros((C, 128), F32)
    dy, dx = each_sweep(sweep, (zero, zero))
    part = to_row(dy, dx)
    keep_ref[pl.ds(0, 1), :] = part
    send_ref[pl.ds(0, 1), :] = part
    refs = (keep_ref, send_ref)
    last = store_kernel_grad(refs, 0, padded_grad_rows(s_hi, s_lo, a_hi, a_lo), buf_ref)
    if layer != 1:
        last_ref[...] = last
        return
    rows = first_grad_rows(lambda n: split(gyp_ref[:, lanes_from(n * POS, POS)]), grid0)
    last0 = store_kernel_grad(refs, 1, rows, buf_ref)
    none = jnp.zeros((TAP_ROWS, 128), F32)
    store_half(refs, 2, [last0, none, none, none], [last, last2_ref[...], last3_ref[...], none])


def pick_channels(tile, pair, lane):
    row = lax.broadcasted_iota(jnp.int32, (C, 128), 0)
    want = 2 * pair + jnp.where(lane < C, 0, 1)
    return jnp.sum(jnp.where(row == want, tile, 0.0), axis=0, keepdims=True)


def own_rows_kernel(
    g_ref, stats_ref, gb_ref, first_red, red3, red2, sums1, sums2, sums3, norm_ref, out_ref, scale_ref, *, stride
):
    stats = stats_ref[...]
    gain, _ = gain_bias(gb_ref, 0)
    scale, mean_dy, mean_dx, sums0 = grad_scales(rows_of(g_ref, stride, 0), stats, gain)
    for l, row in enumerate((sums0, sums1[...], sums2[...], sums3[...])):
        norm_ref[pl.ds(l, 1), :] = row[:, C:]
        norm_ref[pl.ds(LAYERS + l, 1), :] = row[:, :C]
    for i, tile in enumerate((scale, mean_dy, mean_dx)):
        scale_ref[pl.ds(i * C, C), :] = tile
    lane = lanes128()
    count = red3.shape[0]
    peers = BLOCK // count
    spot = lax.axis_index(WIDE)

    def first_grad(raw, normed, plain, pair):
        return pick_channels(scale, pair, lane) * (
            raw - pick_channels(mean_dy, pair, lane) * plain - pick_channels(mean_dx, pair, lane) * normed
        )

    for j in range(count):
        pair = lax.rem(j * peers + spot, TAP_ROWS)
        here, raw, ends = (
            jnp.sum(rows_of(g_ref, stride, 1 + q * count + j), axis=0, keepdims=True) for q in range(3)
        )
        normed, plain, end = (first_red[pl.ds(q * count + j, 1), :] for q in range(3))
        plain_peer = lax.div(j * peers + spot, TAP_ROWS) == 1
        end_grad = pick_channels(scale, pair, lane) * (
            ends - pick_channels(jnp.where(plain_peer, mean_dy, mean_dx), pair, lane) * end
        )
        ends = jnp.where(first_core(), end_grad, ends)
        own = (first_grad(raw, normed, plain, pair), here, red2[pl.ds(j, 1), :], red3[pl.ds(j, 1), :], ends)
        for q in range(5):
            at = pl.ds(q * count + j, peers, stride=5 * count)
            out_ref[at, :] = jnp.broadcast_to(own[q], (peers, 128))


def last_back_kernel(
    z_ref, gy_ref, stats_ref, scale_ref, kept_ref, w_ref, pg_ref, t_hi, t_lo, u_hi, oht_ref, buf_ref
):
    mean, inv = stats_ref[pl.ds(0, C), :], stats_ref[pl.ds(C, C), :]
    scale, mean_dy, mean_dx = (scale_ref[pl.ds(i * C, C), :] for i in range(3))
    lane = lanes128()
    v_hi, v_lo = split(first_backward_weights(w_ref, buf_ref))

    def sweep(n, _):
        for ref in (t_hi, t_lo):
            ref[:, pl.ds(POS, OW)] = jnp.zeros((2 * C, OW), BF16)
        for r in range(OH):
            at = lanes_from(n * POS + r * OW)
            xhat = (z_ref[:, at] - mean) * inv
            gz = scale * (gy_ref[:, at] - mean_dy - xhat * mean_dx)
            put(t_hi, t_lo, 0, r * OW, gz)
            put(t_hi, t_lo, C, r * OW, from_right(gz, lane))
        v = dot3(dot_nn, v_hi, v_lo, t_hi[...], t_lo[...])
        for pc in range(2):
            above = v[pc * C : (pc + 1) * C, OW:]
            here = v[(2 + pc) * C : (3 + pc) * C, :POS]
            below = v[(4 + pc) * C : (5 + pc) * C, :POS]
            for pr, u in ((0, here), (1, below + above)):
                at = pl.ds((pr * 2 + pc) * POS, POS)
                hi, lo = split(u)
                u_hi[pl.ds(0, C), at] = hi
                u_hi[pl.ds(C, C), at] = lo
        build_onehot(oht_ref, targets_of(kept_ref, n))
        picked = dot_nn(u_hi[...], oht_ref[...])
        pg_ref[pl.ds(pl.multiple_of(n * C, C), C), :] = picked[:C] + picked[C:]
        return _

    each_sweep(sweep)


def pair_kernel(*refs, mode, stride):
    *ins, out_ref = refs
    peers = out_ref.shape[0] // stride
    if len(ins) == 1:
        keep_ref, got_ref = ins[0].at[pl.ds(0, 8)], ins[0].at[pl.ds(8, 8)]
    else:
        keep_ref, got_ref = ins
    mine, other = keep_ref[pl.ds(0, 1), :], got_ref[pl.ds(0, 1), :]
    both = mine + other
    lane = lax.broadcasted_iota(jnp.int32, (1, 128), 1)

    def swap(v):
        return pltpu.roll(jnp.broadcast_to(v, (8, 128)), C, 1)[:1]

    if mode == "stats":
        gap = mine - other
        both = jnp.where(lane < C, 0.5 * both, both + (0.5 * NPOS) * swap(gap * gap))
    if mode == "pillars":
        m_num, o_num = keep_ref[pl.ds(1, 1), :], got_ref[pl.ds(1, 1), :]
        number = m_num + o_num
        gap = mine / m_num - other / o_num
        both = jnp.where(lane < C, both, both + (m_num * o_num / number) * swap(gap * gap))
        out_ref[pl.ds(1, peers, stride=stride), :] = jnp.broadcast_to(number, (peers, 128))
    row = jnp.broadcast_to(both, (peers, 128))
    if stride == 1:
        out_ref[...] = row
    else:
        out_ref[pl.ds(0, peers, stride=stride), :] = row
    for j, start in enumerate(range(8, keep_ref.shape[0], peers)):
        at = pl.ds(start, peers)
        out_ref[pl.ds(1 + j, peers, stride=stride), :] = keep_ref[at, :] + got_ref[at, :]


def assemble_kernel(both_ref, out_ref, *, peers):
    count = BLOCK // peers
    per_peer = (LAYERS + 1) * count

    def rows_at(core, start, size):
        return both_ref[pl.ds(core * peers * per_peer + start, size, stride=per_peer), :]

    for l in range(LAYERS):
        for j in range(count):
            for core in range(2):
                at = pl.ds((core * BLOCK + j * peers) * LAYERS + l, peers, stride=LAYERS)
                out_ref[at, :] = rows_at(core, l * count + j, peers)
        size = min(peers, TAP_ROWS)
        for step in range(0, TAP_ROWS, size):
            start = max(l - 1, 0) * TAP_ROWS + step
            rows = rows_at(min(l, 1), start % peers * per_peer + LAYERS * count + start // peers, size)
            if l == 0:
                start += TAP_ROWS
                rows = rows + rows_at(0, start % peers * per_peer + LAYERS * count + start // peers, size)
            out_ref[pl.ds((2 * BLOCK + step) * LAYERS + l, size, stride=LAYERS), :] = rows


def call(kernel, name, outs, args, scratch=(), copies=False, **params):
    specs = [pl.BlockSpec(memory_space=pltpu.HBM if copies else pltpu.VMEM)] * len(args)
    return pl.pallas_call(
        functools.partial(kernel, **params) if params else kernel,
        name=name,
        out_shape=tuple(jax.ShapeDtypeStruct(shape, dtype) for shape, dtype in outs),
        in_specs=specs,
        scratch_shapes=[pltpu.VMEM(shape, dtype) for shape, dtype in scratch]
        + [pltpu.SemaphoreType.DMA((len(args),))] * copies,
        compiler_params=None if copies else pltpu.CompilerParams(vmem_limit_bytes=20 << 20),
        interpret=INTERPRET,
    )(*args)


def partner(v):
    return lax.ppermute(v, "k", [(0, 1), (1, 0)])


def to_peers(rows, peers):
    sent = rows.reshape(peers, -1, 1, 128)
    return lax.all_to_all(sent, WIDE, 0, 0, tiled=True).reshape(-1, 128)


def exchange(name, mode, keep, peers, send=None):
    pair = (lax.all_gather(keep, "k", tiled=True),) if send is None else (keep, partner(send))
    rows = (2 if mode == "pillars" else 1) + (keep.shape[0] - 8) // peers
    (out,) = call(pair_kernel, name, [((peers * rows, 128), F32)], pair, mode=mode, stride=rows)
    return to_peers(out, peers)


def per_device(
    points, counts, cells, pfn_weight, pfn_gain, pfn_bias, conv_weight, bn_gain, bn_bias, cotangent,
    *, sizes,
):
    peers = sizes["x"] * sizes["y"] * sizes["z"]
    count = BLOCK // peers
    w = conv_weight.reshape(LAYERS, 9, TAP_ROWS, 128).transpose(1, 2, 0, 3).reshape(9 * TAP_ROWS * LAYERS, 128)
    row = ((1, 128), F32)
    rows8 = ((8, 128), F32)
    tile = ((128, 128), F32)
    plane = ((C, NPOS), F32)
    pad = ((3 * C, NS * PADW), BF16)
    buf = ((C, C), F32)
    end = ((TAP_ROWS, 128), F32)

    ints = ((NS, PILL), jnp.int32)
    vectors = [((LAYERS, C), F32)] * 2 + [((1, C), F32)] * 2
    kept, part = call(
        pfn_kernel, "pfn", [((KEPT_ROWS, NS * PILL), F32), rows8],
        (
            points.reshape(NS * 4 * MAXP, PILL), counts, cells, pfn_weight,
            bn_gain, bn_bias, pfn_gain[None], pfn_bias[None],
        ),
        [((C, NS * PILL), F32), tile, ((NS * 4 * MAXP, PILL), F32), ints, ints, ((9, C), F32)] + vectors,
        copies=True,
    )
    got = exchange("pair_p", "pillars", part, peers)
    ev = ((3 * C, NS * POS), BF16)
    od = ((3 * C, NS * (POS + OW)), BF16)
    z, part, *grid0 = call(
        first_conv_kernel, "conv0", [plane, rows8, ev, ev, od, od],
        (got, kept, w),
        [((GH * GW, PILL), BF16), ((2 * C, GH * GW), F32), buf],
    )
    pre = [z]
    stats = []
    for l in range(1, LAYERS):
        got = exchange("pair_s", "stats", part, peers, part if l == 1 else None)
        z, part, st = call(
            conv_kernel, f"conv{l}", [plane, rows8, tile], (got, pre[-1], kept, w), [pad, pad, buf], layer=l
        )
        pre.append(z)
        stats.append(st)
    got = exchange("pair_s", "stats", part, peers)
    slab = ((NS * C * OH, OW), F32)
    three = ((8 + 3 * BLOCK, 128), F32)
    feat, gy, keep, send, st = call(
        turn_kernel, "turn", [slab, plane, three, three, tile],
        (got, pre[-1], kept, cotangent.reshape(NS * C * OH, OW), pre[0], stats[0], *grid0), [buf],
    )
    stats.append(st)
    sums = [None] * LAYERS
    reds = []
    ends = []
    for l in range(LAYERS - 1, 0, -1):
        got = exchange("pair_g", "sums", keep, peers, send)
        blocks = got.shape[0] // peers - 1
        fresh = ((8 + (3 if l == 1 else 1) * BLOCK, 128), F32)
        gy, sums[l], red, keep, send, *last = call(
            back_kernel, f"back{l}",
            [plane, row, ((blocks, 128), F32), fresh, fresh] + [end] * (l > 1),
            (got, pre[l], gy, stats[l], kept, pre[l - 1], stats[l - 1], w) + ((*grid0, *ends) if l == 1 else ()),
            [pad, pad, pad, pad, plane, buf], layer=l, stride=blocks + 1,
        )
        reds.append(red)
        ends += last
    got = exchange("pair_z", "sums", keep, peers, send)
    rows = (LAYERS + 1) * count
    norm_grads, own, scales = call(
        own_rows_kernel, "own_rows", [((2 * LAYERS, C), F32), ((peers * rows, 128), F32), ((3 * C, 128), F32)],
        (got, stats[0], kept, *reds, *sums[1:]), stride=got.shape[0] // peers,
    )
    both = lax.all_gather(to_peers(own, peers), "k", tiled=True)
    tbuf = ((2 * C, POS + OW), BF16)
    (pillar_grad,) = call(
        last_back_kernel, "back0", [((NS * C, PILL), F32)],
        (pre[0], gy, stats[0], scales, kept, w),
        [tbuf, tbuf, ((2 * C, GH * GW), BF16), ((GH * GW, PILL), BF16), buf],
    )
    (total,) = call(
        assemble_kernel, "assemble", [((9 * TAP_ROWS * LAYERS, 128), F32)], (both,), peers=peers
    )
    total = total.reshape(9, TAP_ROWS, LAYERS, 128).transpose(2, 0, 1, 3).reshape(LAYERS, 9, C * C)
    return (
        feat.reshape(NS, C, OH, OW),
        total,
        norm_grads.reshape(2, LAYERS, C),
        pillar_grad.reshape(NS, C, PILL),
    )


def build(finer):
    sizes = dict(finer.shape)
    split4 = P(ALL, None, None, None)
    return jax.shard_map(
        functools.partial(per_device, sizes=sizes),
        mesh=finer,
        in_specs=(split4, P(ALL, None), P(ALL, None), P(), P(), P(), P(), P(), P(), split4),
        out_specs=(split4, P(), P(), P(ALL, None, None)),
        check_vma=False,
    )


def solution(mesh):
    return build(Mesh(mesh.devices.reshape(4, 2, 4, 8), ALL))
```

```python
import functools

import jax
import jax.numpy as jnp
from jax import lax
from jax.experimental import pallas as pl
from jax.experimental.pallas import tpu as pltpu
from jax.sharding import Mesh
from jax.sharding import PartitionSpec as P

C = 64
MAXP = 32
LAYERS = 4
GH = 8
GW = 256
PILL = 256
NS = 2
TAP_ROWS = C * C // 128
BLOCK = 4 * TAP_ROWS
OH = GH // 2
OW = GW // 2
POS = OH * OW
NPOS = NS * POS
PADW = (OH + 2) * OW
EPS = 1e-05
F32 = jnp.float32
BF16 = jnp.bfloat16
ALL = ("x", "k", "y", "z")
WIDE = ("x", "y", "z")
INTERPRET = False
GB_ROW = C
TARGET_ROW = C + 8
KEPT_ROWS = C + 16


def split(v):
    hi = v.astype(BF16)
    return hi, (v - hi.astype(F32)).astype(BF16)


def dot_nn(a, b):
    return lax.dot_general(a, b, (((1,), (0,)), ((), ())), preferred_element_type=F32)


def dot_nt(a, b):
    return lax.dot_general(a, b, (((1,), (1,)), ((), ())), preferred_element_type=F32)


def dot3(dot, a_hi, a_lo, b_hi, b_lo):
    m = a_hi.shape[0]
    both = dot(jnp.concatenate([a_hi, a_lo], axis=0), b_hi)
    return both[:m] + both[m:] + dot(a_hi, b_lo)


def columns(row):
    return jnp.transpose(jnp.broadcast_to(row, (128, 128)))


def to_row(top, bottom):
    return jnp.sum(jnp.transpose(jnp.concatenate([top, bottom], axis=0)), axis=0, keepdims=True)


def lanes128():
    return lax.broadcasted_iota(jnp.int32, (C, 128), 1)


def from_left(v, lane):
    return jnp.where(lane == 0, 0.0, pltpu.roll(v, 1, 1))


def from_right(v, lane):
    return jnp.where(lane == 127, 0.0, pltpu.roll(v, 127, 1))


def lanes_from(start, size=OW):
    if isinstance(start, int):
        return pl.ds(start, size)
    return pl.ds(pl.multiple_of(start, 128), size)


def each_sweep(body, init=0):
    return lax.fori_loop(0, NS, body, init)


def each_row(body):
    for t in range(NS * OH):
        body(lanes_from(t * OW), t // OH, t % OH)


def put(hi_ref, lo_ref, row, col, v):
    hi, lo = split(v)
    hi_ref[pl.ds(row, C), lanes_from(col)] = hi
    lo_ref[pl.ds(row, C), lanes_from(col)] = lo


def put_shifted(hi_ref, lo_ref, n, r, v, lane):
    col = n * PADW + (r + 1) * OW
    put(hi_ref, lo_ref, 0, col, from_left(v, lane))
    put(hi_ref, lo_ref, C, col, v)
    put(hi_ref, lo_ref, 2 * C, col, from_right(v, lane))


def zero_borders(refs):
    for ref in refs:
        for n in range(NS):
            for r in (0, OH + 1):
                ref[:, pl.ds(n * PADW + r * OW, OW)] = jnp.zeros((3 * C, OW), BF16)


def conv_padded(w_hi, w_lo, hi_ref, lo_ref, n):
    cols = lanes_from(n * PADW, PADW)
    p = dot3(dot_nn, w_hi, w_lo, hi_ref[:, cols], lo_ref[:, cols])
    return p[:C, :POS] + p[C : 2 * C, OW : OW + POS] + p[2 * C :, 2 * OW : 2 * OW + POS]


def tap_block(w_ref, buf_ref, layer, tap):
    packed = w_ref[pl.ds(tap * TAP_ROWS * LAYERS + layer, TAP_ROWS, stride=LAYERS), :]
    buf_ref[pl.ds(0, TAP_ROWS, stride=2), :] = packed[:, :C]
    buf_ref[pl.ds(1, TAP_ROWS, stride=2), :] = packed[:, C:]
    return buf_ref[...]


def forward_weights(w_ref, buf_ref, layer):
    rows = []
    for a in range(3):
        rows.append(jnp.concatenate([tap_block(w_ref, buf_ref, layer, 3 * a + b) for b in range(3)], axis=1))
    return jnp.concatenate(rows, axis=0)


def backward_weights(w_ref, buf_ref, layer):
    rows = []
    for a in range(3):
        blocks = [jnp.transpose(tap_block(w_ref, buf_ref, layer, 3 * (2 - a) + 2 - b)) for b in range(3)]
        rows.append(jnp.concatenate(blocks, axis=1))
    return jnp.concatenate(rows, axis=0)


def first_backward_weights(w_ref, buf_ref):
    rows = []
    for a in range(3):
        left, mid, right = (jnp.transpose(tap_block(w_ref, buf_ref, 0, 3 * a + b)) for b in range(3))
        rows.append(jnp.concatenate([mid, jnp.zeros((C, C), F32)], axis=1))
        rows.append(jnp.concatenate([right, left], axis=1))
    return jnp.concatenate(rows, axis=0)


def gain_bias(gb_ref, row):
    gb = columns(gb_ref[pl.ds(GB_ROW + row, 1), pl.ds(0, 128)])
    return gb[:C], gb[C:]


def first_core():
    return lax.axis_index("k") == 0


def store_half(refs, slot, mine_first, mine_second):
    keep_ref, send_ref = refs
    first = first_core()
    for t in range(4):
        at = pl.ds(8 + slot * BLOCK + t * TAP_ROWS, TAP_ROWS)
        keep_ref[at, :] = jnp.where(first, mine_first[t], mine_second[t])
        send_ref[at, :] = jnp.where(first, mine_second[t], mine_first[t])


def store_kernel_grad(refs, slot, per_row, buf_ref):
    def packed(tap):
        a, b = divmod(tap, 3)
        buf_ref[...] = per_row[a][:, b * C : (b + 1) * C]
        even = buf_ref[pl.ds(0, TAP_ROWS, stride=2), :]
        odd = buf_ref[pl.ds(1, TAP_ROWS, stride=2), :]
        return jnp.concatenate([even, odd], axis=1)

    taps = [packed(tap) for tap in range(9)]
    store_half(refs, slot, taps[:4], taps[4:8])
    return taps[8]


def rows_of(g_ref, stride, index):
    peers = g_ref.shape[0] // stride
    if stride == 1:
        return g_ref[...]
    return g_ref[pl.ds(index, peers, stride=stride), :]


def reduced_rows(g_ref, stride, red_ref, count):
    for j in range(count):
        red_ref[pl.ds(j, 1), :] = jnp.sum(rows_of(g_ref, stride, 1 + j), axis=0, keepdims=True)


def store_stats(z_ref, part_ref):
    acc = z_ref[:, pl.ds(0, 128)]
    for t in range(1, NPOS // 128):
        acc = acc + z_ref[:, pl.ds(t * 128, 128)]
    mean = jnp.sum(acc, axis=1, keepdims=True) * (1.0 / NPOS)
    sq = jnp.zeros((C, 128), F32)
    for t in range(NPOS // 128):
        d = z_ref[:, pl.ds(t * 128, 128)] - mean
        sq = sq + d * d
    lane = lax.broadcasted_iota(jnp.int32, (1, 128), 1)
    part_ref[pl.ds(0, 1), :] = to_row(acc, sq) * jnp.where(lane < C, 1.0 / NPOS, 1.0)


def gathered_stats(g):
    rows = g.shape[0]
    total = jnp.sum(g, axis=0, keepdims=True)
    mean = total * (1.0 / rows)
    dev = g - mean
    spread = jnp.sum(dev * dev, axis=0, keepdims=True)
    each = 2.0 * NPOS
    var = (total + each * pltpu.roll(jnp.broadcast_to(spread, (8, 128)), C, 1)[:1]) * (1.0 / (each * rows))
    lane = lax.broadcasted_iota(jnp.int32, (1, 128), 1)
    return jnp.where(lane < C, mean, lax.rsqrt(var + EPS))


def pfn_kernel(
    pts_in, cnt_in, cell_in, w_in, gain_in, bias_in, pgain_in, pbias_in,
    kept_ref, part_ref,
    base_ref, w_pad, pts_ref, cnt_ref, cell_ref, w_ref, gain_ref, bias_ref, pgain_ref, pbias_ref, sems,
):
    copies = [
        pltpu.make_async_copy(src, dst, sems.at[i])
        for i, (src, dst) in enumerate(
            (
                (pts_in, pts_ref), (cnt_in, cnt_ref), (cell_in, cell_ref), (w_in, w_ref),
                (gain_in, gain_ref), (bias_in, bias_ref), (pgain_in, pgain_ref), (pbias_in, pbias_ref),
            )
        )
    ]
    for copy in copies:
        copy.start()
    for copy in copies:
        copy.wait()
    kept_ref[pl.ds(GB_ROW, 16), :] = jnp.zeros((16, NS * PILL), F32)
    lanes = pl.ds(0, 128)
    kept_ref[pl.ds(GB_ROW, LAYERS), lanes] = jnp.concatenate([gain_ref[...], bias_ref[...]], axis=1)
    kept_ref[pl.ds(GB_ROW + LAYERS, 1), lanes] = jnp.concatenate([pgain_ref[...], pbias_ref[...]], axis=1)
    kept_ref[pl.ds(TARGET_ROW, NS), pl.ds(0, PILL)] = target_lane(cell_ref[...]).astype(F32)
    w_pad[...] = jnp.zeros((128, 128), F32)
    w_pad[pl.ds(0, 9), pl.ds(0, C)] = w_ref[...]
    w_cols = jnp.transpose(w_pad[...])

    def col(j):
        return w_cols[:C, j : j + 1]

    wx = col(0) + col(4) + col(7)
    wy = col(1) + col(5) + col(8)
    wz = col(2) + col(6)
    wr = col(3)
    slot = lax.broadcasted_iota(jnp.int32, (MAXP, PILL), 0)
    total = jnp.zeros((C, 1), F32)
    number = jnp.zeros((1, 1), F32)
    for n in range(NS):
        count_i = cnt_ref[pl.ds(n, 1), :]
        count = count_i.astype(F32)
        valid = slot < count_i
        sums = []
        for j in range(4):
            p = pts_ref[pl.ds((n * 4 + j) * MAXP, MAXP), :]
            sums.append(jnp.sum(jnp.where(valid, p, 0.0), axis=0, keepdims=True))
        cell = cell_ref[pl.ds(n, 1), :]
        col_pos = jnp.bitwise_and(cell, GW - 1).astype(F32) * (2.0 / GW) - 1.0
        row_pos = jnp.right_shift(cell, 8).astype(F32) * (2.0 / GH) - 1.0
        base = -(
            col(4) * (sums[0] / count)
            + col(5) * (sums[1] / count)
            + col(6) * (sums[2] / count)
            + col(7) * col_pos
            + col(8) * row_pos
        )
        base_ref[:, pl.ds(n * PILL, PILL)] = base
        weighted = wx * sums[0] + wy * sums[1] + wz * sums[2] + wr * sums[3] + base * count
        total = total + jnp.sum(weighted, axis=1, keepdims=True)
        number = number + jnp.sum(count, axis=1, keepdims=True)
    mean = total / number
    sq_parts = []
    half = C // 2
    for c0 in (0, half):
        ch = slice(c0, c0 + half)
        bx = jnp.broadcast_to(wx[ch], (half, 128))
        by = jnp.broadcast_to(wy[ch], (half, 128))
        bz = jnp.broadcast_to(wz[ch], (half, 128))
        br = jnp.broadcast_to(wr[ch], (half, 128))
        mb = jnp.broadcast_to(mean[ch], (half, 128))

        def tile(t, sq, c0=c0, bx=bx, by=by, bz=bz, br=br, mb=mb):
            n = lax.div(t, PILL // 128)
            lanes = lanes_from((t - n * (PILL // 128)) * 128)
            base = base_ref[pl.ds(c0, half), lanes_from(t * 128)] - mb
            count = jnp.where(n == 0, cnt_ref[pl.ds(0, 1), lanes], cnt_ref[pl.ds(1, 1), lanes])

            def step(k8, carry):
                best, sq = carry
                p = [
                    pts_ref[pl.ds(pl.multiple_of((n * 4 + j) * MAXP + k8 * 8, 8), 8), lanes] for j in range(4)
                ]
                for i in range(8):
                    px, py, pz, pr = (v[i : i + 1] for v in p)
                    d = bx * px + by * py + (bz * pz + br * pr) + base
                    ok = jnp.broadcast_to(k8 * 8 + i < count, (half, 128))
                    best = jnp.where(ok, jnp.maximum(best, d), best)
                    sq = sq + jnp.where(ok, d * d, 0.0)
                return best, sq

            best, sq = lax.fori_loop(0, MAXP // 8, step, (jnp.full((half, 128), -3.0e38, F32), sq))
            kept_ref[pl.ds(c0, half), lanes_from(t * 128)] = best + mb
            return sq

        sq = lax.fori_loop(0, NS * PILL // 128, tile, jnp.zeros((half, 128), F32))
        sq_parts.append(sq)
    lane = lanes128()
    part_ref[pl.ds(0, 1), :] = to_row(
        jnp.where(lane == 0, total, 0.0), jnp.concatenate(sq_parts, axis=0)
    )
    part_ref[pl.ds(1, 1), :] = jnp.broadcast_to(number, (1, 128))


def targets_of(kept_ref, n):
    at = pl.ds(0, PILL)
    first, second = kept_ref[pl.ds(TARGET_ROW, 1), at], kept_ref[pl.ds(TARGET_ROW + 1, 1), at]
    return jnp.where(n == 0, first, second).astype(jnp.int32)


def weights_kernel(w_ref, f_hi, f_lo, b_hi, b_lo, buf_ref):
    for l in range(LAYERS):
        at = pl.ds(l * 3 * C, 3 * C)
        f_hi[at, :], f_lo[at, :] = split(forward_weights(w_ref, buf_ref, l))
        if l > 0:
            at = pl.ds((l - 1) * 3 * C, 3 * C)
            b_hi[at, :], b_lo[at, :] = split(backward_weights(w_ref, buf_ref, l))


def target_lane(cell):
    row = jnp.right_shift(cell, 8)
    col = jnp.bitwise_and(cell, GW - 1)
    phase = jnp.bitwise_and(row, 1) * 2 + jnp.bitwise_and(col, 1)
    return phase * POS + jnp.right_shift(row, 1) * OW + jnp.right_shift(col, 1)


def build_onehot(oht_ref, target):
    wide = jnp.broadcast_to(target, (256, PILL))
    iota = lax.broadcasted_iota(jnp.int32, (256, PILL), 0)

    def step(t, _):
        rows = pl.ds(pl.multiple_of(t * 256, 256), 256)
        oht_ref[rows, :] = jnp.where(iota + t * 256 == wide, 1.0, 0.0).astype(BF16)
        return _

    lax.fori_loop(0, GH * GW // 256, step, 0)


def first_conv_kernel(
    g_ref, kept_ref, wh_ref, wl_ref,
    z_ref, part_ref, ev_hi, ev_lo, od_hi, od_lo,
    oht_ref, place_ref,
):
    s = rows_of(g_ref, 2, 0)
    num = rows_of(g_ref, 2, 1)
    total = jnp.sum(s, axis=0, keepdims=True)
    number = jnp.sum(num, axis=0, keepdims=True)
    mean = total / number
    dev = s / num - mean
    spread = jnp.sum(num * dev * dev, axis=0, keepdims=True)
    var = (total + pltpu.roll(jnp.broadcast_to(spread, (8, 128)), C, 1)[:1]) / number
    lane_row = lax.broadcasted_iota(jnp.int32, (1, 128), 1)
    stats = columns(jnp.where(lane_row < C, mean, lax.rsqrt(var + EPS)))
    mean_c, inv_c = stats[:C], stats[C:]
    gain, bias = gain_bias(kept_ref, LAYERS)
    lane = lanes128()
    w_hi, w_lo = (ref[pl.ds(0, 3 * C), :] for ref in (wh_ref, wl_ref))
    outer_hi = jnp.concatenate([w_hi[:C], w_hi[2 * C :]], axis=0)
    outer_lo = jnp.concatenate([w_lo[:C], w_lo[2 * C :]], axis=0)

    def sweep(n, _):
        build_onehot(oht_ref, targets_of(kept_ref, n))
        tiles = []
        for q in range(PILL // 128):
            h = kept_ref[pl.ds(0, C), lanes_from(n * PILL + q * 128)]
            tiles.append(jnp.maximum(gain * (h - mean_c) * inv_c + bias, 0.0))
        p_hi, p_lo = split(jnp.concatenate(tiles, axis=1))
        place_ref[...] = dot_nt(jnp.concatenate([p_hi, p_lo], axis=0), oht_ref[...])
        for pr, refs in ((0, (ev_hi, ev_lo)), (1, (od_hi, od_lo))):
            for part, ref in enumerate(refs):
                width = POS + pr * OW
                if pr:
                    ref[:, lanes_from(n * width)] = jnp.zeros((3 * C, OW), BF16)
                for r in range(OH):
                    even = place_ref[pl.ds(part * C, C), pl.ds(pr * 2 * POS + r * OW, OW)]
                    odd = place_ref[pl.ds(part * C, C), pl.ds((pr * 2 + 1) * POS + r * OW, OW)]
                    at = lanes_from(n * width + (r + pr) * OW)
                    ref[pl.ds(0, C), at] = from_left(odd, lane).astype(BF16)
                    ref[pl.ds(C, C), at] = even.astype(BF16)
                    ref[pl.ds(2 * C, C), at] = odd.astype(BF16)
        at = lanes_from(n * POS, POS)
        z = dot3(dot_nn, w_hi[C : 2 * C], w_lo[C : 2 * C], ev_hi[:, at], ev_lo[:, at])
        at = lanes_from(n * (POS + OW), POS + OW)
        p = dot3(dot_nn, outer_hi, outer_lo, od_hi[:, at], od_lo[:, at])
        z_ref[:, lanes_from(n * POS, POS)] = z + p[:C, :POS] + p[C:, OW:]
        return _

    each_sweep(sweep)
    store_stats(z_ref, part_ref)


def first_grad_rows(grad_of, grid_refs, extra=0):
    ev_hi, ev_lo, od_hi, od_lo = grid_refs
    ones = [jnp.ones((extra, POS), BF16)] * (extra > 0)

    def sweep(n, rows):
        g_hi, g_lo = grad_of(n)
        whole = jnp.concatenate([g_hi, g_lo, *ones], axis=0)
        upper = jnp.concatenate([g_hi, *ones], axis=0) if extra else g_hi
        out = []
        for row, hi, lo, start in zip(
            rows,
            (od_hi, ev_hi, od_hi),
            (od_lo, ev_lo, od_lo),
            (n * (POS + OW), n * POS, n * (POS + OW) + OW),
        ):
            at = lanes_from(start, POS)
            high = dot_nt(whole, hi[:, at])
            both = jnp.concatenate([high[:C] + high[C : 2 * C], high[2 * C :]], axis=0) if extra else high[:C] + high[C:]
            out.append(row + both + dot_nt(upper, lo[:, at]))
        return tuple(out)

    return each_sweep(sweep, tuple(jnp.zeros((C + extra, 3 * C), F32) for _ in range(3)))


def conv_kernel(
    g_ref, z_ref, gb_ref, wh_ref, wl_ref, out_ref, part_ref, stats_ref, s_hi, s_lo, *, layer
):
    stats = columns(gathered_stats(g_ref[...]))
    stats_ref[...] = stats
    mean, inv = stats[:C], stats[C:]
    gain, bias = gain_bias(gb_ref, layer - 1)
    lane = lanes128()
    zero_borders((s_hi, s_lo))
    w_hi, w_lo = (ref[pl.ds(layer * 3 * C, 3 * C), :] for ref in (wh_ref, wl_ref))

    def activate(at, n, r):
        y = gain * ((z_ref[:, at] - mean) * inv) + bias
        put_shifted(s_hi, s_lo, n, r, y * jax.nn.sigmoid(y), lane)

    def sweep(n, _):
        out_ref[:, lanes_from(n * POS, POS)] = conv_padded(w_hi, w_lo, s_hi, s_lo, n)
        return _

    each_row(activate)
    each_sweep(sweep)
    store_stats(out_ref, part_ref)


def turn_kernel(
    g_ref, z_ref, gb_ref, ct_ref, z0_ref, stats0_ref, ev_hi, ev_lo, od_hi, od_lo,
    feat_ref, gy_ref, keep_ref, send_ref, stats_ref,
    buf_ref,
):
    stats = columns(gathered_stats(g_ref[...]))
    stats_ref[...] = stats
    mean, inv = stats[:C], stats[C:]
    gain, bias = gain_bias(gb_ref, LAYERS - 1)
    dy = jnp.zeros((C, 128), F32)
    dx = jnp.zeros((C, 128), F32)
    for n in range(NS):
        for r in range(OH):
            at = pl.ds(n * POS + r * OW, OW)
            rows = pl.ds(n * C * OH + r, C, stride=OH)
            xhat = (z_ref[:, at] - mean) * inv
            y = gain * xhat + bias
            sg = jax.nn.sigmoid(y)
            feat_ref[rows, :] = y * sg
            gy = ct_ref[rows, :] * (sg * (1.0 + y * (1.0 - sg)))
            gy_ref[:, at] = gy
            dy = dy + gy
            dx = dx + gy * xhat
    part = to_row(dy, dx)
    keep_ref[pl.ds(0, 1), :] = part
    send_ref[pl.ds(0, 1), :] = part
    mean0, inv0 = stats0_ref[pl.ds(0, C), pl.ds(0, 1)], stats0_ref[pl.ds(C, C), pl.ds(0, 1)]
    grads = first_grad_rows(
        lambda n: split((z0_ref[:, lanes_from(n * POS, POS)] - mean0) * inv0), (ev_hi, ev_lo, od_hi, od_lo), 16
    )
    refs = (keep_ref, send_ref)
    none = jnp.zeros((TAP_ROWS, 128), F32)
    last = store_kernel_grad(refs, 0, [row[:C] for row in grads], buf_ref)
    sums = [jnp.broadcast_to(row[C : C + 1], (C, 3 * C)) for row in grads]
    last_sums = store_kernel_grad(refs, 1, sums, buf_ref)
    store_half(refs, 2, [last, last_sums, none, none], [none] * 4)


def grad_scales(g, stats, gain):
    total = jnp.sum(g, axis=0, keepdims=True)
    entries = 2.0 * NPOS * g.shape[0]
    t = columns(total * (1.0 / entries))
    return gain * stats[C:], t[:C], t[C:], total


def padded_grad_rows(s_hi, s_lo, a_hi, a_lo):
    span = NS * PADW - 2 * OW
    g_at = pl.ds(OW, span)
    g_hi, g_lo = s_hi[pl.ds(C, C), g_at], s_lo[pl.ds(C, C), g_at]
    return [
        dot3(dot_nt, g_hi, g_lo, a_hi[:, pl.ds(a * OW, span)], a_lo[:, pl.ds(a * OW, span)]) for a in range(3)
    ]


def back_kernel(
    g_ref, z_ref, gy_ref, stats_ref, gb_ref, zp_ref, statsp_ref, wh_ref, wl_ref, *refs, layer, stride
):
    if layer == 1:
        grid0, last3_ref, last2_ref, refs = refs[:4], refs[4], refs[5], refs[6:]
    gyp_ref, sums_ref, red_ref, keep_ref, send_ref, *refs = refs
    if layer != 1:
        last_ref, *refs = refs
    s_hi, s_lo, a_hi, a_lo, slope_ref, buf_ref = refs
    reduced_rows(g_ref, stride, red_ref, red_ref.shape[0])
    stats = stats_ref[...]
    mean, inv = stats[:C], stats[C:]
    gain, _ = gain_bias(gb_ref, layer)
    scale, mean_dy, mean_dx, sums_ref[...] = grad_scales(rows_of(g_ref, stride, 0), stats, gain)
    statsp = statsp_ref[...]
    meanp, invp = statsp[:C], statsp[C:]
    gainp, biasp = gain_bias(gb_ref, layer - 1)
    lane = lanes128()
    zero_borders((s_hi, s_lo, a_hi, a_lo))
    w_hi, w_lo = (ref[pl.ds((layer - 1) * 3 * C, 3 * C), :] for ref in (wh_ref, wl_ref))

    def turn_back(at, n, r):
        xhat = (z_ref[:, at] - mean) * inv
        gz = scale * (gy_ref[:, at] - mean_dy - xhat * mean_dx)
        put_shifted(s_hi, s_lo, n, r, gz, lane)
        y = gainp * ((zp_ref[:, at] - meanp) * invp) + biasp
        sg = jax.nn.sigmoid(y)
        slope_ref[:, at] = sg * (1.0 + y * (1.0 - sg))
        put_shifted(a_hi, a_lo, n, r, y * sg, lane)

    def sweep(n, carry):
        dy, dx = carry
        u = conv_padded(w_hi, w_lo, s_hi, s_lo, n)
        for r in range(OH):
            at = lanes_from(n * POS + r * OW)
            gy = u[:, r * OW : (r + 1) * OW] * slope_ref[:, at]
            gyp_ref[:, at] = gy
            dy = dy + gy
            dx = dx + gy * ((zp_ref[:, at] - meanp) * invp)
        return dy, dx

    each_row(turn_back)
    zero = jnp.zeros((C, 128), F32)
    dy, dx = each_sweep(sweep, (zero, zero))
    part = to_row(dy, dx)
    keep_ref[pl.ds(0, 1), :] = part
    send_ref[pl.ds(0, 1), :] = part
    refs = (keep_ref, send_ref)
    last = store_kernel_grad(refs, 0, padded_grad_rows(s_hi, s_lo, a_hi, a_lo), buf_ref)
    if layer != 1:
        last_ref[...] = last
        return
    rows = first_grad_rows(lambda n: split(gyp_ref[:, lanes_from(n * POS, POS)]), grid0)
    last0 = store_kernel_grad(refs, 1, rows, buf_ref)
    none = jnp.zeros((TAP_ROWS, 128), F32)
    store_half(refs, 2, [last0, none, none, none], [last, last2_ref[...], last3_ref[...], none])


def pick_channels(tile, pair, lane):
    row = lax.broadcasted_iota(jnp.int32, (C, 128), 0)
    want = 2 * pair + jnp.where(lane < C, 0, 1)
    return jnp.sum(jnp.where(row == want, tile, 0.0), axis=0, keepdims=True)


def own_rows_kernel(
    g_ref, stats_ref, gb_ref, first_red, red3, red2, sums1, sums2, sums3, norm_ref, out_ref, scale_ref, *, stride
):
    stats = stats_ref[...]
    gain, _ = gain_bias(gb_ref, 0)
    scale, mean_dy, mean_dx, sums0 = grad_scales(rows_of(g_ref, stride, 0), stats, gain)
    for l, row in enumerate((sums0, sums1[...], sums2[...], sums3[...])):
        norm_ref[pl.ds(l, 1), :] = row[:, C:]
        norm_ref[pl.ds(LAYERS + l, 1), :] = row[:, :C]
    for i, tile in enumerate((scale, mean_dy, mean_dx)):
        scale_ref[pl.ds(i * C, C), :] = tile
    lane = lanes128()
    count = red3.shape[0]
    peers = BLOCK // count
    spot = lax.axis_index(WIDE)

    def first_grad(raw, normed, plain, pair):
        return pick_channels(scale, pair, lane) * (
            raw - pick_channels(mean_dy, pair, lane) * plain - pick_channels(mean_dx, pair, lane) * normed
        )

    for j in range(count):
        pair = lax.rem(j * peers + spot, TAP_ROWS)
        here, raw, ends = (
            jnp.sum(rows_of(g_ref, stride, 1 + q * count + j), axis=0, keepdims=True) for q in range(3)
        )
        normed, plain, end = (first_red[pl.ds(q * count + j, 1), :] for q in range(3))
        plain_peer = lax.div(j * peers + spot, TAP_ROWS) == 1
        end_grad = pick_channels(scale, pair, lane) * (
            ends - pick_channels(jnp.where(plain_peer, mean_dy, mean_dx), pair, lane) * end
        )
        ends = jnp.where(first_core(), end_grad, ends)
        own = (first_grad(raw, normed, plain, pair), here, red2[pl.ds(j, 1), :], red3[pl.ds(j, 1), :], ends)
        for q in range(5):
            at = pl.ds(q * count + j, peers, stride=5 * count)
            out_ref[at, :] = jnp.broadcast_to(own[q], (peers, 128))


def last_back_kernel(
    z_ref, gy_ref, stats_ref, scale_ref, kept_ref, w_ref, pg_ref, t_hi, t_lo, u_hi, oht_ref, buf_ref
):
    mean, inv = stats_ref[pl.ds(0, C), :], stats_ref[pl.ds(C, C), :]
    scale, mean_dy, mean_dx = (scale_ref[pl.ds(i * C, C), :] for i in range(3))
    lane = lanes128()
    v_hi, v_lo = split(first_backward_weights(w_ref, buf_ref))

    def sweep(n, _):
        for ref in (t_hi, t_lo):
            ref[:, pl.ds(POS, OW)] = jnp.zeros((2 * C, OW), BF16)
        for r in range(OH):
            at = lanes_from(n * POS + r * OW)
            xhat = (z_ref[:, at] - mean) * inv
            gz = scale * (gy_ref[:, at] - mean_dy - xhat * mean_dx)
            put(t_hi, t_lo, 0, r * OW, gz)
            put(t_hi, t_lo, C, r * OW, from_right(gz, lane))
        v = dot3(dot_nn, v_hi, v_lo, t_hi[...], t_lo[...])
        for pc in range(2):
            above = v[pc * C : (pc + 1) * C, OW:]
            here = v[(2 + pc) * C : (3 + pc) * C, :POS]
            below = v[(4 + pc) * C : (5 + pc) * C, :POS]
            for pr, u in ((0, here), (1, below + above)):
                at = pl.ds((pr * 2 + pc) * POS, POS)
                hi, lo = split(u)
                u_hi[pl.ds(0, C), at] = hi
                u_hi[pl.ds(C, C), at] = lo
        build_onehot(oht_ref, targets_of(kept_ref, n))
        picked = dot_nn(u_hi[...], oht_ref[...])
        pg_ref[pl.ds(pl.multiple_of(n * C, C), C), :] = picked[:C] + picked[C:]
        return _

    each_sweep(sweep)


def pair_kernel(*refs, mode, stride):
    *ins, out_ref = refs
    peers = out_ref.shape[0] // stride
    if len(ins) == 1:
        keep_ref, got_ref = ins[0].at[pl.ds(0, 8)], ins[0].at[pl.ds(8, 8)]
    else:
        keep_ref, got_ref = ins
    mine, other = keep_ref[pl.ds(0, 1), :], got_ref[pl.ds(0, 1), :]
    both = mine + other
    lane = lax.broadcasted_iota(jnp.int32, (1, 128), 1)

    def swap(v):
        return pltpu.roll(jnp.broadcast_to(v, (8, 128)), C, 1)[:1]

    if mode == "stats":
        gap = mine - other
        both = jnp.where(lane < C, 0.5 * both, both + (0.5 * NPOS) * swap(gap * gap))
    if mode == "pillars":
        m_num, o_num = keep_ref[pl.ds(1, 1), :], got_ref[pl.ds(1, 1), :]
        number = m_num + o_num
        gap = mine / m_num - other / o_num
        both = jnp.where(lane < C, both, both + (m_num * o_num / number) * swap(gap * gap))
        out_ref[pl.ds(1, peers, stride=stride), :] = jnp.broadcast_to(number, (peers, 128))
    row = jnp.broadcast_to(both, (peers, 128))
    if stride == 1:
        out_ref[...] = row
    else:
        out_ref[pl.ds(0, peers, stride=stride), :] = row
    for j, start in enumerate(range(8, keep_ref.shape[0], peers)):
        at = pl.ds(start, peers)
        out_ref[pl.ds(1 + j, peers, stride=stride), :] = keep_ref[at, :] + got_ref[at, :]


def assemble_kernel(both_ref, out_ref, *, peers):
    count = BLOCK // peers
    per_peer = (LAYERS + 1) * count

    def rows_at(core, start, size):
        return both_ref[pl.ds(core * peers * per_peer + start, size, stride=per_peer), :]

    for l in range(LAYERS):
        for j in range(count):
            for core in range(2):
                at = pl.ds((core * BLOCK + j * peers) * LAYERS + l, peers, stride=LAYERS)
                out_ref[at, :] = rows_at(core, l * count + j, peers)
        size = min(peers, TAP_ROWS)
        for step in range(0, TAP_ROWS, size):
            start = max(l - 1, 0) * TAP_ROWS + step
            rows = rows_at(min(l, 1), start % peers * per_peer + LAYERS * count + start // peers, size)
            if l == 0:
                start += TAP_ROWS
                rows = rows + rows_at(0, start % peers * per_peer + LAYERS * count + start // peers, size)
            out_ref[pl.ds((2 * BLOCK + step) * LAYERS + l, size, stride=LAYERS), :] = rows


def call(kernel, name, outs, args, scratch=(), copies=False, **params):
    specs = [pl.BlockSpec(memory_space=pltpu.HBM if copies else pltpu.VMEM)] * len(args)
    return pl.pallas_call(
        functools.partial(kernel, **params) if params else kernel,
        name=name,
        out_shape=tuple(jax.ShapeDtypeStruct(shape, dtype) for shape, dtype in outs),
        in_specs=specs,
        scratch_shapes=[pltpu.VMEM(shape, dtype) for shape, dtype in scratch]
        + [pltpu.SemaphoreType.DMA((len(args),))] * copies,
        compiler_params=None if copies else pltpu.CompilerParams(vmem_limit_bytes=20 << 20),
        interpret=INTERPRET,
    )(*args)


def partner(v):
    return lax.ppermute(v, "k", [(0, 1), (1, 0)])


def to_peers(rows, peers):
    sent = rows.reshape(peers, -1, 1, 128)
    return lax.all_to_all(sent, WIDE, 0, 0, tiled=True).reshape(-1, 128)


def exchange(name, mode, keep, peers, send=None):
    pair = (lax.all_gather(keep, "k", tiled=True),) if send is None else (keep, partner(send))
    rows = (2 if mode == "pillars" else 1) + (keep.shape[0] - 8) // peers
    (out,) = call(pair_kernel, name, [((peers * rows, 128), F32)], pair, mode=mode, stride=rows)
    return to_peers(out, peers)


def per_device(
    points, counts, cells, pfn_weight, pfn_gain, pfn_bias, conv_weight, bn_gain, bn_bias, cotangent,
    *, sizes,
):
    peers = sizes["x"] * sizes["y"] * sizes["z"]
    count = BLOCK // peers
    w = conv_weight.reshape(LAYERS, 9, TAP_ROWS, 128).transpose(1, 2, 0, 3).reshape(9 * TAP_ROWS * LAYERS, 128)
    row = ((1, 128), F32)
    rows8 = ((8, 128), F32)
    tile = ((128, 128), F32)
    plane = ((C, NPOS), F32)
    pad = ((3 * C, NS * PADW), BF16)
    buf = ((C, C), F32)
    end = ((TAP_ROWS, 128), F32)

    ints = ((NS, PILL), jnp.int32)
    vectors = [((LAYERS, C), F32)] * 2 + [((1, C), F32)] * 2
    kept, part = call(
        pfn_kernel, "pfn", [((KEPT_ROWS, NS * PILL), F32), rows8],
        (
            points.reshape(NS * 4 * MAXP, PILL), counts, cells, pfn_weight,
            bn_gain, bn_bias, pfn_gain[None], pfn_bias[None],
        ),
        [((C, NS * PILL), F32), tile, ((NS * 4 * MAXP, PILL), F32), ints, ints, ((9, C), F32)] + vectors,
        copies=True,
    )
    half = [((LAYERS * 3 * C, 3 * C), BF16)] * 2
    *w_fwd, b_hi, b_lo = call(
        weights_kernel, "weights", half + [(((LAYERS - 1) * 3 * C, 3 * C), BF16)] * 2, (w,), [buf]
    )
    got = exchange("pair_p", "pillars", part, peers)
    ev = ((3 * C, NS * POS), BF16)
    od = ((3 * C, NS * (POS + OW)), BF16)
    z, part, *grid0 = call(
        first_conv_kernel, "conv0", [plane, rows8, ev, ev, od, od],
        (got, kept, *w_fwd),
        [((GH * GW, PILL), BF16), ((2 * C, GH * GW), F32)],
    )
    pre = [z]
    stats = []
    for l in range(1, LAYERS):
        got = exchange("pair_s", "stats", part, peers)
        z, part, st = call(
            conv_kernel, f"conv{l}", [plane, rows8, tile], (got, pre[-1], kept, *w_fwd), [pad, pad], layer=l
        )
        pre.append(z)
        stats.append(st)
    got = exchange("pair_s", "stats", part, peers)
    slab = ((NS * C * OH, OW), F32)
    three = ((8 + 3 * BLOCK, 128), F32)
    feat, gy, keep, send, st = call(
        turn_kernel, "turn", [slab, plane, three, three, tile],
        (got, pre[-1], kept, cotangent.reshape(NS * C * OH, OW), pre[0], stats[0], *grid0), [buf],
    )
    stats.append(st)
    sums = [None] * LAYERS
    reds = []
    ends = []
    for l in range(LAYERS - 1, 0, -1):
        got = exchange("pair_g", "sums", keep, peers, send)
        blocks = got.shape[0] // peers - 1
        fresh = ((8 + (3 if l == 1 else 1) * BLOCK, 128), F32)
        gy, sums[l], red, keep, send, *last = call(
            back_kernel, f"back{l}",
            [plane, row, ((blocks, 128), F32), fresh, fresh] + [end] * (l > 1),
            (got, pre[l], gy, stats[l], kept, pre[l - 1], stats[l - 1], b_hi, b_lo) + ((*grid0, *ends) if l == 1 else ()),
            [pad, pad, pad, pad, plane, buf], layer=l, stride=blocks + 1,
        )
        reds.append(red)
        ends += last
    got = exchange("pair_z", "sums", keep, peers, send)
    rows = (LAYERS + 1) * count
    norm_grads, own, scales = call(
        own_rows_kernel, "own_rows", [((2 * LAYERS, C), F32), ((peers * rows, 128), F32), ((3 * C, 128), F32)],
        (got, stats[0], kept, *reds, *sums[1:]), stride=got.shape[0] // peers,
    )
    both = lax.all_gather(to_peers(own, peers), "k", tiled=True)
    tbuf = ((2 * C, POS + OW), BF16)
    (pillar_grad,) = call(
        last_back_kernel, "back0", [((NS * C, PILL), F32)],
        (pre[0], gy, stats[0], scales, kept, w),
        [tbuf, tbuf, ((2 * C, GH * GW), BF16), ((GH * GW, PILL), BF16), buf],
    )
    (total,) = call(
        assemble_kernel, "assemble", [((9 * TAP_ROWS * LAYERS, 128), F32)], (both,), peers=peers
    )
    total = total.reshape(9, TAP_ROWS, LAYERS, 128).transpose(2, 0, 1, 3).reshape(LAYERS, 9, C * C)
    return (
        feat.reshape(NS, C, OH, OW),
        total,
        norm_grads.reshape(2, LAYERS, C),
        pillar_grad.reshape(NS, C, PILL),
    )


def build(finer):
    sizes = dict(finer.shape)
    split4 = P(ALL, None, None, None)
    return jax.shard_map(
        functools.partial(per_device, sizes=sizes),
        mesh=finer,
        in_specs=(split4, P(ALL, None), P(ALL, None), P(), P(), P(), P(), P(), P(), split4),
        out_specs=(split4, P(), P(), P(ALL, None, None)),
        check_vma=False,
    )


def solution(mesh):
    return build(Mesh(mesh.devices.reshape(4, 2, 4, 8), ALL))
```
